32 devices in a mesh: shard: 4 (over y, x), ctx: 8 (over z, core).
Axes of the slice: x: 2, y: 2, z: 4, core: 2. Of those that a mesh axis runs over, the one named last changes fastest.
Arguments:
- layer_input: bfloat16 [4, 1024, 768], P('shard', 'ctx'), may hold values from -6 to 6
- positions: int32 [4, 1024], P('shard', 'ctx'), may hold values from 0 to 1023, as said below
- cotangent: bfloat16 [4, 1024, 768], P('shard', 'ctx'), may hold values from -6 to 6
- ln1_gain: float32 [768], replicated, may hold values from 0.5 to 1.5
- ln1_bias: float32 [768], replicated, may hold values from -3 to 3
- ln2_gain: float32 [768], replicated, may hold values from 0.5 to 1.5
- ln2_bias: float32 [768], replicated, may hold values from -3 to 3
- w_qkv: bfloat16 [768, 2304], P('shard')
- qkv_bias: float32 [2304], replicated, may hold values from -3 to 3
- w_out: bfloat16 [768, 768], P('shard'), may hold values from -1.25 to 1.25
- w_up: bfloat16 [768, 3072], P('shard'), may hold values from -0.21875 to 0.21875
- up_bias: float32 [3072], replicated, may hold values from -3 to 3
- w_down: bfloat16 [3072, 768], P('shard'), may hold values from -0.109375 to 0.109375
Outputs:
- layer_output: bfloat16 [4, 1024, 768], P('shard', 'ctx')
- grad_input: bfloat16 [4, 1024, 768], P('shard', 'ctx')
- grad_ln1_gain: float32 [768], replicated
- grad_ln1_bias: float32 [768], replicated
- grad_ln2_gain: float32 [768], replicated
- grad_ln2_bias: float32 [768], replicated
- grad_w_qkv: float32 [768, 2304], P('shard')
- grad_qkv_bias: float32 [2304], replicated
- grad_w_out: float32 [768, 768], P('shard')
- grad_w_up: float32 [768, 3072], P('shard')
- grad_up_bias: float32 [3072], replicated
- grad_w_down: float32 [3072, 768], P('shard')
The draws below stay inside these ranges and needn't reach their ends.
Inputs may be any that keep to these rules, and one draw needn't show every extreme that they name: In each sequence, the 128 tokens that one device holds along ctx carry consecutive positions starting at a multiple of 128; every position of the sequence occurs once.
All inputs are finite; a program needn't handle non-finite values.
Results may differ from the reference program's by a relative error of at most 0.018.
Values may be sent and summed in bfloat16 or wider, within the bound.
A program may use at most 128 MiB of HBM per device.

```python
import math
import jax
import jax.numpy as jnp
from jax import lax

D = 768
HEADS = 12
HEAD_DIM = 64
ROTARY = 16
FF = 3072
BLOCK = 128
SEQS = 4
LENGTH = 1024


def draw_positions(key, part):
    run_count = LENGTH // BLOCK
    seq_keys = jax.random.split(key, SEQS)
    orders = jax.vmap(lambda seq_key: jax.random.permutation(seq_key, run_count))(seq_keys)
    offsets = jnp.arange(BLOCK, dtype=jnp.int32)
    starts = orders.astype(jnp.int32)[:, :, None] * BLOCK
    return (starts + offsets[None, None, :]).reshape(SEQS, LENGTH).astype(jnp.int32)


def draw_w_qkv(key, part):
    base = jax.random.normal(key, (D, 3 * D), jnp.float32) * D ** (-0.5)
    return base.astype(jnp.bfloat16)


def block_scale(rng, dims, cuts, least, top_value):
    factor_of, own = 1.0, jax.random.fold_in(rng, 6)
    for dim, parts in cuts:
        heights = jnp.exp(jax.random.uniform(jax.random.fold_in(own, dim), (parts,), jnp.float32, least / len(cuts), top_value / len(cuts)))
        factor_of = factor_of * jnp.repeat(heights, dims[dim] // parts).reshape([-1 if axis == dim else 1 for axis in range(len(dims))])
    return factor_of


def centred(own_key, shape, width, bound, pieces=(), kind=jnp.bfloat16):
    values = width * jax.random.normal(own_key, shape, jnp.float32)
    if pieces:
        values = values * block_scale(own_key, shape, pieces, -0.22, 0.18)
    return jnp.clip(values, -bound, bound).astype(kind)


def setup_inputs(seed: int = 0) -> dict:
    streams_of = jax.random.split(jax.random.key(seed), 14)
    layer_input = centred(streams_of[0], (SEQS, LENGTH, D), 1.0, 6.0, ((0, 4), (1, 8)))
    positions = draw_positions(jax.random.fold_in(streams_of[13], 71), 0)
    cotangent = centred(streams_of[2], (SEQS, LENGTH, D), 1.0, 6.0, ((0, 4), (1, 8)))
    ln1_gain = jnp.clip(1.0 + 0.1 * jax.random.normal(streams_of[3], (D,), jnp.float32), 0.5, 1.5)
    ln1_bias = centred(streams_of[4], (D,), 0.5, 3.0, (), jnp.float32)
    ln2_gain = jnp.clip(1.0 + 0.1 * jax.random.normal(streams_of[5], (D,), jnp.float32), 0.5, 1.5)
    ln2_bias = centred(streams_of[6], (D,), 0.5, 3.0, (), jnp.float32)
    w_qkv = draw_w_qkv(jax.random.fold_in(streams_of[13], 71), 0)
    qkv_bias = centred(streams_of[8], (3 * D,), 0.5, 3.0, (), jnp.float32)
    w_out = centred(streams_of[9], (D, D), (D // 32) ** -0.5, 1.25, ((0, 4),))
    w_up = centred(streams_of[10], (D, FF), D ** -0.5, 0.21875, ((0, 4),))
    up_bias = centred(streams_of[11], (FF,), 0.5, 3.0, (), jnp.float32)
    w_down = centred(streams_of[12], (FF, D), FF ** -0.5, 0.109375, ((0, 4),))
    return {"layer_input": layer_input, "positions": positions, "cotangent": cotangent, "ln1_gain": ln1_gain, "ln1_bias": ln1_bias, "ln2_gain": ln2_gain, "ln2_bias": ln2_bias, "w_qkv": w_qkv, "qkv_bias": qkv_bias, "w_out": w_out, "w_up": w_up, "up_bias": up_bias, "w_down": w_down}


EPSILON = 1e-05
NEGATIVE = -1e+30
HIGH = lax.Precision.HIGHEST

@jax.custom_vjp
def low(v):
    return lax.optimization_barrier(v.astype(jnp.bfloat16)).astype(jnp.float32)

@jax.custom_vjp
def low_back(v):
    return v

def low_keep(v):
    return (low(v), None)

def low_pass(kept, grad):
    return (grad,)

def back_keep(v):
    return (v, None)

def back_low(kept, grad):
    return (low(grad),)
low.defvjp(low_keep, low_pass)
low_back.defvjp(back_keep, back_low)

def layer_norm(values_in, gain_vec, bias_vec):
    centered = values_in - lax.optimization_barrier(jnp.mean(values_in, axis=-1, keepdims=True))
    variance = lax.optimization_barrier(jnp.mean(centered * centered, axis=-1, keepdims=True))
    return centered * lax.rsqrt(variance + EPSILON) * gain_vec + bias_vec

def rotary_tables(position_ids):
    half_dim = ROTARY // 2
    inverse_freq = 1.0 / 10000.0 ** (jnp.arange(half_dim, dtype=jnp.float32) * (2.0 / ROTARY))
    angles = position_ids.astype(jnp.float32)[..., None] * inverse_freq
    return (jnp.cos(angles), jnp.sin(angles))

def rotate(field_in, cosine, sine_table):
    half_dim = cosine.shape[-1]
    lead_part = field_in[..., :half_dim]
    second = field_in[..., half_dim:2 * half_dim]
    remain = field_in[..., 2 * half_dim:]
    cos_wide = cosine[..., None, :]
    sin_wide = sine_table[..., None, :]
    return jnp.concatenate([lead_part * cos_wide - second * sin_wide, second * cos_wide + lead_part * sin_wide, remain], axis=-1)

def one_sequence(params, tokens, position):
    gain_one, bias_one, gain_two, bias_two, weight_qkv, bias_qkv, weight_out, weight_up, bias_up, weight_down = params
    length = tokens.shape[0]
    normed_one = low(layer_norm(tokens, gain_one, bias_one))
    normed_two = low(layer_norm(tokens, gain_two, bias_two))
    projected = low_back(jnp.dot(normed_one, weight_qkv, precision=HIGH) + bias_qkv)
    split_heads = projected.reshape(length, 3, HEADS, HEAD_DIM)
    cosine, sine_table = rotary_tables(position)
    queries = low(rotate(split_heads[:, 0], cosine, sine_table))
    key_rows = low(rotate(split_heads[:, 1], cosine, sine_table))
    values = low(split_heads[:, 2])
    score_scale = HEAD_DIM ** (-0.5)
    rows_block = math.gcd(length, 512)

    def attend(block_pair):
        query_block, query_pos = block_pair
        scores = low_back(jnp.einsum('qhd,khd->hqk', query_block, key_rows, precision=HIGH) * score_scale)
        allowed = position[None, None, :] <= query_pos[None, :, None]
        masked = jnp.where(allowed, scores, NEGATIVE)
        row_top = lax.optimization_barrier(jnp.max(masked, axis=-1, keepdims=True))
        exponent = jnp.exp(masked - row_top)
        probability = low(exponent / lax.optimization_barrier(jnp.sum(exponent, axis=-1, keepdims=True)))
        return jnp.einsum('hqk,khd->qhd', probability, values, precision=HIGH)
    mixed = lax.map(jax.checkpoint(attend), (queries.reshape(length // rows_block, rows_block, HEADS, HEAD_DIM), position.reshape(length // rows_block, rows_block)))
    attended = low(low_back(mixed.reshape(length, D)))
    attn_branch = jnp.dot(attended, weight_out, precision=HIGH)
    hidden_pre = low_back(jnp.dot(normed_two, weight_up, precision=HIGH) + bias_up)
    hidden = low(jax.nn.gelu(hidden_pre, approximate=False))
    mlp_branch = jnp.dot(hidden, weight_down, precision=HIGH)
    return tokens + attn_branch + mlp_branch

def reference(layer_input, positions, cotangent, ln1_gain, ln1_bias, ln2_gain, ln2_bias, w_qkv, qkv_bias, w_out, w_up, up_bias, w_down):
    params = (ln1_gain, ln1_bias, ln2_gain, ln2_bias, w_qkv.astype(jnp.float32), qkv_bias, w_out.astype(jnp.float32), w_up.astype(jnp.float32), up_bias, w_down.astype(jnp.float32))
    tokens = layer_input.astype(jnp.float32)
    step_fn = jax.checkpoint(one_sequence)

    def forward(params_in, tokens_in):

        def scan_body(carried, seq_item):
            return (carried, step_fn(params_in, seq_item[0], seq_item[1]))
        unused, results = lax.scan(scan_body, jnp.zeros((), jnp.float32), (tokens_in, positions))
        return results
    result, pullback = jax.vjp(forward, params, tokens)
    grad_params, grad_tokens = pullback(cotangent.astype(jnp.float32))
    return (result.astype(jnp.bfloat16), grad_tokens.astype(jnp.bfloat16), grad_params[0], grad_params[1], grad_params[2], grad_params[3], grad_params[4], grad_params[5], grad_params[6], grad_params[7], grad_params[8], grad_params[9])
```

```python
import jax
import jax.numpy as jnp
import numpy as np
from jax import lax
from jax.experimental import pallas as pl
from jax.experimental.pallas import tpu as pltpu
from jax.sharding import PartitionSpec as P

HEADS = 12
HEAD_DIM = 64
ROTARY = 16


EPSILON = 1e-05
NEGATIVE = -1e30


def shifted(shard, axis, by):
    count = lax.axis_size(axis)
    return lax.ppermute(shard, axis, [(i, (i + by) % count) for i in range(count)])


def layer_norm(values_in, gain_vec, bias_vec):
    centered = values_in - jnp.mean(values_in, axis=-1, keepdims=True)
    variance = jnp.mean(centered * centered, axis=-1, keepdims=True)
    return centered * lax.rsqrt(variance + EPSILON) * gain_vec + bias_vec


def rotary_tables(position_ids):
    half_dim = ROTARY // 2
    inverse_freq = 1.0 / 10000.0 ** (jnp.arange(half_dim, dtype=jnp.float32) * (2.0 / ROTARY))
    angles = position_ids.astype(jnp.float32)[..., None] * inverse_freq
    return (jnp.cos(angles), jnp.sin(angles))


def rotate(field_in, cosine, sine_table):
    half_dim = cosine.shape[-1]
    lead_part = field_in[..., :half_dim]
    second = field_in[..., half_dim : 2 * half_dim]
    remain = field_in[..., 2 * half_dim :]
    cos_wide = cosine[..., None, :]
    sin_wide = sine_table[..., None, :]
    return jnp.concatenate(
        [
            lead_part * cos_wide - second * sin_wide,
            second * cos_wide + lead_part * sin_wide,
            remain,
        ],
        axis=-1,
    )


def gelu_exact(field_in):
    return jax.nn.gelu(field_in, approximate=False)


MESH = pl.DeviceIdType.MESH
LOW = jnp.bfloat16
FULL = jnp.float32
ROWS_CONTRACT = (((0,), (0,)), ((), ()))
COLS_CONTRACT = (((1,), (1,)), ((), ()))
INV_ROOT_TWO = 0.7071067811865476
INV_ROOT_TWO_PI = 0.3989422804014327
LINE_LAG = 3


def dot(lhs, rhs, dims=(((1,), (0,)), ((), ()))):
    return lax.dot_general(lhs, rhs, dims, preferred_element_type=FULL)


def flip(index, bits):
    for power in (1, 2, 4, 8):
        if bits & power:
            index = index + power - 2 * power * lax.rem(lax.div(index, power), 2)
    return index


def at16(value):
    return pl.multiple_of(value, 16)


def at128(value):
    return pl.multiple_of(value, 128)


def rotary_constants(blocks, block_len):
    lane = np.arange(128) % HEAD_DIM
    half = ROTARY // 2
    turning = lane < ROTARY
    freq = np.where(turning, 10000.0 ** (-(lane % half) * (2.0 / ROTARY)), 0.0)
    sign = np.where(lane < half, -1.0, 1.0) * turning
    offset = np.arange(block_len)[:, None] * freq
    start = (np.arange(blocks) * block_len)[:, None] * freq
    parts = (np.cos(offset), np.sin(offset) * sign, np.cos(start), np.sin(start) * sign)
    return np.concatenate(parts).astype(np.float32)


def fused_body(
    x_ref,
    pos_ref,
    gain1_ref,
    bias1_ref,
    gain2_ref,
    bias2_ref,
    qkvb_ref,
    upb_ref,
    rot_ref,
    cot_hbm,
    wsel_hbm,
    wup_hbm,
    wout_hbm,
    wdn_hbm,
    y_ref,
    dx_ref,
    fin_ref,
    qkvfin_ref,
    small_ref,
    wq,
    wup,
    wout,
    wdn,
    n1,
    n2,
    cot,
    pos_tx,
    pos_rx,
    pos_sm,
    qkv,
    q_s,
    k_s,
    v_s,
    do_tx,
    do_rx,
    do_s,
    o_s,
    dq_s,
    dk_s,
    dv_s,
    gp_s,
    gp_e,
    o_tx,
    o_rx,
    attn_low,
    a1_p,
    a1_d2d,
    a1_c,
    a1_rx,
    gq_tx,
    gq_rx,
    gq_sum,
    out_acc,
    a2_acc,
    out_tx,
    out_rx,
    a2_tx,
    a2_rx,
    gd16,
    gd_rx,
    gu16,
    gu_rx,
    gu_tx,
    go16,
    go_rx,
    go_tx,
    go_x,
    line_own,
    line_rx,
    line_near,
    line_far,
    small_a,
    small_rx,
    small_b,
    small_bx,
    ssem,
    rsem,
    lsem,
):
    shards = lax.axis_size("shard")
    ctxs = lax.axis_size("ctx")
    s = lax.axis_index("shard")
    i = lax.axis_index("ctx")
    c = lax.rem(i, 2)
    z = lax.div(i, 2)
    other = 1 - c
    planes = range(1, shards)
    mates = range(1, ctxs)
    even = range(2, ctxs, 2)
    block = x_ref.shape[0]
    width = x_ref.shape[1]
    rows = width // shards
    half_rows = rows // 2
    sent = []
    used = [0]

    def channels(count):
        first = used[0]
        used[0] += count
        return first

    def remote(k, src, dst, device):
        return pltpu.make_async_remote_copy(
            src_ref=src,
            dst_ref=dst,
            send_sem=ssem.at[k],
            recv_sem=rsem.at[k],
            device_id=device,
            device_id_type=MESH,
        )

    def send(k, src, dst, **device):
        copy = remote(k, src, dst, device)
        copy.start()
        sent.append(copy)

    def arrived(k, dst):
        remote(k, dst, dst, {"ctx": flip(i, 1)}).wait_recv()

    def plane(d):
        return flip(s, d)

    def mate(e):
        return flip(i, e)

    loads = []

    def load(k, src, dst):
        copy = pltpu.make_async_copy(src, dst, lsem.at[k])
        copy.start()
        loads.append(copy)

    my_rows = pl.ds(at16(s * rows), rows)
    load(0, cot_hbm, cot.at[pl.ds(0, block)])
    load(1, wsel_hbm, wq.at[my_rows])
    load(2, wout_hbm, wout.at[my_rows])
    load(3, wup_hbm.at[:, pl.ds(at128(s * width), width)], wup.at[my_rows])
    load(4, wdn_hbm, wdn)

    barrier = pltpu.get_barrier_semaphore()
    for d in planes:
        pl.semaphore_signal(barrier, inc=1, device_id={"shard": plane(d)}, device_id_type=MESH)
    for e in mates:
        pl.semaphore_signal(barrier, inc=1, device_id={"ctx": mate(e)}, device_id_type=MESH)
    pl.semaphore_wait(barrier, shards + ctxs - 2)

    K_WQ = channels(shards)
    K_WO = channels(shards)
    K_WO2 = channels(shards)
    K_WU = channels(shards)
    K_WU2 = channels(shards)
    K_COT = channels(shards)
    K_N2 = channels(shards)
    K_POS = channels(ctxs)
    K_N1 = channels(ctxs)
    for d in planes:
        send(K_WQ + d, wsel_hbm, wq.at[my_rows], shard=plane(d))
    my_half = pl.ds(at16(s * rows + c * half_rows), half_rows)
    for d in planes:
        send(
            K_WO + d, wout_hbm.at[pl.ds(at16(c * half_rows), half_rows)], wout.at[my_half],
            shard=plane(d),
        )
    pos_tx[...] = jnp.broadcast_to(pos_ref[...], pos_tx.shape)
    x = x_ref[...].astype(FULL)
    mean = jnp.mean(x, axis=-1, keepdims=True)
    centered = x - mean
    r = lax.rsqrt(jnp.mean(centered * centered, axis=-1, keepdims=True) + EPSILON)
    normal = centered * r
    n1[pl.ds(0, block)] = (normal * gain1_ref[...] + bias1_ref[...]).astype(LOW)
    n2[pl.ds(0, block)] = (normal * gain2_ref[...] + bias2_ref[...]).astype(LOW)
    pos_rx[0] = pos_tx[...]
    for e in mates:
        send(K_POS + e, pos_tx, pos_rx.at[e], ctx=mate(e))
    for e in (1, *even):
        send(K_N1 + e, n1.at[pl.ds(0, block)], n1.at[pl.ds(block * e, block)], ctx=mate(e))
    for d in planes:
        send(
            K_WU + d,
            wup_hbm.at[
                pl.ds(at16(c * half_rows), half_rows), pl.ds(at128(plane(d) * width), width)
            ],
            wup.at[my_half],
            shard=plane(d),
        )
    for d in planes:
        send(K_N2 + d, n2.at[pl.ds(0, block)], n2.at[pl.ds(block * d, block)], shard=plane(d))
    for d in planes:
        send(K_COT + d, cot_hbm, cot.at[pl.ds(block * d, block)], shard=plane(d))
    for copy in loads:
        copy.wait()

    def rows_of(d, core):
        return pl.ds(at16(plane(d) * rows + core * half_rows), half_rows)

    for d in planes:
        arrived(K_WO + d, wout.at[rows_of(d, c)])
        send(K_WO2 + d, wout.at[rows_of(d, c)], wout.at[rows_of(d, c)], ctx=mate(1))
    for d in planes:
        arrived(K_WO2 + d, wout.at[rows_of(d, other)])

    lane = lax.broadcasted_iota(jnp.int32, (block, 128), 1)
    low_lanes = lane < HEAD_DIM
    K_DO = channels(ctxs)
    grad_attn = dot(cot[pl.ds(0, block)], wout[...], COLS_CONTRACT)
    for w in range(width // 384):
        t0, t1, t2 = (grad_attn[:, 384 * w + 128 * t : 384 * w + 128 * (t + 1)] for t in range(3))
        turned = pltpu.roll(t1, HEAD_DIM, 1)
        do_tx[4 * w] = t0.astype(LOW)
        do_tx[4 * w + 1] = jnp.where(low_lanes, pltpu.roll(t0, HEAD_DIM, 1), turned).astype(LOW)
        do_tx[4 * w + 2] = jnp.where(low_lanes, turned, pltpu.roll(t2, HEAD_DIM, 1)).astype(LOW)
        do_tx[4 * w + 3] = t2.astype(LOW)
    for e in mates:
        send(K_DO + e, do_tx.at[mate(e)], do_rx.at[e], ctx=mate(e))
    do_rx[0] = do_tx[i]

    for e in even:
        arrived(K_N1 + e, n1.at[pl.ds(block * e, block)])
        send(K_N1 + e + 1, n1.at[pl.ds(block * e, block)], n1.at[pl.ds(block * (e + 1), block)], ctx=mate(1))
    arrived(K_N1 + 1, n1.at[pl.ds(block, block)])
    for e in even:
        arrived(K_N1 + e + 1, n1.at[pl.ds(block * (e + 1), block)])
    for d in planes:
        arrived(K_WQ + d, wq.at[pl.ds(at16(plane(d) * rows), rows)])

    @pl.loop(0, ctxs // 2)
    def _(m):
        here = pl.ds(at128(m * 2 * block), 2 * block)
        qkv[pl.ds(2 * m, 2)] = dot(n1[here], wq[...]).reshape(2, block, 384)

    for e in mates:
        arrived(K_POS + e, pos_rx.at[e])
    to_scalar = pltpu.make_async_copy(pos_rx, pos_sm, lsem.at[5])
    to_scalar.start()
    to_scalar.wait()
    rank = [lax.div(pos_sm[e, 0, 0], block) for e in range(ctxs)]
    place = []
    for g in range(ctxs):
        found = jnp.int32(0)
        for e in range(1, ctxs):
            found = found + e * (rank[e] == g).astype(jnp.int32)
        place.append(lax.rem(found, ctxs))

    leads = lax.rem(lane, HEAD_DIM) < ROTARY // 2

    def across(field):
        return jnp.where(
            leads,
            pltpu.roll(field, 128 - ROTARY // 2, 1),
            pltpu.roll(field, ROTARY // 2, 1),
        )

    def tables(g):
        off_cos, off_sin = rot_ref[pl.ds(0, block)], rot_ref[pl.ds(block, block)]
        start_cos = rot_ref[pl.ds(2 * block + g, 1)]
        start_sin = rot_ref[pl.ds(2 * block + ctxs + g, 1)]
        cosine = start_cos * off_cos - start_sin * off_sin
        sine = start_sin * off_cos + start_cos * off_sin
        return cosine, sine

    for e in mates:
        arrived(K_DO + e, do_rx.at[e])
    for g in range(ctxs):
        here = pl.ds(block * g, block)
        field = qkv[place[g]] + qkvb_ref[...]
        cosine, sine = tables(g)
        q_raw, k_raw = field[:, :128], field[:, 128:256]
        turned_q = (q_raw * cosine + across(q_raw) * sine).astype(LOW)
        q_s[here] = turned_q * jnp.asarray(HEAD_DIM**-0.5, LOW)
        k_s[here] = (k_raw * cosine + across(k_raw) * sine).astype(LOW)
        v_s[here] = field[:, 256:].astype(LOW)
        do_s[here] = do_rx[place[g]]

    for d in planes:
        arrived(K_WU + d, wup.at[rows_of(d, c)])
        send(K_WU2 + d, wup.at[rows_of(d, c)], wup.at[rows_of(d, c)], ctx=mate(1))

    o_s[...] = jnp.zeros_like(o_s)
    dq_s[...] = jnp.zeros_like(dq_s)
    dk_s[...] = jnp.zeros_like(dk_s)
    dv_s[...] = jnp.zeros_like(dv_s)

    @pl.loop(0, 2)
    def _(h):
        mine = lax.div(lane, HEAD_DIM) == h
        for g in range(ctxs):
            share = 0 if g % 4 in (0, 3) else 1

            @pl.when((h == c) | (c == share))
            def _():
                here = pl.ds(block * g, block)
                upto = pl.ds(0, block * (g + 1))
                span = block * (g + 1)
                zero = jnp.zeros((block, 128), LOW)
                q_h = jnp.where(mine, q_s[here], zero)
                do_h = jnp.where(mine, do_s[here], zero)
                scores = dot(q_h, k_s[upto], COLS_CONTRACT)
                token = lax.broadcasted_iota(jnp.int32, (block, span), 0) + block * g
                key = lax.broadcasted_iota(jnp.int32, (block, span), 1)
                masked = jnp.where(key <= token, scores, NEGATIVE)
                top = jnp.max(masked, axis=-1, keepdims=True)
                weight = jnp.exp(masked - top)
                probability = weight * (1.0 / jnp.sum(weight, axis=-1, keepdims=True))
                prob_low = probability.astype(LOW)
                attended = jnp.where(mine, dot(prob_low, v_s[upto]), 0.0)
                o_s[g] += attended
                grad_prob = dot(do_h, v_s[upto], COLS_CONTRACT)
                row_delta = jnp.sum(do_h.astype(FULL) * attended, axis=-1, keepdims=True)
                grad_score = (probability * (grad_prob - row_delta)).astype(LOW)
                dq_s[here] += jnp.where(mine, dot(grad_score, k_s[upto]), 0.0)
                dk_s[upto] += dot(grad_score, q_h, ROWS_CONTRACT)
                dv_s[upto] += dot(prob_low, do_h, ROWS_CONTRACT)

    K_O = channels(ctxs)
    for e in range(ctxs):
        o_tx[e] = o_s[rank[e]].astype(LOW)
    for e in mates:
        send(K_O + e, o_tx.at[e], o_rx.at[e], ctx=mate(e))
    o_rx[0] = o_tx[0]

    bias_sum = jnp.zeros((1, 384), FULL)
    for g in range(ctxs):
        here = pl.ds(block * g, block)
        cosine, sine = tables(g)
        dq = dq_s[here] * (HEAD_DIM**-0.5)
        dk = dk_s[here]
        parts = (dq * cosine - across(dq) * sine, dk * cosine - across(dk) * sine, dv_s[here])
        part = jnp.concatenate(parts, axis=1).astype(LOW)
        gp_s[g] = part
        bias_sum = bias_sum + jnp.sum(part.astype(FULL), axis=0, keepdims=True)
    for e in range(ctxs):
        gp_e[pl.ds(block * e, block)] = gp_s[rank[e]]

    @pl.loop(0, ctxs * block // 256)
    def _(m):
        here = pl.ds(at128(m * 256), 256)
        a1_p[here] = dot(gp_e[here], wq[...], COLS_CONTRACT).astype(LOW)

    K_A1 = channels(ctxs)
    K_A1D = channels(ctxs)
    for k in range(ctxs // 2):
        send(K_A1D + k, a1_p.at[pl.ds(block * (2 * k + 1), block)], a1_d2d.at[k], ctx=mate(1))

    @pl.loop(0, width // 256)
    def _(m):
        here = pl.ds(at128(m * 256), 256)
        gq_tx[here] = dot(n1[:, here], gp_e[...], ROWS_CONTRACT).astype(LOW)

    K_GQ = channels(shards)
    for d in planes:
        send(K_GQ + d, gq_tx.at[pl.ds(at16(plane(d) * rows), rows)], gq_rx.at[d], shard=plane(d))
    for k in range(ctxs // 2):
        arrived(K_A1D + k, a1_d2d.at[k])
        total = a1_p[pl.ds(block * 2 * k, block)].astype(FULL) + a1_d2d[k].astype(FULL)
        a1_c[k] = total.astype(LOW)
        if k:
            send(K_A1 + k, a1_c.at[k], a1_rx.at[k], ctx=mate(2 * k))

    for d in planes:
        arrived(K_WU2 + d, wup.at[rows_of(d, other)])
        arrived(K_N2 + d, n2.at[pl.ds(block * d, block)])
        arrived(K_COT + d, cot.at[pl.ds(block * d, block)])
    out_acc[...] = jnp.zeros_like(out_acc)
    a2_acc[...] = jnp.zeros_like(a2_acc)

    @pl.loop(0, width // 256)
    def _(t):
        units = pl.ds(at128(t * 256), 256)
        bias = upb_ref[:, pl.ds(at128(s * width + t * 256), 256)]
        pre = dot(n2[...], wup[:, units]) + bias
        cdf = 0.5 * (1.0 + lax.erf(pre * INV_ROOT_TWO))
        hidden = (pre * cdf).astype(LOW)
        slope = cdf + pre * (jnp.exp(-0.5 * pre * pre) * INV_ROOT_TWO_PI)
        grad_hidden = dot(cot[...], wdn[units], COLS_CONTRACT)
        grad_pre = (grad_hidden * slope).astype(LOW)
        small_a[4:5, units] = jnp.sum(grad_pre.astype(FULL), axis=0, keepdims=True)
        out_acc[...] += dot(hidden, wdn[units])
        a2_acc[...] += dot(grad_pre, wup[:, units], COLS_CONTRACT)
        gd16[units] = dot(hidden, cot[...], ROWS_CONTRACT).astype(LOW)
        gu16[:, units] = dot(n2[...], grad_pre, ROWS_CONTRACT).astype(LOW)

    K_GD = channels(1)
    K_GU = channels(shards)
    K_GUX = channels(shards)
    K_OUT = channels(shards)
    K_A2 = channels(shards)
    half_width = width // 2
    send(K_GD, gd16.at[pl.ds(at16(other * half_width), half_width)], gd_rx, ctx=mate(1))
    for d in range(shards):
        send(K_GU + d, gu16.at[rows_of(d, other)], gu_rx.at[d], ctx=mate(1))
    for d in planes:
        out_tx[d] = out_acc[pl.ds(block * d, block)].astype(LOW)
        a2_tx[d] = a2_acc[pl.ds(block * d, block)].astype(LOW)

    def up_rows(index):
        return pl.ds(at16(half_width + index * half_rows), half_rows)

    Z = ctxs // 2
    is_end = (z == 0) | (z == Z - 1)
    is_centre = (z == Z // 2 - 1) | (z == Z // 2)
    inward = jnp.where(z < Z // 2, 2, -2)
    to_inner = jnp.where(is_centre, 1, 0)
    line_rows = half_width + rows * shards // 2 + half_rows
    chunk = half_rows
    chunks = line_rows // chunk
    K_LINE = channels(2 * chunks)
    K_FAR = channels(chunks)
    K_FIN = channels(chunks)

    def span_of(q):
        return pl.ds(q * chunk, chunk)

    def near_copy(q, src):
        return pltpu.make_async_remote_copy(
            src_ref=src.at[span_of(q)],
            dst_ref=line_rx.at[to_inner, span_of(q)],
            send_sem=ssem.at[K_LINE + q],
            recv_sem=rsem.at[K_LINE + chunks * to_inner + q],
            device_id={"ctx": i + inward},
            device_id_type=MESH,
        )

    def far_copy(q):
        return pltpu.make_async_remote_copy(
            src_ref=line_far.at[span_of(q)],
            dst_ref=line_rx.at[1, span_of(q)],
            send_sem=ssem.at[K_FAR + q],
            recv_sem=rsem.at[K_LINE + chunks + q],
            device_id={"ctx": i - inward},
            device_id_type=MESH,
        )

    def near(q):
        @pl.when(is_end)
        def _():
            line_rx[0, span_of(q)] = jnp.zeros((chunk, width), LOW)
            near_copy(q, line_own).start()

        @pl.when(jnp.logical_not(is_end))
        def _():
            arrived(K_LINE + q, line_rx.at[0, span_of(q)])
            line_near[span_of(q)] = (
                line_rx[0, span_of(q)].astype(FULL) + line_own[span_of(q)].astype(FULL)
            ).astype(LOW)
            near_copy(q, line_near).start()

    def far(q):
        arrived(K_LINE + chunks + q, line_rx.at[1, span_of(q)])
        beyond = line_rx[1, span_of(q)].astype(FULL) + line_own[span_of(q)].astype(FULL)

        @pl.when(jnp.logical_not(is_end))
        def _():
            line_far[span_of(q)] = beyond.astype(LOW)
            far_copy(q).start()

        fin_ref[c, span_of(q)] = (beyond + line_rx[0, span_of(q)].astype(FULL)).astype(LOW)
        send(K_FIN + q, fin_ref.at[c, span_of(q)], fin_ref.at[c, span_of(q)], ctx=mate(1))

    for d in range(shards):
        arrived(K_GU + d, gu_rx.at[d])
        total = (gu16[rows_of(d, c)].astype(FULL) + gu_rx[d].astype(FULL)).astype(LOW)
        if d:
            gu_tx[d] = total
            send(K_GUX + d, gu_tx.at[d], line_own.at[up_rows(s)], shard=plane(d))
        else:
            line_own[up_rows(s)] = total
    for d in planes:
        send(K_OUT + d, out_tx.at[d], out_rx.at[d], shard=plane(d))
        send(K_A2 + d, a2_tx.at[d], a2_rx.at[d], shard=plane(d))
    arrived(K_GD, gd_rx)
    line_own[pl.ds(0, half_width)] = (
        gd16[pl.ds(at16(c * half_width), half_width)].astype(FULL) + gd_rx[...].astype(FULL)
    ).astype(LOW)
    for q in range(4):
        near(q)

    for e in mates:
        arrived(K_O + e, o_rx.at[e])
    for w in range(width // 384):
        p0, p1, p2, p3 = (o_rx[flip(i, 4 * w + t)].astype(FULL) for t in range(4))
        r1, r2 = pltpu.roll(p1, HEAD_DIM, 1), pltpu.roll(p2, HEAD_DIM, 1)
        base = 384 * w
        attn_low[:, base : base + 128] = (p0 + jnp.where(low_lanes, 0.0, r1)).astype(LOW)
        attn_low[:, base + 128 : base + 256] = jnp.where(low_lanes, r1, r2).astype(LOW)
        attn_low[:, base + 256 : base + 384] = (p3 + jnp.where(low_lanes, r2, 0.0)).astype(LOW)

    @pl.loop(0, width // 256)
    def _(m):
        here = pl.ds(at128(m * 256), 256)
        go16[here] = dot(attn_low[:, here], cot[pl.ds(0, block)], ROWS_CONTRACT).astype(LOW)

    K_GO = channels(shards)
    K_GOX = channels(shards)
    for d in range(shards):
        send(K_GO + d, go16.at[rows_of(d, other)], go_rx.at[d], ctx=mate(1))
    attn_branch = dot(attn_low[...], wout[...])

    K_GQA = channels(ctxs)
    own_gq = gq_tx[my_rows].astype(FULL)
    for d in planes:
        arrived(K_GQ + d, gq_rx.at[d])
        own_gq = own_gq + gq_rx[d].astype(FULL)
    qkvfin_ref[i] = own_gq.astype(LOW)
    for e in (1, *even):
        send(K_GQA + e, qkvfin_ref.at[i], qkvfin_ref.at[i], ctx=mate(e))
    for d in range(shards):
        arrived(K_GO + d, go_rx.at[d])
        total = (go16[rows_of(d, c)].astype(FULL) + go_rx[d].astype(FULL)).astype(LOW)
        go_tx[d] = total
        if d:
            send(K_GOX + d, go_tx.at[d], go_x.at[d], shard=plane(d))
    for d in planes:
        arrived(K_GUX + d, line_own.at[up_rows(plane(d))])
    for q in range(4, 8):
        near(q)
        far(q - 4)

    total = x_ref[...].astype(FULL) + attn_branch + out_acc[pl.ds(0, block)]
    for d in planes:
        arrived(K_OUT + d, out_rx.at[d])
        total = total + out_rx[d].astype(FULL)
    y_ref[...] = total.astype(LOW)

    own_go = go_tx[0].astype(FULL)
    for d in planes:
        arrived(K_GOX + d, go_x.at[d])
        own_go = own_go + go_x[d].astype(FULL)
    line_own[pl.ds(line_rows - half_rows, half_rows)] = own_go.astype(LOW)
    near(8)
    for q in range(4, 8):
        far(q)

    a2 = a2_acc[pl.ds(0, block)]
    for d in planes:
        arrived(K_A2 + d, a2_rx.at[d])
        a2 = a2 + a2_rx[d].astype(FULL)
    a1 = a1_c[0].astype(FULL)
    for k in range(1, ctxs // 2):
        arrived(K_A1 + k, a1_rx.at[k])
        a1 = a1 + a1_rx[k].astype(FULL)
    small_a[0:1] = jnp.sum(a1 * normal, axis=0, keepdims=True)
    small_a[1:2] = jnp.sum(a1, axis=0, keepdims=True)
    small_a[2:3] = jnp.sum(a2 * normal, axis=0, keepdims=True)
    small_a[3:4] = jnp.sum(a2, axis=0, keepdims=True)
    small_a[5:6, 0:384] = bias_sum
    small_a[5:6, 384:768] = jnp.zeros((1, 384), FULL)
    small_a[6:8] = jnp.zeros((2, width), FULL)
    K_SM = channels(ctxs)
    K_SMX = channels(shards)
    for e in mates:
        send(K_SM + e, small_a, small_rx.at[e], ctx=mate(e))
    mixed = a1 * gain1_ref[...] + a2 * gain2_ref[...]
    back = r * (
        mixed
        - jnp.mean(mixed, axis=-1, keepdims=True)
        - normal * jnp.mean(mixed * normal, axis=-1, keepdims=True)
    )
    dx_ref[...] = (cot[pl.ds(0, block)].astype(FULL) + back).astype(LOW)

    for e in even:
        arrived(K_GQA + e, qkvfin_ref.at[mate(e)])
        send(K_GQA + e + 1, qkvfin_ref.at[mate(e)], qkvfin_ref.at[mate(e)], ctx=mate(1))

    small_rx[0] = small_a[...]
    for e in mates:
        arrived(K_SM + e, small_rx.at[e])
    summed = small_rx[0]
    for e in mates:
        summed = summed + small_rx[e]
    small_b[0, 0:8] = summed
    for j in range(ctxs):
        small_b[0, 8 + j : 9 + j] = small_rx[flip(i, j), 5:6]
    for d in planes:
        send(K_SMX + d, small_b.at[0], small_b.at[d], shard=plane(d))
    far(8)
    for d in planes:
        arrived(K_SMX + d, small_b.at[d])
    whole = small_b[0]
    for d in planes:
        whole = whole + small_b[d]
    small_ref[0:16] = whole
    for j in range(shards):
        small_ref[16 + j : 17 + j] = small_b[flip(s, j), 4:5]
    small_ref[20:24] = jnp.zeros((4, width), FULL)

    arrived(K_GQA + 1, qkvfin_ref.at[mate(1)])
    for e in even:
        arrived(K_GQA + e + 1, qkvfin_ref.at[mate(e + 1)])
    for q in range(chunks):
        arrived(K_FIN + q, fin_ref.at[other, span_of(q)])
    for copy in sent:
        copy.wait_send()
    for q in range(chunks):
        near_copy(q, line_own).wait_send()

        @pl.when(jnp.logical_not(is_end))
        def _():
            far_copy(q).wait_send()


def ring_on_device(
    layer_input,
    positions,
    cotangent,
    ln1_gain,
    ln1_bias,
    ln2_gain,
    ln2_bias,
    w_qkv,
    qkv_bias,
    w_out,
    w_up,
    up_bias,
    w_down,
):
    seqs_here, block_len, feature_count = layer_input.shape
    row_count = seqs_here * block_len
    head_count = HEADS
    head_size = HEAD_DIM
    score_scale = head_size ** (-0.5)
    whole_qkv, whole_out, whole_up, whole_down = (
        lax.all_gather(w_qkv, "shard", axis=0, tiled=True),
        lax.all_gather(w_out, "shard", axis=0, tiled=True),
        lax.all_gather(w_up, "shard", axis=0, tiled=True),
        lax.all_gather(w_down, "shard", axis=0, tiled=True),
    )
    all_positions = lax.all_gather(positions, "ctx", axis=1, tiled=True)
    cycle_size = lax.axis_size("ctx")
    my_index = lax.axis_index("ctx")
    inputs = layer_input.astype(jnp.float32).reshape(row_count, feature_count)
    normed_one = layer_norm(inputs, ln1_gain, ln1_bias).astype(jnp.bfloat16)
    normed_two = layer_norm(inputs, ln2_gain, ln2_bias).astype(jnp.bfloat16)
    projected = jnp.dot(normed_one, whole_qkv, preferred_element_type=jnp.float32) + qkv_bias
    split_heads = projected.reshape(seqs_here, block_len, 3, head_count, head_size)
    cosine, sine_table = rotary_tables(positions)
    queries = rotate(split_heads[:, :, 0], cosine, sine_table).astype(jnp.bfloat16)
    key_rows = rotate(split_heads[:, :, 1], cosine, sine_table).astype(jnp.bfloat16)
    value_rows = split_heads[:, :, 2].astype(jnp.bfloat16)
    top_query = jnp.max(positions)

    def attend_block(running, key_blk, value_blk, key_pos):

        def attend_update(current):
            run_max, run_sum, run_acc = current
            scores = (
                jnp.einsum("sqhd,skhd->shqk", queries, key_blk, preferred_element_type=jnp.float32)
                * score_scale
            )
            allowed = key_pos[:, None, None, :] <= positions[:, None, :, None]
            masked = jnp.where(allowed, scores, NEGATIVE)
            new_max = jnp.maximum(run_max, jnp.max(masked, axis=-1))
            shrink = jnp.exp(run_max - new_max)
            weights_now = jnp.where(allowed, jnp.exp(masked - new_max[..., None]), 0.0)
            run_sum = run_sum * shrink + jnp.sum(weights_now, axis=-1)
            added_term = jnp.einsum(
                "shqk,skhd->sqhd",
                weights_now.astype(jnp.bfloat16),
                value_blk,
                preferred_element_type=jnp.float32,
            )
            run_acc = run_acc * jnp.transpose(shrink, (0, 2, 1))[..., None] + added_term
            return (new_max, run_sum, run_acc)

        return lax.cond(
            jnp.min(key_pos) <= top_query, attend_update, lambda unchanged: unchanged, running
        )

    initial = (
        jnp.full((seqs_here, head_count, block_len), NEGATIVE, jnp.float32),
        jnp.zeros((seqs_here, head_count, block_len), jnp.float32),
        jnp.zeros((seqs_here, block_len, head_count, head_size), jnp.float32),
    )
    own_block = attend_block(initial, key_rows, value_rows, positions)

    def cycle_forward(turn_index, carried):
        current, key_cur, value_cur = carried
        key_cur, value_cur = shifted((key_cur, value_cur), "ctx", 1)
        source = (my_index - turn_index) % cycle_size
        key_pos = lax.dynamic_slice_in_dim(all_positions, source * block_len, block_len, 1)
        return (attend_block(current, key_cur, value_cur, key_pos), key_cur, value_cur)

    (run_max, run_sum, run_acc), unused_key, unused_value = lax.fori_loop(
        1, cycle_size, cycle_forward, (own_block, key_rows, value_rows)
    )
    attn_vals = run_acc / jnp.transpose(run_sum, (0, 2, 1))[..., None]
    log_total = run_max + jnp.log(run_sum)
    attn_low = attn_vals.astype(jnp.bfloat16).reshape(row_count, feature_count)
    attn_branch = jnp.dot(attn_low, whole_out, preferred_element_type=jnp.float32)
    hidden_pre = jnp.dot(normed_two, whole_up, preferred_element_type=jnp.float32) + up_bias
    hidden_low = gelu_exact(hidden_pre).astype(jnp.bfloat16)
    mlp_branch = jnp.dot(hidden_low, whole_down, preferred_element_type=jnp.float32)
    layer_output = (
        (inputs + attn_branch + mlp_branch)
        .astype(jnp.bfloat16)
        .reshape(seqs_here, block_len, feature_count)
    )
    cot_low = cotangent.reshape(row_count, feature_count)
    cot_full = cot_low.astype(jnp.float32)
    grad_down = jnp.einsum("rf,rd->fd", hidden_low, cot_low, preferred_element_type=jnp.float32)
    grad_hidden = jnp.einsum("rd,fd->rf", cot_low, whole_down, preferred_element_type=jnp.float32)
    unused_gelu, gelu_back = jax.vjp(gelu_exact, hidden_pre)
    grad_pre = gelu_back(grad_hidden)[0].astype(jnp.bfloat16)
    grad_up_bias = jnp.sum(grad_pre.astype(jnp.float32), axis=0)
    grad_up = jnp.einsum("rd,rf->df", normed_two, grad_pre, preferred_element_type=jnp.float32)
    grad_two = jnp.einsum("rf,df->rd", grad_pre, whole_up, preferred_element_type=jnp.float32)
    grad_out = jnp.einsum("rd,re->de", attn_low, cot_low, preferred_element_type=jnp.float32)
    grad_attn = (
        jnp.einsum("re,de->rd", cot_low, whole_out, preferred_element_type=jnp.float32)
        .astype(jnp.bfloat16)
        .reshape(seqs_here, block_len, head_count, head_size)
    )
    row_delta = jnp.transpose(
        jnp.sum(grad_attn.astype(jnp.float32) * attn_vals, axis=-1), (0, 2, 1)
    )

    def back_block(grads_in, key_blk, value_blk, key_pos):

        def back_update(current):
            grad_query, grad_key, grad_value = current
            scores = (
                jnp.einsum("sqhd,skhd->shqk", queries, key_blk, preferred_element_type=jnp.float32)
                * score_scale
            )
            allowed = key_pos[:, None, None, :] <= positions[:, None, :, None]
            masked = jnp.where(allowed, scores, NEGATIVE)
            probability = jnp.exp(masked - log_total[..., None])
            prob_low = probability.astype(jnp.bfloat16)
            grad_value = grad_value + jnp.einsum(
                "shqk,sqhd->skhd", prob_low, grad_attn, preferred_element_type=jnp.float32
            )
            grad_prob = jnp.einsum(
                "sqhd,skhd->shqk", grad_attn, value_blk, preferred_element_type=jnp.float32
            )
            grad_score = (probability * (grad_prob - row_delta[..., None])).astype(jnp.bfloat16)
            grad_query = (
                grad_query
                + jnp.einsum(
                    "shqk,skhd->sqhd", grad_score, key_blk, preferred_element_type=jnp.float32
                )
                * score_scale
            )
            grad_key = (
                grad_key
                + jnp.einsum(
                    "shqk,sqhd->skhd", grad_score, queries, preferred_element_type=jnp.float32
                )
                * score_scale
            )
            return (grad_query, grad_key, grad_value)

        return lax.cond(
            jnp.min(key_pos) <= top_query, back_update, lambda unchanged: unchanged, grads_in
        )

    zero_rows = jnp.zeros((seqs_here, block_len, head_count, head_size), jnp.float32)

    def pass_back(grad_key, grad_value):
        return (
            shifted(grad_key.astype(jnp.bfloat16), "ctx", 1).astype(grad_key.dtype),
            shifted(grad_value.astype(jnp.bfloat16), "ctx", 1).astype(grad_value.dtype),
        )

    grad_query, grad_key, grad_value = back_block(
        (zero_rows, zero_rows, zero_rows), key_rows, value_rows, positions
    )
    grad_key, grad_value = pass_back(grad_key, grad_value)

    def cycle_backward(turn_index, carried):
        grad_query, key_cur, value_cur, grad_key, grad_value = carried
        key_cur, value_cur = shifted((key_cur, value_cur), "ctx", 1)
        source = (my_index - turn_index) % cycle_size
        key_pos = lax.dynamic_slice_in_dim(all_positions, source * block_len, block_len, 1)
        grad_query, grad_key, grad_value = back_block(
            (grad_query, grad_key, grad_value), key_cur, value_cur, key_pos
        )
        grad_key, grad_value = pass_back(grad_key, grad_value)
        return (grad_query, key_cur, value_cur, grad_key, grad_value)

    grad_query, unused_key, unused_value, grad_key, grad_value = lax.fori_loop(
        1, cycle_size, cycle_backward, (grad_query, key_rows, value_rows, grad_key, grad_value)
    )
    unused_rot, rotate_back = jax.vjp(
        lambda field_in: rotate(field_in, cosine, sine_table), zero_rows
    )
    query_pre = rotate_back(grad_query)[0]
    key_pre = rotate_back(grad_key)[0]
    grad_proj = (
        jnp.stack([query_pre, key_pre, grad_value], axis=2)
        .reshape(row_count, 3 * feature_count)
        .astype(jnp.bfloat16)
    )
    grad_qkv_bias = jnp.sum(grad_proj.astype(jnp.float32), axis=0)
    grad_qkv = jnp.einsum("rd,re->de", normed_one, grad_proj, preferred_element_type=jnp.float32)
    grad_one = jnp.einsum("re,de->rd", grad_proj, whole_qkv, preferred_element_type=jnp.float32)
    unused_one, norm_back_one = jax.vjp(layer_norm, inputs, ln1_gain, ln1_bias)
    input_one, grad_gain_one, grad_bias_one = norm_back_one(grad_one)
    unused_two, norm_back_two = jax.vjp(layer_norm, inputs, ln2_gain, ln2_bias)
    input_two, grad_gain_two, grad_bias_two = norm_back_two(grad_two)
    grad_input = (
        (cot_full + input_one + input_two)
        .astype(jnp.bfloat16)
        .reshape(seqs_here, block_len, feature_count)
    )
    summed = (
        lax.psum(grad_qkv.astype(jnp.bfloat16), "ctx").astype(jnp.float32),
        lax.psum(grad_out.astype(jnp.bfloat16), "ctx").astype(jnp.float32),
        lax.psum(grad_up.astype(jnp.bfloat16), "ctx").astype(jnp.float32),
        lax.psum(grad_down.astype(jnp.bfloat16), "ctx").astype(jnp.float32),
        lax.psum(grad_gain_one.astype(jnp.bfloat16), "ctx").astype(jnp.float32),
        lax.psum(grad_bias_one.astype(jnp.bfloat16), "ctx").astype(jnp.float32),
        lax.psum(grad_gain_two.astype(jnp.bfloat16), "ctx").astype(jnp.float32),
        lax.psum(grad_bias_two.astype(jnp.bfloat16), "ctx").astype(jnp.float32),
        lax.psum(grad_qkv_bias.astype(jnp.bfloat16), "ctx").astype(jnp.float32),
        lax.psum(grad_up_bias.astype(jnp.bfloat16), "ctx").astype(jnp.float32),
    )
    sum_qkv, sum_out, sum_up, sum_down = (
        lax.psum_scatter(
            summed[0].astype(jnp.bfloat16), "shard", scatter_dimension=0, tiled=True
        ).astype(jnp.float32),
        lax.psum_scatter(
            summed[1].astype(jnp.bfloat16), "shard", scatter_dimension=0, tiled=True
        ).astype(jnp.float32),
        lax.psum_scatter(
            summed[2].astype(jnp.bfloat16), "shard", scatter_dimension=0, tiled=True
        ).astype(jnp.float32),
        lax.psum_scatter(
            summed[3].astype(jnp.bfloat16), "shard", scatter_dimension=0, tiled=True
        ).astype(jnp.float32),
    )
    sum_small = (
        lax.psum(summed[4].astype(jnp.bfloat16), "shard").astype(jnp.float32),
        lax.psum(summed[5].astype(jnp.bfloat16), "shard").astype(jnp.float32),
        lax.psum(summed[6].astype(jnp.bfloat16), "shard").astype(jnp.float32),
        lax.psum(summed[7].astype(jnp.bfloat16), "shard").astype(jnp.float32),
        lax.psum(summed[8].astype(jnp.bfloat16), "shard").astype(jnp.float32),
        lax.psum(summed[9].astype(jnp.bfloat16), "shard").astype(jnp.float32),
    )
    return (
        layer_output,
        grad_input,
        sum_small[0],
        sum_small[1],
        sum_small[2],
        sum_small[3],
        sum_qkv,
        sum_small[4],
        sum_out,
        sum_up,
        sum_small[5],
        sum_down,
    )


def fused_on_device(
    layer_input,
    positions,
    cotangent,
    ln1_gain,
    ln1_bias,
    ln2_gain,
    ln2_bias,
    w_qkv,
    qkv_bias,
    w_out,
    w_up,
    up_bias,
    w_down,
):
    shards, ctxs = lax.axis_size("shard"), lax.axis_size("ctx")
    block, width = layer_input.shape[1:]
    rows = w_qkv.shape[0]
    i = lax.axis_index("ctx")
    first = HEAD_DIM * (3 * (i // 2) + i % 2)
    wsel = lax.dynamic_slice(
        w_qkv.reshape(rows, 3, width), (0, 0, first), (rows, 3, 2 * HEAD_DIM)
    ).reshape(rows, 6 * HEAD_DIM)
    bsel = lax.dynamic_slice(
        qkv_bias.reshape(3, width), (0, first), (3, 2 * HEAD_DIM)
    ).reshape(1, 6 * HEAD_DIM)
    line_rows = width // 2 + rows * shards // 2 + rows // 2
    vmem = pl.BlockSpec(memory_space=pltpu.VMEM)
    hbm = pl.BlockSpec(memory_space=pl.ANY)
    low, full = (lambda *shape: pltpu.VMEM(shape, LOW)), (lambda *shape: pltpu.VMEM(shape, FULL))
    half = rows // 2
    scratch = [
        low(width, 384),
        low(width, width),
        low(width, width),
        low(width, width),
        low(ctxs * block, width),
        low(shards * block, width),
        low(shards * block, width),
        pltpu.VMEM((8, block), jnp.int32),
        pltpu.VMEM((ctxs, 8, block), jnp.int32),
        pltpu.SMEM((ctxs, 8, block), jnp.int32),
        full(ctxs, block, 384),
        low(ctxs * block, 128),
        low(ctxs * block, 128),
        low(ctxs * block, 128),
        low(ctxs, block, 128),
        low(ctxs, block, 128),
        low(ctxs * block, 128),
        full(ctxs, block, 128),
        full(ctxs * block, 128),
        full(ctxs * block, 128),
        full(ctxs * block, 128),
        low(ctxs, block, 384),
        low(ctxs * block, 384),
        low(ctxs, block, 128),
        low(ctxs, block, 128),
        low(block, width),
        low(ctxs * block, width),
        low(ctxs // 2, block, width),
        low(ctxs // 2, block, width),
        low(ctxs // 2, block, width),
        low(width, 384),
        low(shards, rows, 384),
        low(rows, 384),
        full(shards * block, width),
        full(shards * block, width),
        low(shards, block, width),
        low(shards, block, width),
        low(shards, block, width),
        low(shards, block, width),
        low(width, width),
        low(width // 2, width),
        low(width, width),
        low(shards, half, width),
        low(shards, half, width),
        low(width, width),
        low(shards, half, width),
        low(shards, half, width),
        low(shards, half, width),
        low(line_rows, width),
        low(2, line_rows, width),
        low(line_rows, width),
        low(line_rows, width),
        full(8, width),
        full(ctxs, 8, width),
        full(shards, 16, width),
        full(shards, 16, width),
        pltpu.SemaphoreType.DMA((256,)),
        pltpu.SemaphoreType.DMA((256,)),
        pltpu.SemaphoreType.DMA((8,)),
    ]
    row = lambda vector: vector.reshape(1, -1)
    y, dx, fin, qkvfin, small = pl.pallas_call(
        fused_body,
        out_shape=(
            jax.ShapeDtypeStruct((block, width), LOW),
            jax.ShapeDtypeStruct((block, width), LOW),
            jax.ShapeDtypeStruct((2, line_rows, width), LOW),
            jax.ShapeDtypeStruct((ctxs, rows, 384), LOW),
            jax.ShapeDtypeStruct((24, width), FULL),
        ),
        in_specs=[vmem] * 9 + [hbm] * 5,
        out_specs=(vmem,) * 5,
        scratch_shapes=scratch,
        compiler_params=pltpu.CompilerParams(
            collective_id=0, has_side_effects=True, vmem_limit_bytes=60 * 1024 * 1024
        ),
        name="layer",
    )(
        layer_input[0],
        positions,
        row(ln1_gain),
        row(ln1_bias),
        row(ln2_gain),
        row(ln2_bias),
        bsel,
        row(up_bias),
        jnp.asarray(rotary_constants(ctxs, block)),
        cotangent[0],
        wsel,
        w_up,
        w_out,
        w_down,
    )
    fin = fin.astype(FULL)
    cut = width // 2
    grad_down = fin[:, :cut].reshape(width, width)
    grad_up = (
        fin[:, cut : cut + shards * half]
        .reshape(2, shards, half, width)
        .transpose(0, 2, 1, 3)
        .reshape(rows, shards * width)
    )
    grad_out = fin[:, cut + shards * half :].reshape(rows, width)

    def heads_of(slabs, count):
        slabs = slabs.astype(FULL).reshape(ctxs // 2, 2, count, 3, 2, HEAD_DIM)
        one = slabs[:, 0, :, :, 0]
        two = slabs[:, 0, :, :, 1] + slabs[:, 1, :, :, 0]
        three = slabs[:, 1, :, :, 1]
        return (
            jnp.stack([one, two, three], axis=3).transpose(1, 2, 0, 3, 4).reshape(count, 3 * width)
        )

    return (
        y[None],
        dx[None],
        small[0],
        small[1],
        small[2],
        small[3],
        heads_of(qkvfin, rows),
        heads_of(small[8 : 8 + ctxs, :384], 1).reshape(-1),
        grad_out,
        grad_up,
        small[16 : 16 + shards].reshape(-1),
        grad_down,
    )


def on_device(layer_input, positions, cotangent, *params):
    shards, ctxs = lax.axis_size("shard"), lax.axis_size("ctx")
    seqs, block, width = layer_input.shape
    rows, ff = params[4].shape[0], params[7].shape[1]
    fits = (
        seqs == 1
        and block == 128
        and (shards, ctxs) == (4, 8)
        and 3 * ctxs == 2 * HEADS
        and HEAD_DIM == 64
        and rows * shards == width == HEADS * HEAD_DIM
        and ff == shards * width
    )
    path = fused_on_device if fits else ring_on_device
    return path(layer_input, positions, cotangent, *params)


def solution(mesh):
    placed = (
        P("shard", "ctx", None),
        P("shard", "ctx"),
        P("shard", "ctx", None),
        P(),
        P(),
        P(),
        P(),
        P("shard", None),
        P(),
        P("shard", None),
        P("shard", None),
        P(),
        P("shard", None),
    )
    return jax.shard_map(
        on_device,
        mesh=mesh,
        in_specs=placed,
        out_specs=(
            P("shard", "ctx", None),
            P("shard", "ctx", None),
            P(),
            P(),
            P(),
            P(),
            P("shard", None),
            P(),
            P("shard", None),
            P("shard", None),
            P(),
            P("shard", None),
        ),
        check_vma=False,
    )
```

```python
import functools

import jax
import jax.numpy as jnp
import numpy as np
from jax import lax
from jax.experimental import pallas as pl
from jax.experimental.pallas import tpu as pltpu
from jax.sharding import PartitionSpec as P

HEADS = 12
HEAD_DIM = 64
ROTARY = 16


EPSILON = 1e-05
NEGATIVE = -1e30


def shifted(shard, axis, by):
    count = lax.axis_size(axis)
    return lax.ppermute(shard, axis, [(i, (i + by) % count) for i in range(count)])


def layer_norm(values_in, gain_vec, bias_vec):
    centered = values_in - jnp.mean(values_in, axis=-1, keepdims=True)
    variance = jnp.mean(centered * centered, axis=-1, keepdims=True)
    return centered * lax.rsqrt(variance + EPSILON) * gain_vec + bias_vec


def rotary_tables(position_ids):
    half_dim = ROTARY // 2
    inverse_freq = 1.0 / 10000.0 ** (jnp.arange(half_dim, dtype=jnp.float32) * (2.0 / ROTARY))
    angles = position_ids.astype(jnp.float32)[..., None] * inverse_freq
    return (jnp.cos(angles), jnp.sin(angles))


def rotate(field_in, cosine, sine_table):
    half_dim = cosine.shape[-1]
    lead_part = field_in[..., :half_dim]
    second = field_in[..., half_dim : 2 * half_dim]
    remain = field_in[..., 2 * half_dim :]
    cos_wide = cosine[..., None, :]
    sin_wide = sine_table[..., None, :]
    return jnp.concatenate(
        [
            lead_part * cos_wide - second * sin_wide,
            second * cos_wide + lead_part * sin_wide,
            remain,
        ],
        axis=-1,
    )


def gelu_exact(field_in):
    return jax.nn.gelu(field_in, approximate=False)


MESH = pl.DeviceIdType.MESH
LOW = jnp.bfloat16
FULL = jnp.float32
ROWS_CONTRACT = (((0,), (0,)), ((), ()))
COLS_CONTRACT = (((1,), (1,)), ((), ()))
INV_ROOT_TWO = 0.7071067811865476
INV_ROOT_TWO_PI = 0.3989422804014327
CHUNK = 48
LAG = 2


def dot(lhs, rhs, dims=(((1,), (0,)), ((), ()))):
    return lax.dot_general(lhs, rhs, dims, preferred_element_type=FULL)


def flip(index, bits):
    for power in (1, 2, 4, 8):
        if bits & power:
            index = index + power - 2 * power * lax.rem(lax.div(index, power), 2)
    return index


def at16(value):
    return pl.multiple_of(value, 16)


def at128(value):
    return pl.multiple_of(value, 128)


def rotary_constants(blocks, block_len):
    lane = np.arange(128) % HEAD_DIM
    half = ROTARY // 2
    turning = lane < ROTARY
    freq = np.where(turning, 10000.0 ** (-(lane % half) * (2.0 / ROTARY)), 0.0)
    sign = np.where(lane < half, -1.0, 1.0) * turning
    offset = np.arange(block_len)[:, None] * freq
    start = (np.arange(blocks) * block_len)[:, None] * freq
    parts = (np.cos(offset), np.sin(offset) * sign, np.cos(start), np.sin(start) * sign)
    return np.concatenate(parts).astype(np.float32)


def fused_body(names, *refs):
    (
        x_ref, pos_ref, gain1_ref, bias1_ref, gain2_ref, bias2_ref, qkvb_ref, upb_ref, rot_ref,
        cot_hbm, wqkv_hbm, wup_hbm, wout_hbm, wdn_hbm,
        y_ref, dx_ref, fin_ref, qkvfin_ref, early_ref, late_ref,
    ) = refs[:20]
    scratch = dict(zip(names, refs[20:]))
    run_layer(
        x_ref, pos_ref, gain1_ref, bias1_ref, gain2_ref, bias2_ref, qkvb_ref, upb_ref, rot_ref,
        cot_hbm, wqkv_hbm, wup_hbm, wout_hbm, wdn_hbm,
        y_ref, dx_ref, fin_ref, qkvfin_ref, early_ref, late_ref, **scratch,
    )


def run_layer(
    x_ref, pos_ref, gain1_ref, bias1_ref, gain2_ref, bias2_ref, qkvb_ref, upb_ref, rot_ref,
    cot_hbm, wqkv_hbm, wup_hbm, wout_hbm, wdn_hbm,
    y_ref, dx_ref, fin_ref, qkvfin_ref, early_ref, late_ref,
    *,
    wq, wraw, wup, wout, wdn, n1, n2, cot, pos_tx, pos_rx, pos_sm, qkv, q_s, k_s, v_s, do_tx, do_mid, do_rx, do_s,
    o_s, dq_s, dk_s, dv_s, gp_s, gp_e, o_tx, o_rx, attn, a1_p, a1_d2d, a1_own, a1_tx_r, a1_tx_l, a1_rx_r, a1_rx_l,
    gq_tx, gq_rx, out_acc, a2_acc, out_tx, out_rx, a2_tx, a2_rx, gd16, gd_rx, gu16, gu_rx, gu_tx,
    go16, go_rx, line_own, line_rx, line_near, line_far, early_a, early_rx, early_b,
    late_a, late_rx, late_b, ssem, rsem, lsem,
):
    shards = lax.axis_size("shard")
    ctxs = lax.axis_size("ctx")
    s = lax.axis_index("shard")
    i = lax.axis_index("ctx")
    c = lax.rem(i, 2)
    z = lax.div(i, 2)
    other = 1 - c
    Z = ctxs // 2
    planes = range(1, shards)
    mates = range(1, ctxs)
    block = x_ref.shape[0]
    width = x_ref.shape[1]
    rows = width // shards
    half_rows = rows // 2
    half_width = width // 2
    sent = []
    used = [0]
    always = None

    def channels(count):
        first = used[0]
        used[0] += count
        return first

    def copy_of(send_k, recv_k, src, dst, device):
        return pltpu.make_async_remote_copy(
            src_ref=src,
            dst_ref=dst,
            send_sem=ssem.at[send_k],
            recv_sem=rsem.at[recv_k],
            device_id=device,
            device_id_type=MESH,
        )

    def send(k, src, dst, device, recv_k=None, when=always):
        copy = copy_of(k, k if recv_k is None else recv_k, src, dst, device)
        sent.append((copy, when))
        if when is always:
            copy.start()
        else:
            pl.when(when)(copy.start)

    def arrived(k, dst):
        copy_of(k, k, dst, dst, {"ctx": flip(i, 1)}).wait_recv()

    def plane(d):
        return flip(s, d)

    def mate(e):
        return flip(i, e)

    partner = {"ctx": flip(i, 1)}
    right = {"ctx": i + 2}
    left = {"ctx": i - 2}
    has_left = z > 0
    has_right = z < Z - 1

    loads = []

    def load(src, dst):
        copy = pltpu.make_async_copy(src, dst, lsem.at[len(loads)])
        copy.start()
        loads.append(copy)

    my_rows = pl.ds(at16(s * rows), rows)
    first = HEAD_DIM * (3 * z + c)
    base = jnp.minimum(128 * lax.div(first, 128), width - 256)
    for part in range(3):
        load(wqkv_hbm.at[:, pl.ds(at128(width * part + base), 256)], wraw.at[part])
    load(cot_hbm, cot.at[pl.ds(0, block)])
    load(wout_hbm.at[pl.ds(0, 128)], wout.at[pl.ds(0, 128)])
    load(wout_hbm.at[pl.ds(HEAD_DIM, 128)], wout.at[pl.ds(128, 128)])
    load(wup_hbm.at[:, pl.ds(at128(s * width), width)], wup.at[my_rows])
    load(wdn_hbm, wdn)

    barrier = pltpu.get_barrier_semaphore()
    for d in range(shards):
        for e in range(ctxs):
            if d or e:
                pl.semaphore_signal(
                    barrier,
                    inc=1,
                    device_id={"shard": plane(d), "ctx": mate(e)},
                    device_id_type=MESH,
                )
    pl.semaphore_wait(barrier, shards * ctxs - 1)

    K_COT = channels(shards)
    K_WQ = channels(shards)
    K_WU = channels(shards)
    K_WU2 = channels(shards)
    K_N2 = channels(shards)
    K_POS = channels(ctxs)
    for d in planes:
        send(K_COT + d, cot_hbm, cot.at[pl.ds(block * d, block)], {"shard": plane(d)})

    def two_heads(here, there):
        wide = lax.broadcasted_iota(jnp.int32, here.shape, 1)
        turned = jnp.where(
            wide < HEAD_DIM, pltpu.roll(here, HEAD_DIM, 1), pltpu.roll(there, HEAD_DIM, 1)
        )
        return jnp.where(
            first == base, here, jnp.where(first == base + HEAD_DIM, turned, there)
        )

    for copy in loads[:3]:
        copy.wait()
    for part in range(3):
        raw = wraw[part].astype(FULL)
        wq[my_rows, 128 * part : 128 * (part + 1)] = two_heads(raw[:, :128], raw[:, 128:]).astype(LOW)
    qkv_bias = jnp.concatenate(
        [
            two_heads(
                jnp.broadcast_to(qkvb_ref[pl.ds(at128(width * part + base), 128)][None, :], (8, 128)),
                jnp.broadcast_to(qkvb_ref[pl.ds(at128(width * part + base + 128), 128)][None, :], (8, 128)),
            )
            for part in range(3)
        ],
        axis=1,
    )[:1]
    gain1, gain2 = gain1_ref[...][None, :], gain2_ref[...][None, :]
    bias1, bias2 = bias1_ref[...][None, :], bias2_ref[...][None, :]
    pos_tx[...] = jnp.broadcast_to(pos_ref[...], pos_tx.shape)
    x = x_ref[...].astype(FULL)
    mean = jnp.mean(x, axis=-1, keepdims=True)
    centered = x - mean
    r = lax.rsqrt(jnp.mean(centered * centered, axis=-1, keepdims=True) + EPSILON)
    normal = centered * r

    def tokens(j):
        return pl.ds(at128(block * j), block)

    n1[tokens(i)] = (normal * gain1 + bias1).astype(LOW)
    n2[pl.ds(0, block)] = (normal * gain2 + bias2).astype(LOW)
    pos_rx[i] = pos_tx[...]
    for e in mates:
        send(K_POS + e, pos_tx, pos_rx.at[i], {"ctx": mate(e)})

    class Relay:
        def __init__(self, piece):
            self.piece = piece
            self.direct = channels(Z)
            self.across = channels(2 * Z)
            self.to_right = channels(Z)
            self.to_left = channels(Z)

        def begin(self):
            mine = self.piece(i)
            send(self.to_right, mine, mine, right, self.direct + z, has_right)
            send(self.to_left, mine, mine, left, self.direct + z, has_left)
            send(self.across, mine, mine, partner, self.across + z)

        def step(self, k):
            @pl.when(z >= k)
            def _():
                arrived(self.direct + z - k, self.piece(i - 2 * k))

            piece = self.piece(i - 2 * k)
            if k < Z - 1:
                send(self.to_right + k, piece, piece, right, self.direct + z - k, (z >= k) & has_right)
            send(self.across + 2 * k - 1, piece, piece, partner, self.across + z - k, z >= k)

            @pl.when(z + k < Z)
            def _():
                arrived(self.direct + z + k, self.piece(i + 2 * k))

            piece = self.piece(i + 2 * k)
            if k < Z - 1:
                send(self.to_left + k, piece, piece, left, self.direct + z + k, (z + k < Z) & has_left)
            send(self.across + 2 * k, piece, piece, partner, self.across + z + k, z + k < Z)

        def end(self):
            for to in range(Z):
                arrived(self.across + to, self.piece(2 * to + other))

    normed = Relay(lambda j: n1.at[tokens(j)])
    normed.begin()
    for copy in loads[3:]:
        copy.wait()

    K_DO = channels(ctxs)
    K_DOS = channels(ctxs)
    K_DOM = channels(shards)

    def grad_attn(d):
        if d:
            arrived(K_COT + d, cot.at[pl.ds(block * d, block)])
        field = dot(cot[pl.ds(block * d, block)], wout[...], COLS_CONTRACT)
        for core in range(2):
            do_tx[d, core] = field[:, 128 * core : 128 * (core + 1)].astype(LOW)
        if d:
            send(K_DOM + d, do_tx.at[d], do_mid.at[d], {"shard": plane(d)})
        else:
            do_mid[0] = do_tx[0]

    def grad_attn_on(d):
        if d:
            arrived(K_DOM + d, do_mid.at[d])
        for core in range(2):
            target = 2 * plane(d) + core
            piece = do_mid.at[d, core]
            send(K_DOS + 2 * d + core, piece, do_rx.at[i], {"ctx": target}, K_DO + i, i != target)

            @pl.when(i == target)
            def _():
                do_rx[i] = do_mid[d, core]

    def send_wq(d):
        send(K_WQ + d, wq.at[my_rows], wq.at[my_rows], {"shard": plane(d)})

    near_planes, last_plane = planes[:-1], planes[-1]
    for d in (0, *near_planes):
        grad_attn(d)
    for d in near_planes:
        send_wq(d)
    normed.step(1)
    grad_attn_on(0)
    grad_attn(last_plane)
    send_wq(last_plane)
    my_half = pl.ds(at16(s * rows + c * half_rows), half_rows)
    for d in planes:
        send(
            K_WU + d,
            wup_hbm.at[
                pl.ds(at16(c * half_rows), half_rows), pl.ds(at128(plane(d) * width), width)
            ],
            wup.at[my_half],
            {"shard": plane(d)},
        )
    for d in planes:
        send(K_N2 + d, n2.at[pl.ds(0, block)], n2.at[pl.ds(block * d, block)], {"shard": plane(d)})
    for d in near_planes:
        grad_attn_on(d)
    normed.step(2)
    grad_attn_on(last_plane)
    for k in range(3, Z):
        normed.step(k)
    normed.end()
    for d in planes:
        arrived(K_WQ + d, wq.at[pl.ds(at16(plane(d) * rows), rows)])

    @pl.loop(0, ctxs // 2)
    def _(m):
        here = pl.ds(at128(m * 2 * block), 2 * block)
        qkv[pl.ds(2 * m, 2)] = dot(n1[here], wq[...]).reshape(2, block, 384)

    for e in mates:
        arrived(K_POS + e, pos_rx.at[mate(e)])
    to_scalar = pltpu.make_async_copy(pos_rx, pos_sm, lsem.at[len(loads)])
    to_scalar.start()
    to_scalar.wait()
    rank = [lax.div(pos_sm[j, 0, 0], block) for j in range(ctxs)]
    place = []
    for g in range(ctxs):
        found = jnp.int32(0)
        for j in range(1, ctxs):
            found = found + j * (rank[j] == g).astype(jnp.int32)
        place.append(lax.rem(found, ctxs))

    lane = lax.broadcasted_iota(jnp.int32, (block, 128), 1)
    leads = lax.rem(lane, HEAD_DIM) < ROTARY // 2

    def across(field):
        return jnp.where(
            leads,
            pltpu.roll(field, 128 - ROTARY // 2, 1),
            pltpu.roll(field, ROTARY // 2, 1),
        )

    def tables(g):
        off_cos, off_sin = rot_ref[pl.ds(0, block)], rot_ref[pl.ds(block, block)]
        start_cos = rot_ref[pl.ds(2 * block + g, 1)]
        start_sin = rot_ref[pl.ds(2 * block + ctxs + g, 1)]
        cosine = start_cos * off_cos - start_sin * off_sin
        sine = start_sin * off_cos + start_cos * off_sin
        return cosine, sine

    for j in range(ctxs):

        @pl.when(j != i)
        def _():
            arrived(K_DO + j, do_rx.at[j])

    for g in range(ctxs):
        here = pl.ds(block * g, block)
        field = qkv[place[g]] + qkv_bias
        cosine, sine = tables(g)
        q_raw, k_raw = field[:, :128], field[:, 128:256]
        turned_q = (q_raw * cosine + across(q_raw) * sine).astype(LOW)
        q_s[here] = turned_q * jnp.asarray(HEAD_DIM**-0.5, LOW)
        k_s[here] = (k_raw * cosine + across(k_raw) * sine).astype(LOW)
        v_s[here] = field[:, 256:].astype(LOW)
        do_s[here] = do_rx[place[g]]

    o_s[...] = jnp.zeros_like(o_s)
    dq_s[...] = jnp.zeros_like(dq_s)
    dk_s[...] = jnp.zeros_like(dk_s)
    dv_s[...] = jnp.zeros_like(dv_s)

    @pl.loop(0, 2)
    def _(h):
        mine = lax.div(lane, HEAD_DIM) == h
        for g in range(ctxs):
            share = 0 if g % 4 in (0, 3) else 1

            @pl.when((h == c) | (c == share))
            def _():
                here = pl.ds(block * g, block)
                upto = pl.ds(0, block * (g + 1))
                span = block * (g + 1)
                zero = jnp.zeros((block, 128), LOW)
                q_h = jnp.where(mine, q_s[here], zero)
                do_h = jnp.where(mine, do_s[here], zero)
                scores = dot(q_h, k_s[upto], COLS_CONTRACT)
                token = lax.broadcasted_iota(jnp.int32, (block, span), 0) + block * g
                key = lax.broadcasted_iota(jnp.int32, (block, span), 1)
                masked = jnp.where(key <= token, scores, NEGATIVE)
                top = jnp.max(masked, axis=-1, keepdims=True)
                weight = jnp.exp(masked - top)
                probability = weight * (1.0 / jnp.sum(weight, axis=-1, keepdims=True))
                prob_low = probability.astype(LOW)
                attended = jnp.where(mine, dot(prob_low, v_s[upto]), 0.0)
                o_s[g] += attended
                grad_prob = dot(do_h, v_s[upto], COLS_CONTRACT)
                row_delta = jnp.sum(do_h.astype(FULL) * attended, axis=-1, keepdims=True)
                grad_score = (probability * (grad_prob - row_delta)).astype(LOW)
                dq_s[here] += jnp.where(mine, dot(grad_score, k_s[upto]), 0.0)
                dk_s[upto] += dot(grad_score, q_h, ROWS_CONTRACT)
                dv_s[upto] += dot(prob_low, do_h, ROWS_CONTRACT)

    K_O = channels(2 * shards)
    K_OS = channels(ctxs)
    for j in range(ctxs):
        o_tx[j] = o_s[rank[j]].astype(LOW)
        away = (s != z) | (j != i)
        send(K_OS + j, o_tx.at[j], o_rx.at[2 * s + c], {"shard": z, "ctx": j}, K_O + 2 * s + c, away)

        @pl.when(jnp.logical_not(away))
        def _():
            o_rx[2 * s + c] = o_tx[j]

    bias_sum = jnp.zeros((1, 384), FULL)
    for g in range(ctxs):
        here = pl.ds(block * g, block)
        cosine, sine = tables(g)
        dq = dq_s[here] * (HEAD_DIM**-0.5)
        dk = dk_s[here]
        parts = (dq * cosine - across(dq) * sine, dk * cosine - across(dk) * sine, dv_s[here])
        part = jnp.concatenate(parts, axis=1).astype(LOW)
        gp_s[g] = part
        bias_sum = bias_sum + jnp.sum(part.astype(FULL), axis=0, keepdims=True)
    for j in range(ctxs):
        gp_e[pl.ds(block * j, block)] = gp_s[rank[j]]

    @pl.loop(0, ctxs // 2)
    def _(m):
        here = pl.ds(at128(m * 2 * block), 2 * block)
        a1_p[pl.ds(2 * m, 2)] = (
            dot(gp_e[here], wq[...], COLS_CONTRACT).astype(LOW).reshape(2, block, width)
        )

    K_A1D = channels(Z)
    for t in range(Z):
        send(K_A1D + t, a1_p.at[2 * t + other], a1_d2d.at[t], partner)

    @pl.loop(0, width // 256)
    def _(m):
        here = pl.ds(at128(m * 256), 256)
        gq_tx[here] = dot(n1[:, here], gp_e[...], ROWS_CONTRACT).astype(LOW)

    K_GQ = channels(shards)
    for d in planes:
        send(
            K_GQ + d, gq_tx.at[pl.ds(at16(plane(d) * rows), rows)], gq_rx.at[d], {"shard": plane(d)}
        )

    for t in range(Z):
        arrived(K_A1D + t, a1_d2d.at[t])
        a1_own[t] = (a1_p[2 * t + c].astype(FULL) + a1_d2d[t].astype(FULL)).astype(LOW)

    K_A1R = channels(Z)
    K_A1L = channels(Z)

    def a1_ends():
        for t in reversed(range(1, Z)):
            send(K_A1R + t, a1_own.at[t], a1_rx_r.at[t], right, None, z == 0)
        for t in range(Z - 1):
            send(K_A1L + t, a1_own.at[t], a1_rx_l.at[t], left, None, z == Z - 1)

    low_side = z < Z // 2

    def a1_right(t, here):
        when = (z > 0) & (z < t) & here

        @pl.when(when)
        def _():
            arrived(K_A1R + t, a1_rx_r.at[t])
            a1_tx_r[t] = (a1_own[t].astype(FULL) + a1_rx_r[t].astype(FULL)).astype(LOW)

        send(K_A1R + t, a1_tx_r.at[t], a1_rx_r.at[t], right, None, when)

    def a1_left(t, here):
        when = (z < Z - 1) & (z > t) & here

        @pl.when(when)
        def _():
            arrived(K_A1L + t, a1_rx_l.at[t])
            a1_tx_l[t] = (a1_own[t].astype(FULL) + a1_rx_l[t].astype(FULL)).astype(LOW)

        send(K_A1L + t, a1_tx_l.at[t], a1_rx_l.at[t], left, None, when)

    a1_ends()

    @pl.when(z == 0)
    def _():
        a1_rx_r[0] = jnp.zeros((block, width), LOW)

    @pl.when(z == Z - 1)
    def _():
        a1_rx_l[Z - 1] = jnp.zeros((block, width), LOW)

    early_a[...] = jnp.zeros_like(early_a)
    for d in planes:
        arrived(K_WU + d, wup.at[pl.ds(at16(plane(d) * rows + c * half_rows), half_rows)])
        part = wup.at[pl.ds(at16(plane(d) * rows + c * half_rows), half_rows)]
        send(K_WU2 + d, part, part, partner)
    for d in planes:
        arrived(K_N2 + d, n2.at[pl.ds(block * d, block)])
    for d in planes:
        arrived(K_WU2 + d, wup.at[pl.ds(at16(plane(d) * rows + other * half_rows), half_rows)])
    out_acc[...] = jnp.zeros_like(out_acc)
    a2_acc[...] = jnp.zeros_like(a2_acc)

    @pl.loop(0, width // 256)
    def _(t):
        units = pl.ds(at128(t * 256), 256)
        bias = upb_ref[pl.ds(at128(s * width + t * 256), 256)][None, :]
        pre = dot(n2[...], wup[:, units]) + bias
        cdf = 0.5 * (1.0 + lax.erf(pre * INV_ROOT_TWO))
        hidden = (pre * cdf).astype(LOW)
        slope = cdf + pre * (jnp.exp(-0.5 * pre * pre) * INV_ROOT_TWO_PI)
        grad_hidden = dot(cot[...], wdn[units], COLS_CONTRACT)
        grad_pre = (grad_hidden * slope).astype(LOW)
        early_a[pl.ds(t, 1)] = jnp.sum(grad_pre.astype(FULL), axis=0, keepdims=True)
        out_acc[...] += dot(hidden, wdn[units])
        a2_acc[...] += dot(grad_pre, wup[:, units], COLS_CONTRACT)
        gd16[units] = dot(hidden, cot[...], ROWS_CONTRACT).astype(LOW)
        gu16[:, units] = dot(n2[...], grad_pre, ROWS_CONTRACT).astype(LOW)

    K_GD = channels(1)
    K_GU = channels(shards)
    K_GUX = channels(shards)
    K_OUT = channels(shards)
    K_A2 = channels(shards)
    K_GO = channels(1)

    def rows_of(d, core):
        return pl.ds(at16(plane(d) * rows + core * half_rows), half_rows)

    for d in range(shards):
        send(K_GU + d, gu16.at[rows_of(d, other)], gu_rx.at[d], partner)
    send(K_GD, gd16.at[pl.ds(at16(other * half_width), half_width)], gd_rx, partner)
    for d in planes:
        a2_tx[d] = a2_acc[pl.ds(block * d, block)].astype(LOW)

    for seq in range(shards):
        for core in range(2):
            k = 2 * seq + core

            @pl.when((seq != s) | (2 * s + core != i))
            def _():
                arrived(K_O + k, o_rx.at[k])

            attn[pl.ds(block * seq, block), 128 * core : 128 * (core + 1)] = o_rx[k]
    for d in range(shards):
        mine = attn[tokens(plane(d))]
        total = out_acc[pl.ds(block * d, block)] + dot(mine, wout[...])
        if d:
            out_tx[d] = total.astype(LOW)
        else:
            out_acc[pl.ds(0, block)] = total
    go = dot(attn[tokens(plane(0))], cot[pl.ds(0, block)], ROWS_CONTRACT)
    for d in planes:
        go = go + dot(attn[tokens(plane(d))], cot[pl.ds(block * d, block)], ROWS_CONTRACT)
    go16[pl.ds(0, HEAD_DIM)] = go[:HEAD_DIM].astype(LOW)
    go16[pl.ds(HEAD_DIM, HEAD_DIM)] = (
        go[HEAD_DIM : 2 * HEAD_DIM] + go[2 * HEAD_DIM : 3 * HEAD_DIM]
    ).astype(LOW)
    go16[pl.ds(2 * HEAD_DIM, HEAD_DIM)] = go[3 * HEAD_DIM :].astype(LOW)
    send(K_GO, go16.at[pl.ds(at16(other * half_rows), half_rows)], go_rx, partner)

    UP = half_width + half_rows

    def up_rows(index):
        return pl.ds(at16(UP + index * half_rows), half_rows)

    for d in (*planes, 0):
        arrived(K_GU + d, gu_rx.at[d])
        total = (gu16[rows_of(d, c)].astype(FULL) + gu_rx[d].astype(FULL)).astype(LOW)
        if d:
            gu_tx[d] = total
            send(K_GUX + d, gu_tx.at[d], line_own.at[up_rows(s)], {"shard": plane(d)})
        else:
            line_own[up_rows(s)] = total
    for d in planes:
        send(K_A2 + d, a2_tx.at[d], a2_rx.at[d], {"shard": plane(d)})
    for d in planes:
        send(K_OUT + d, out_tx.at[d], out_rx.at[d], {"shard": plane(d)})

    is_end = (z == 0) | (z == Z - 1)
    is_mid = jnp.logical_not(is_end)
    is_centre = (z == Z // 2 - 1) | (z == Z // 2)
    inward = jnp.where(z < Z // 2, 2, -2)
    inner = {"ctx": i + inward}
    outer = {"ctx": i - inward}
    to_inner = jnp.where(is_centre, 1, 0)
    line_rows = half_width + half_rows + shards * half_rows
    chunks = line_rows // CHUNK
    first_up = UP // CHUNK
    K_OUTER = channels(chunks)
    K_INNER = channels(chunks)
    K_NEAR = channels(chunks)
    K_FAR = channels(chunks)
    K_FIN = channels(chunks)

    def span_of(q):
        return pl.ds(q * CHUNK, CHUNK)

    def near_end(q):
        send(
            K_NEAR + q,
            line_own.at[span_of(q)],
            line_rx.at[to_inner, span_of(q)],
            inner,
            K_OUTER + chunks * to_inner + q,
            is_end,
        )

    def near_mid(q):
        @pl.when(is_mid)
        def _():
            arrived(K_OUTER + q, line_rx.at[0, span_of(q)])
            line_near[span_of(q)] = (
                line_rx[0, span_of(q)].astype(FULL) + line_own[span_of(q)].astype(FULL)
            ).astype(LOW)

        send(
            K_INNER + q,
            line_near.at[span_of(q)],
            line_rx.at[to_inner, span_of(q)],
            inner,
            K_OUTER + chunks * to_inner + q,
            is_mid,
        )

    def far(q):
        arrived(K_INNER + q, line_rx.at[1, span_of(q)])
        beyond = line_rx[1, span_of(q)].astype(FULL) + line_own[span_of(q)].astype(FULL)

        @pl.when(is_mid)
        def _():
            line_far[span_of(q)] = beyond.astype(LOW)

        send(
            K_FAR + q, line_far.at[span_of(q)], line_rx.at[1, span_of(q)], outer, K_INNER + q, is_mid
        )
        fin_ref[c, span_of(q)] = (beyond + line_rx[0, span_of(q)].astype(FULL)).astype(LOW)
        send(K_FIN + q, fin_ref.at[c, span_of(q)], fin_ref.at[c, span_of(q)], partner)

    @pl.when(is_end)
    def _():
        line_rx[0] = jnp.zeros((line_rows, width), LOW)

    arrived(K_GD, gd_rx)
    line_own[pl.ds(0, half_width)] = (
        gd16[pl.ds(at16(c * half_width), half_width)].astype(FULL) + gd_rx[...].astype(FULL)
    ).astype(LOW)
    for q in range(half_width // CHUNK):
        near_end(q)
    arrived(K_GO, go_rx)
    line_own[pl.ds(half_width, half_rows)] = (
        go16[pl.ds(at16(c * half_rows), half_rows)].astype(FULL) + go_rx[...].astype(FULL)
    ).astype(LOW)
    for q in range(half_width // CHUNK, first_up):
        near_end(q)

    for t in reversed(range(1, Z)):
        a1_right(t, low_side)
        a1_left(Z - 1 - t, jnp.logical_not(low_side))

    own_gq = gq_tx[my_rows].astype(FULL)
    for d in planes:
        arrived(K_GQ + d, gq_rx.at[d])
        own_gq = own_gq + gq_rx[d].astype(FULL)
    qkvfin_ref[i] = own_gq.astype(LOW)
    spread = Relay(lambda j: qkvfin_ref.at[j])

    for t in reversed(range(1, Z)):
        a1_right(t, jnp.logical_not(low_side))
        a1_left(Z - 1 - t, low_side)
    K_E = channels(ctxs)
    K_EX = channels(shards)
    early_a[3:4] = bias_sum[:, :256]
    early_a[4:5, 0:128] = bias_sum[:, 256:]
    for e in mates:
        send(K_E + e, early_a, early_rx.at[e], {"ctx": mate(e)})
    early_rx[0] = early_a[...]

    for q in range(4):
        near_mid(q)
    spread.begin()
    for d in planes:
        arrived(K_GUX + d, line_own.at[up_rows(plane(d))])
    for q in range(first_up, chunks):
        near_end(q)
    near_mid(4)
    far(0)
    near_mid(5)
    far(1)
    near_mid(6)
    far(2)
    near_mid(7)
    far(3)
    near_mid(8)
    far(4)
    near_mid(9)
    far(5)
    a1 = a1_own[z].astype(FULL)

    @pl.when(has_left)
    def _():
        arrived(K_A1R + z, a1_rx_r.at[z])

    @pl.when(has_right)
    def _():
        arrived(K_A1L + z, a1_rx_l.at[z])

    a1 = a1 + a1_rx_r[z].astype(FULL) + a1_rx_l[z].astype(FULL)
    a2 = a2_acc[pl.ds(0, block)]
    for d in planes:
        arrived(K_A2 + d, a2_rx.at[d])
        a2 = a2 + a2_rx[d].astype(FULL)
    sums = (a1 * normal, a1, a2 * normal, a2)
    for k, field in enumerate(sums):
        total = jnp.sum(field, axis=0, keepdims=True)
        late_a[2 * k : 2 * k + 1] = total[:, :half_width]
        late_a[2 * k + 1 : 2 * k + 2] = total[:, half_width:]
    K_L = channels(ctxs)
    K_LX = channels(shards)
    for e in mates:
        send(K_L + e, late_a, late_rx.at[e], {"ctx": mate(e)})
    late_rx[0] = late_a[...]
    mixed = a1 * gain1 + a2 * gain2
    back = r * (
        mixed
        - jnp.mean(mixed, axis=-1, keepdims=True)
        - normal * jnp.mean(mixed * normal, axis=-1, keepdims=True)
    )
    dx_ref[...] = (cot[pl.ds(0, block)].astype(FULL) + back).astype(LOW)
    for q in range(10, 12):
        near_mid(q)
        far(q - 4)
    spread.step(1)
    for q in range(12, 15):
        near_mid(q)
        far(q - 4)
    total = x_ref[...].astype(FULL) + out_acc[pl.ds(0, block)]
    for d in planes:
        arrived(K_OUT + d, out_rx.at[d])
        total = total + out_rx[d].astype(FULL)
    y_ref[...] = total.astype(LOW)
    for e in mates:
        arrived(K_E + e, early_rx.at[e])
    summed = early_rx[0]
    for e in mates:
        summed = summed + early_rx[e]
    early_b[0, 0:8] = summed
    for j in range(ctxs):
        early_b[0, 8 + 2 * j : 10 + 2 * j] = early_rx[flip(i, j), 3:5]
    for e in mates:
        arrived(K_L + e, late_rx.at[e])
    summed = late_rx[0]
    for e in mates:
        summed = summed + late_rx[e]
    late_b[0] = summed
    for d in planes:
        send(K_EX + d, early_b.at[0], early_b.at[d], {"shard": plane(d)})
        send(K_LX + d, late_b.at[0], late_b.at[d], {"shard": plane(d)})
    spread.step(2)
    for q in range(15, chunks):
        near_mid(q)
        far(q - 4)
    for q in range(chunks - 4, chunks):
        far(q)
    for d in planes:
        arrived(K_EX + d, early_b.at[d])
        arrived(K_LX + d, late_b.at[d])
    whole = early_b[0]
    late = late_b[0]
    for d in planes:
        whole = whole + early_b[d]
        late = late + late_b[d]
    late_ref[...] = late
    early_ref[0:24] = whole
    for j in range(shards):
        early_ref[24 + 8 * j : 32 + 8 * j] = early_b[flip(s, j), 0:8]
    for k in range(3, Z):
        spread.step(k)
    spread.end()
    for q in range(chunks):
        arrived(K_FIN + q, fin_ref.at[other, span_of(q)])
    assert used[0] <= ssem.shape[0]
    for copy, when in sent:
        if when is always:
            copy.wait_send()
        else:
            pl.when(when)(copy.wait_send)


def ring_on_device(
    layer_input,
    positions,
    cotangent,
    ln1_gain,
    ln1_bias,
    ln2_gain,
    ln2_bias,
    w_qkv,
    qkv_bias,
    w_out,
    w_up,
    up_bias,
    w_down,
):
    seqs_here, block_len, feature_count = layer_input.shape
    row_count = seqs_here * block_len
    head_count = HEADS
    head_size = HEAD_DIM
    score_scale = head_size ** (-0.5)
    whole_qkv, whole_out, whole_up, whole_down = (
        lax.all_gather(w_qkv, "shard", axis=0, tiled=True),
        lax.all_gather(w_out, "shard", axis=0, tiled=True),
        lax.all_gather(w_up, "shard", axis=0, tiled=True),
        lax.all_gather(w_down, "shard", axis=0, tiled=True),
    )
    all_positions = lax.all_gather(positions, "ctx", axis=1, tiled=True)
    cycle_size = lax.axis_size("ctx")
    my_index = lax.axis_index("ctx")
    inputs = layer_input.astype(jnp.float32).reshape(row_count, feature_count)
    normed_one = layer_norm(inputs, ln1_gain, ln1_bias).astype(jnp.bfloat16)
    normed_two = layer_norm(inputs, ln2_gain, ln2_bias).astype(jnp.bfloat16)
    projected = jnp.dot(normed_one, whole_qkv, preferred_element_type=jnp.float32) + qkv_bias
    split_heads = projected.reshape(seqs_here, block_len, 3, head_count, head_size)
    cosine, sine_table = rotary_tables(positions)
    queries = rotate(split_heads[:, :, 0], cosine, sine_table).astype(jnp.bfloat16)
    key_rows = rotate(split_heads[:, :, 1], cosine, sine_table).astype(jnp.bfloat16)
    value_rows = split_heads[:, :, 2].astype(jnp.bfloat16)
    top_query = jnp.max(positions)

    def attend_block(running, key_blk, value_blk, key_pos):

        def attend_update(current):
            run_max, run_sum, run_acc = current
            scores = (
                jnp.einsum("sqhd,skhd->shqk", queries, key_blk, preferred_element_type=jnp.float32)
                * score_scale
            )
            allowed = key_pos[:, None, None, :] <= positions[:, None, :, None]
            masked = jnp.where(allowed, scores, NEGATIVE)
            new_max = jnp.maximum(run_max, jnp.max(masked, axis=-1))
            shrink = jnp.exp(run_max - new_max)
            weights_now = jnp.where(allowed, jnp.exp(masked - new_max[..., None]), 0.0)
            run_sum = run_sum * shrink + jnp.sum(weights_now, axis=-1)
            added_term = jnp.einsum(
                "shqk,skhd->sqhd",
                weights_now.astype(jnp.bfloat16),
                value_blk,
                preferred_element_type=jnp.float32,
            )
            run_acc = run_acc * jnp.transpose(shrink, (0, 2, 1))[..., None] + added_term
            return (new_max, run_sum, run_acc)

        return lax.cond(
            jnp.min(key_pos) <= top_query, attend_update, lambda unchanged: unchanged, running
        )

    initial = (
        jnp.full((seqs_here, head_count, block_len), NEGATIVE, jnp.float32),
        jnp.zeros((seqs_here, head_count, block_len), jnp.float32),
        jnp.zeros((seqs_here, block_len, head_count, head_size), jnp.float32),
    )
    own_block = attend_block(initial, key_rows, value_rows, positions)

    def cycle_forward(turn_index, carried):
        current, key_cur, value_cur = carried
        key_cur, value_cur = shifted((key_cur, value_cur), "ctx", 1)
        source = (my_index - turn_index) % cycle_size
        key_pos = lax.dynamic_slice_in_dim(all_positions, source * block_len, block_len, 1)
        return (attend_block(current, key_cur, value_cur, key_pos), key_cur, value_cur)

    (run_max, run_sum, run_acc), unused_key, unused_value = lax.fori_loop(
        1, cycle_size, cycle_forward, (own_block, key_rows, value_rows)
    )
    attn_vals = run_acc / jnp.transpose(run_sum, (0, 2, 1))[..., None]
    log_total = run_max + jnp.log(run_sum)
    attn_low = attn_vals.astype(jnp.bfloat16).reshape(row_count, feature_count)
    attn_branch = jnp.dot(attn_low, whole_out, preferred_element_type=jnp.float32)
    hidden_pre = jnp.dot(normed_two, whole_up, preferred_element_type=jnp.float32) + up_bias
    hidden_low = gelu_exact(hidden_pre).astype(jnp.bfloat16)
    mlp_branch = jnp.dot(hidden_low, whole_down, preferred_element_type=jnp.float32)
    layer_output = (
        (inputs + attn_branch + mlp_branch)
        .astype(jnp.bfloat16)
        .reshape(seqs_here, block_len, feature_count)
    )
    cot_low = cotangent.reshape(row_count, feature_count)
    cot_full = cot_low.astype(jnp.float32)
    grad_down = jnp.einsum("rf,rd->fd", hidden_low, cot_low, preferred_element_type=jnp.float32)
    grad_hidden = jnp.einsum("rd,fd->rf", cot_low, whole_down, preferred_element_type=jnp.float32)
    unused_gelu, gelu_back = jax.vjp(gelu_exact, hidden_pre)
    grad_pre = gelu_back(grad_hidden)[0].astype(jnp.bfloat16)
    grad_up_bias = jnp.sum(grad_pre.astype(jnp.float32), axis=0)
    grad_up = jnp.einsum("rd,rf->df", normed_two, grad_pre, preferred_element_type=jnp.float32)
    grad_two = jnp.einsum("rf,df->rd", grad_pre, whole_up, preferred_element_type=jnp.float32)
    grad_out = jnp.einsum("rd,re->de", attn_low, cot_low, preferred_element_type=jnp.float32)
    grad_attn = (
        jnp.einsum("re,de->rd", cot_low, whole_out, preferred_element_type=jnp.float32)
        .astype(jnp.bfloat16)
        .reshape(seqs_here, block_len, head_count, head_size)
    )
    row_delta = jnp.transpose(
        jnp.sum(grad_attn.astype(jnp.float32) * attn_vals, axis=-1), (0, 2, 1)
    )

    def back_block(grads_in, key_blk, value_blk, key_pos):

        def back_update(current):
            grad_query, grad_key, grad_value = current
            scores = (
                jnp.einsum("sqhd,skhd->shqk", queries, key_blk, preferred_element_type=jnp.float32)
                * score_scale
            )
            allowed = key_pos[:, None, None, :] <= positions[:, None, :, None]
            masked = jnp.where(allowed, scores, NEGATIVE)
            probability = jnp.exp(masked - log_total[..., None])
            prob_low = probability.astype(jnp.bfloat16)
            grad_value = grad_value + jnp.einsum(
                "shqk,sqhd->skhd", prob_low, grad_attn, preferred_element_type=jnp.float32
            )
            grad_prob = jnp.einsum(
                "sqhd,skhd->shqk", grad_attn, value_blk, preferred_element_type=jnp.float32
            )
            grad_score = (probability * (grad_prob - row_delta[..., None])).astype(jnp.bfloat16)
            grad_query = (
                grad_query
                + jnp.einsum(
                    "shqk,skhd->sqhd", grad_score, key_blk, preferred_element_type=jnp.float32
                )
                * score_scale
            )
            grad_key = (
                grad_key
                + jnp.einsum(
                    "shqk,sqhd->skhd", grad_score, queries, preferred_element_type=jnp.float32
                )
                * score_scale
            )
            return (grad_query, grad_key, grad_value)

        return lax.cond(
            jnp.min(key_pos) <= top_query, back_update, lambda unchanged: unchanged, grads_in
        )

    zero_rows = jnp.zeros((seqs_here, block_len, head_count, head_size), jnp.float32)

    def pass_back(grad_key, grad_value):
        return (
            shifted(grad_key.astype(jnp.bfloat16), "ctx", 1).astype(grad_key.dtype),
            shifted(grad_value.astype(jnp.bfloat16), "ctx", 1).astype(grad_value.dtype),
        )

    grad_query, grad_key, grad_value = back_block(
        (zero_rows, zero_rows, zero_rows), key_rows, value_rows, positions
    )
    grad_key, grad_value = pass_back(grad_key, grad_value)

    def cycle_backward(turn_index, carried):
        grad_query, key_cur, value_cur, grad_key, grad_value = carried
        key_cur, value_cur = shifted((key_cur, value_cur), "ctx", 1)
        source = (my_index - turn_index) % cycle_size
        key_pos = lax.dynamic_slice_in_dim(all_positions, source * block_len, block_len, 1)
        grad_query, grad_key, grad_value = back_block(
            (grad_query, grad_key, grad_value), key_cur, value_cur, key_pos
        )
        grad_key, grad_value = pass_back(grad_key, grad_value)
        return (grad_query, key_cur, value_cur, grad_key, grad_value)

    grad_query, unused_key, unused_value, grad_key, grad_value = lax.fori_loop(
        1, cycle_size, cycle_backward, (grad_query, key_rows, value_rows, grad_key, grad_value)
    )
    unused_rot, rotate_back = jax.vjp(
        lambda field_in: rotate(field_in, cosine, sine_table), zero_rows
    )
    query_pre = rotate_back(grad_query)[0]
    key_pre = rotate_back(grad_key)[0]
    grad_proj = (
        jnp.stack([query_pre, key_pre, grad_value], axis=2)
        .reshape(row_count, 3 * feature_count)
        .astype(jnp.bfloat16)
    )
    grad_qkv_bias = jnp.sum(grad_proj.astype(jnp.float32), axis=0)
    grad_qkv = jnp.einsum("rd,re->de", normed_one, grad_proj, preferred_element_type=jnp.float32)
    grad_one = jnp.einsum("re,de->rd", grad_proj, whole_qkv, preferred_element_type=jnp.float32)
    unused_one, norm_back_one = jax.vjp(layer_norm, inputs, ln1_gain, ln1_bias)
    input_one, grad_gain_one, grad_bias_one = norm_back_one(grad_one)
    unused_two, norm_back_two = jax.vjp(layer_norm, inputs, ln2_gain, ln2_bias)
    input_two, grad_gain_two, grad_bias_two = norm_back_two(grad_two)
    grad_input = (
        (cot_full + input_one + input_two)
        .astype(jnp.bfloat16)
        .reshape(seqs_here, block_len, feature_count)
    )
    summed = (
        lax.psum(grad_qkv.astype(jnp.bfloat16), "ctx").astype(jnp.float32),
        lax.psum(grad_out.astype(jnp.bfloat16), "ctx").astype(jnp.float32),
        lax.psum(grad_up.astype(jnp.bfloat16), "ctx").astype(jnp.float32),
        lax.psum(grad_down.astype(jnp.bfloat16), "ctx").astype(jnp.float32),
        lax.psum(grad_gain_one.astype(jnp.bfloat16), "ctx").astype(jnp.float32),
        lax.psum(grad_bias_one.astype(jnp.bfloat16), "ctx").astype(jnp.float32),
        lax.psum(grad_gain_two.astype(jnp.bfloat16), "ctx").astype(jnp.float32),
        lax.psum(grad_bias_two.astype(jnp.bfloat16), "ctx").astype(jnp.float32),
        lax.psum(grad_qkv_bias.astype(jnp.bfloat16), "ctx").astype(jnp.float32),
        lax.psum(grad_up_bias.astype(jnp.bfloat16), "ctx").astype(jnp.float32),
    )
    sum_qkv, sum_out, sum_up, sum_down = (
        lax.psum_scatter(
            summed[0].astype(jnp.bfloat16), "shard", scatter_dimension=0, tiled=True
        ).astype(jnp.float32),
        lax.psum_scatter(
            summed[1].astype(jnp.bfloat16), "shard", scatter_dimension=0, tiled=True
        ).astype(jnp.float32),
        lax.psum_scatter(
            summed[2].astype(jnp.bfloat16), "shard", scatter_dimension=0, tiled=True
        ).astype(jnp.float32),
        lax.psum_scatter(
            summed[3].astype(jnp.bfloat16), "shard", scatter_dimension=0, tiled=True
        ).astype(jnp.float32),
    )
    sum_small = (
        lax.psum(summed[4].astype(jnp.bfloat16), "shard").astype(jnp.float32),
        lax.psum(summed[5].astype(jnp.bfloat16), "shard").astype(jnp.float32),
        lax.psum(summed[6].astype(jnp.bfloat16), "shard").astype(jnp.float32),
        lax.psum(summed[7].astype(jnp.bfloat16), "shard").astype(jnp.float32),
        lax.psum(summed[8].astype(jnp.bfloat16), "shard").astype(jnp.float32),
        lax.psum(summed[9].astype(jnp.bfloat16), "shard").astype(jnp.float32),
    )
    return (
        layer_output,
        grad_input,
        sum_small[0],
        sum_small[1],
        sum_small[2],
        sum_small[3],
        sum_qkv,
        sum_small[4],
        sum_out,
        sum_up,
        sum_small[5],
        sum_down,
    )


def finish_body(
    y_in, dx_in, fin, qkvfin, early, late,
    y_out, dx_out, g1_out, b1_out, g2_out, b2_out, gqkv_out, gqkvb_out, gout_out, gup_out, gupb_out, gdown_out,
    gqkv, gout, gup, gdown, sem,
):
    width = y_in.shape[1]
    chips = qkvfin.shape[0] // 2
    rows = qkvfin.shape[1]
    half = rows // 2
    cut = width // 2
    shards = width // rows
    slabs = 8 + 4 * chips
    copies = []

    def out(src, dst):
        copy = pltpu.make_async_copy(src, dst, sem.at[len(copies)])
        copy.start()
        copies.append(copy)

    out(y_in, y_out.at[0])
    out(dx_in, dx_out.at[0])
    for h in range(2):
        gdown[pl.ds(cut * h, cut)] = fin[h, pl.ds(0, cut)].astype(FULL)
        out(gdown.at[pl.ds(cut * h, cut)], gdown_out.at[pl.ds(cut * h, cut)])
    for h in range(2):
        mine = pl.ds(half * h, half)
        for n in range(shards):
            here = fin[h, pl.ds(cut + half + half * n, half)]
            gup[mine, width * n : width * (n + 1)] = here.astype(FULL)
        out(gup.at[mine], gup_out.at[mine])

    def tiles(piece, wide, put):
        lane = lax.broadcasted_iota(jnp.int32, wide, 1)
        low_lanes = lane < HEAD_DIM
        for part in range(3):
            for w in range(chips // 2):
                p0, p1, p2, p3 = (piece(4 * w + t, part) for t in range(4))
                r1, r2 = pltpu.roll(p1, HEAD_DIM, 1), pltpu.roll(p2, HEAD_DIM, 1)
                at = width * part + 384 * w
                put(at, p0 + jnp.where(low_lanes, 0.0, r1))
                put(at + 128, jnp.where(low_lanes, r1, r2))
                put(at + 256, p3 + jnp.where(low_lanes, r2, 0.0))

    def put_rows(at, tile):
        gqkv[:, at : at + 128] = tile

    tiles(
        lambda j, part: qkvfin[j, :, 128 * part : 128 * (part + 1)].astype(FULL),
        (rows, 128),
        put_rows,
    )
    out(gqkv, gqkv_out)
    for h in range(2):
        gout[pl.ds(half * h, half)] = fin[h, pl.ds(cut, half)].astype(FULL)
    out(gout, gout_out)

    def bias_piece(j, part):
        row = early[8 + 2 * j + part // 2, 128 * (part % 2) : 128 * (part % 2 + 1)]
        return jnp.broadcast_to(row[None, :], (8, 128))

    def put_bias(at, tile):
        gqkvb_out[pl.ds(at, 128)] = tile[0]

    tiles(bias_piece, (8, 128), put_bias)
    for n in range(shards):
        for t in range(width // 256):
            gupb_out[pl.ds(width * n + 256 * t, 256)] = early[slabs + 8 * n + t]
    for k, vector in enumerate((g1_out, b1_out, g2_out, b2_out)):
        vector[pl.ds(0, cut)] = late[2 * k]
        vector[pl.ds(cut, cut)] = late[2 * k + 1]
    for copy in copies:
        copy.wait()


def finish(rows, shards, ctxs, *pieces):
    block, width = pieces[0].shape
    vmem = pl.BlockSpec(memory_space=pltpu.VMEM)
    hbm = pl.BlockSpec(memory_space=pl.ANY)
    shape = jax.ShapeDtypeStruct
    vector = shape((width,), FULL)
    return pl.pallas_call(
        finish_body,
        out_shape=(
            shape((1, block, width), LOW),
            shape((1, block, width), LOW),
            vector,
            vector,
            vector,
            vector,
            shape((rows, 3 * width), FULL),
            shape((3 * width,), FULL),
            shape((rows, width), FULL),
            shape((rows, shards * width), FULL),
            shape((shards * width,), FULL),
            shape((width, width), FULL),
        ),
        in_specs=[vmem] * 6,
        out_specs=(hbm, hbm, vmem, vmem, vmem, vmem, hbm, vmem, hbm, hbm, vmem, hbm),
        scratch_shapes=[
            pltpu.VMEM((rows, 3 * width), FULL),
            pltpu.VMEM((rows, width), FULL),
            pltpu.VMEM((rows, shards * width), FULL),
            pltpu.VMEM((width, width), FULL),
            pltpu.SemaphoreType.DMA((8,)),
        ],
        compiler_params=pltpu.CompilerParams(vmem_limit_bytes=24 * 2**20),
        name="finish",
    )(*pieces)


def fused_on_device(
    layer_input,
    positions,
    cotangent,
    ln1_gain,
    ln1_bias,
    ln2_gain,
    ln2_bias,
    w_qkv,
    qkv_bias,
    w_out,
    w_up,
    up_bias,
    w_down,
):
    shards, ctxs = lax.axis_size("shard"), lax.axis_size("ctx")
    block, width = layer_input.shape[1:]
    rows = w_qkv.shape[0]
    half = rows // 2
    line_rows = width // 2 + half + shards * half
    vmem = pl.BlockSpec(memory_space=pltpu.VMEM)
    hbm = pl.BlockSpec(memory_space=pl.ANY)
    low, full = (lambda *shape: pltpu.VMEM(shape, LOW)), (lambda *shape: pltpu.VMEM(shape, FULL))
    chips = ctxs // 2
    scratch = dict(
        wq=low(width, 384),
        wraw=low(3, rows, 256),
        wup=low(width, width),
        wout=low(256, width),
        wdn=low(width, width),
        n1=low(ctxs * block, width),
        n2=low(shards * block, width),
        cot=low(shards * block, width),
        pos_tx=pltpu.VMEM((8, block), jnp.int32),
        pos_rx=pltpu.VMEM((ctxs, 8, block), jnp.int32),
        pos_sm=pltpu.SMEM((ctxs, 8, block), jnp.int32),
        qkv=full(ctxs, block, 384),
        q_s=low(ctxs * block, 128),
        k_s=low(ctxs * block, 128),
        v_s=low(ctxs * block, 128),
        do_tx=low(shards, 2, block, 128),
        do_mid=low(shards, 2, block, 128),
        do_rx=low(ctxs, block, 128),
        do_s=low(ctxs * block, 128),
        o_s=full(ctxs, block, 128),
        dq_s=full(ctxs * block, 128),
        dk_s=full(ctxs * block, 128),
        dv_s=full(ctxs * block, 128),
        gp_s=low(ctxs, block, 384),
        gp_e=low(ctxs * block, 384),
        o_tx=low(ctxs, block, 128),
        o_rx=low(2 * shards, block, 128),
        attn=low(shards * block, 256),
        a1_p=low(ctxs, block, width),
        a1_d2d=low(chips, block, width),
        a1_own=low(chips, block, width),
        a1_tx_r=low(chips, block, width),
        a1_tx_l=low(chips, block, width),
        a1_rx_r=low(chips, block, width),
        a1_rx_l=low(chips, block, width),
        gq_tx=low(width, 384),
        gq_rx=low(shards, rows, 384),
        out_acc=full(shards * block, width),
        a2_acc=full(shards * block, width),
        out_tx=low(shards, block, width),
        out_rx=low(shards, block, width),
        a2_tx=low(shards, block, width),
        a2_rx=low(shards, block, width),
        gd16=low(width, width),
        gd_rx=low(width // 2, width),
        gu16=low(width, width),
        gu_rx=low(shards, half, width),
        gu_tx=low(shards, half, width),
        go16=low(rows, width),
        go_rx=low(half, width),
        line_own=low(line_rows, width),
        line_rx=low(2, line_rows, width),
        line_near=low(line_rows, width),
        line_far=low(line_rows, width),
        early_a=full(8, 256),
        early_rx=full(ctxs, 8, 256),
        early_b=full(shards, 8 + 2 * ctxs, 256),
        late_a=full(8, width // 2),
        late_rx=full(ctxs, 8, width // 2),
        late_b=full(shards, 8, width // 2),
        ssem=pltpu.SemaphoreType.DMA((320,)),
        rsem=pltpu.SemaphoreType.DMA((320,)),
        lsem=pltpu.SemaphoreType.DMA((16,)),
    )
    slabs = 8 + 2 * ctxs
    y, dx, fin, qkvfin, early, late = pl.pallas_call(
        functools.partial(fused_body, tuple(scratch)),
        out_shape=(
            jax.ShapeDtypeStruct((block, width), LOW),
            jax.ShapeDtypeStruct((block, width), LOW),
            jax.ShapeDtypeStruct((2, line_rows, width), LOW),
            jax.ShapeDtypeStruct((ctxs, rows, 384), LOW),
            jax.ShapeDtypeStruct((slabs + 8 * shards, 256), FULL),
            jax.ShapeDtypeStruct((8, width // 2), FULL),
        ),
        in_specs=[vmem] * 9 + [hbm] * 5,
        out_specs=(vmem,) * 6,
        scratch_shapes=list(scratch.values()),
        compiler_params=pltpu.CompilerParams(
            collective_id=0, has_side_effects=True, vmem_limit_bytes=60 * 1024 * 1024
        ),
        name="layer",
    )(
        layer_input[0],
        positions,
        ln1_gain,
        ln1_bias,
        ln2_gain,
        ln2_bias,
        qkv_bias,
        up_bias,
        jnp.asarray(rotary_constants(ctxs, block)),
        cotangent[0],
        w_qkv,
        w_up,
        w_out,
        w_down,
    )
    return finish(rows, shards, ctxs, y, dx, fin, qkvfin, early, late)


def on_device(layer_input, positions, cotangent, *params):
    shards, ctxs = lax.axis_size("shard"), lax.axis_size("ctx")
    seqs, block, width = layer_input.shape
    rows, ff = params[4].shape[0], params[7].shape[1]
    fits = (
        seqs == 1
        and block == 128
        and (shards, ctxs) == (4, 8)
        and 3 * ctxs == 2 * HEADS
        and HEAD_DIM == 64
        and rows * shards == width == HEADS * HEAD_DIM
        and ff == shards * width
    )
    path = fused_on_device if fits else ring_on_device
    return path(layer_input, positions, cotangent, *params)


def solution(mesh):
    placed = (
        P("shard", "ctx", None),
        P("shard", "ctx"),
        P("shard", "ctx", None),
        P(),
        P(),
        P(),
        P(),
        P("shard", None),
        P(),
        P("shard", None),
        P("shard", None),
        P(),
        P("shard", None),
    )
    return jax.shard_map(
        on_device,
        mesh=mesh,
        in_specs=placed,
        out_specs=(
            P("shard", "ctx", None),
            P("shard", "ctx", None),
            P(),
            P(),
            P(),
            P(),
            P("shard", None),
            P(),
            P("shard", None),
            P("shard", None),
            P(),
            P("shard", None),
        ),
        check_vma=False,
    )
```

```python
import functools

import jax
import jax.numpy as jnp
import numpy as np
from jax import lax
from jax.experimental import pallas as pl
from jax.experimental.pallas import tpu as pltpu
from jax.sharding import PartitionSpec as P

HEADS = 12
HEAD_DIM = 64
ROTARY = 16


EPSILON = 1e-05
NEGATIVE = -1e30


def shifted(shard, axis, by):
    count = lax.axis_size(axis)
    return lax.ppermute(shard, axis, [(i, (i + by) % count) for i in range(count)])


def layer_norm(values_in, gain_vec, bias_vec):
    centered = values_in - jnp.mean(values_in, axis=-1, keepdims=True)
    variance = jnp.mean(centered * centered, axis=-1, keepdims=True)
    return centered * lax.rsqrt(variance + EPSILON) * gain_vec + bias_vec


def rotary_tables(position_ids):
    half_dim = ROTARY // 2
    inverse_freq = 1.0 / 10000.0 ** (jnp.arange(half_dim, dtype=jnp.float32) * (2.0 / ROTARY))
    angles = position_ids.astype(jnp.float32)[..., None] * inverse_freq
    return (jnp.cos(angles), jnp.sin(angles))


def rotate(field_in, cosine, sine_table):
    half_dim = cosine.shape[-1]
    lead_part = field_in[..., :half_dim]
    second = field_in[..., half_dim : 2 * half_dim]
    remain = field_in[..., 2 * half_dim :]
    cos_wide = cosine[..., None, :]
    sin_wide = sine_table[..., None, :]
    return jnp.concatenate(
        [
            lead_part * cos_wide - second * sin_wide,
            second * cos_wide + lead_part * sin_wide,
            remain,
        ],
        axis=-1,
    )


def gelu_exact(field_in):
    return jax.nn.gelu(field_in, approximate=False)


MESH = pl.DeviceIdType.MESH
LOW = jnp.bfloat16
FULL = jnp.float32
ROWS_CONTRACT = (((0,), (0,)), ((), ()))
COLS_CONTRACT = (((1,), (1,)), ((), ()))
INV_ROOT_TWO = 0.7071067811865476
INV_ROOT_TWO_PI = 0.3989422804014327
CHUNK = 48
LAG = 2


def dot(lhs, rhs, dims=(((1,), (0,)), ((), ()))):
    return lax.dot_general(lhs, rhs, dims, preferred_element_type=FULL)


def flip(index, bits):
    for power in (1, 2, 4, 8):
        if bits & power:
            index = index + power - 2 * power * lax.rem(lax.div(index, power), 2)
    return index


def at16(value):
    return pl.multiple_of(value, 16)


def at128(value):
    return pl.multiple_of(value, 128)


def rotary_constants(blocks, block_len):
    lane = np.arange(128) % HEAD_DIM
    half = ROTARY // 2
    turning = lane < ROTARY
    freq = np.where(turning, 10000.0 ** (-(lane % half) * (2.0 / ROTARY)), 0.0)
    sign = np.where(lane < half, -1.0, 1.0) * turning
    offset = np.arange(block_len)[:, None] * freq
    start = (np.arange(blocks) * block_len)[:, None] * freq
    parts = (np.cos(offset), np.sin(offset) * sign, np.cos(start), np.sin(start) * sign)
    return np.concatenate(parts).astype(np.float32)


def fused_body(names, *refs):
    (
        x_ref, pos_ref, gain1_ref, bias1_ref, gain2_ref, bias2_ref, qkvb_ref, upb_ref, rot_ref,
        cot_hbm, wqkv_hbm, wup_hbm, wout_hbm, wdn_hbm,
        y_ref, dx_ref, fin_ref, qkvfin_ref, early_ref, late_ref,
    ) = refs[:20]
    scratch = dict(zip(names, refs[20:]))
    run_layer(
        x_ref, pos_ref, gain1_ref, bias1_ref, gain2_ref, bias2_ref, qkvb_ref, upb_ref, rot_ref,
        cot_hbm, wqkv_hbm, wup_hbm, wout_hbm, wdn_hbm,
        y_ref, dx_ref, fin_ref, qkvfin_ref, early_ref, late_ref, **scratch,
    )


def run_layer(
    x_ref, pos_ref, gain1_ref, bias1_ref, gain2_ref, bias2_ref, qkvb_ref, upb_ref, rot_ref,
    cot_hbm, wqkv_hbm, wup_hbm, wout_hbm, wdn_hbm,
    y_ref, dx_ref, fin_ref, qkvfin_ref, early_ref, late_ref,
    *,
    wq, wraw, wup, wout, wdn, n1, n2, cot, pos_tx, pos_rx, pos_sm, qkv, q_s, k_s, v_s, do_tx, do_mid, do_rx, do_s,
    o_s, dq_s, dk_s, dv_s, gp_s, gp_e, o_tx, o_rx, attn, a1_p, a1_d2d, a1_own, a1_tx_r, a1_tx_l, a1_rx_r, a1_rx_l,
    gq_tx, gq_rx, out_acc, a2_acc, out_tx, out_rx, a2_tx, a2_rx, gd16, gd_rx, gu16, gu_rx, gu_tx,
    go16, go_rx, line_own, line_rx, line_near, line_far, early_a, early_rx, early_b,
    late_a, late_rx, late_b, ssem, rsem, lsem,
):
    shards = lax.axis_size("shard")
    ctxs = lax.axis_size("ctx")
    s = lax.axis_index("shard")
    i = lax.axis_index("ctx")
    c = lax.rem(i, 2)
    z = lax.div(i, 2)
    other = 1 - c
    Z = ctxs // 2
    planes = range(1, shards)
    mates = range(1, ctxs)
    block = x_ref.shape[0]
    width = x_ref.shape[1]
    rows = width // shards
    half_rows = rows // 2
    half_width = width // 2
    sent = []
    used = [0]
    always = None

    def channels(count):
        first = used[0]
        used[0] += count
        return first

    def copy_of(send_k, recv_k, src, dst, device):
        return pltpu.make_async_remote_copy(
            src_ref=src,
            dst_ref=dst,
            send_sem=ssem.at[send_k],
            recv_sem=rsem.at[recv_k],
            device_id=device,
            device_id_type=MESH,
        )

    def send(k, src, dst, device, recv_k=None, when=always):
        copy = copy_of(k, k if recv_k is None else recv_k, src, dst, device)
        sent.append((copy, when))
        if when is always:
            copy.start()
        else:
            pl.when(when)(copy.start)

    def arrived(k, dst):
        copy_of(k, k, dst, dst, {"ctx": flip(i, 1)}).wait_recv()

    def plane(d):
        return flip(s, d)

    def mate(e):
        return flip(i, e)

    partner = {"ctx": flip(i, 1)}
    right = {"ctx": i + 2}
    left = {"ctx": i - 2}
    has_left = z > 0
    has_right = z < Z - 1

    loads = []

    def load(src, dst):
        copy = pltpu.make_async_copy(src, dst, lsem.at[len(loads)])
        copy.start()
        loads.append(copy)

    my_rows = pl.ds(at16(s * rows), rows)
    first = HEAD_DIM * (3 * z + c)
    base = jnp.minimum(128 * lax.div(first, 128), width - 256)
    for part in range(3):
        load(wqkv_hbm.at[:, pl.ds(at128(width * part + base), 256)], wraw.at[part])
    load(cot_hbm, cot.at[pl.ds(0, block)])
    load(wout_hbm.at[pl.ds(0, 128)], wout.at[pl.ds(0, 128)])
    load(wout_hbm.at[pl.ds(HEAD_DIM, 128)], wout.at[pl.ds(128, 128)])
    load(wup_hbm.at[:, pl.ds(at128(s * width), width)], wup.at[my_rows])
    load(wdn_hbm, wdn)

    barrier = pltpu.get_barrier_semaphore()
    for d in range(shards):
        for e in range(ctxs):
            if d or e:
                pl.semaphore_signal(
                    barrier,
                    inc=1,
                    device_id={"shard": plane(d), "ctx": mate(e)},
                    device_id_type=MESH,
                )
    pl.semaphore_wait(barrier, shards * ctxs - 1)

    K_COT = channels(shards)
    K_WQ = channels(shards)
    K_WU = channels(shards)
    K_WU2 = channels(shards)
    K_N2 = channels(shards)
    K_POS = channels(ctxs)
    for d in planes:
        send(K_COT + d, cot_hbm, cot.at[pl.ds(block * d, block)], {"shard": plane(d)})

    def two_heads(here, there):
        wide = lax.broadcasted_iota(jnp.int32, here.shape, 1)
        turned = jnp.where(
            wide < HEAD_DIM, pltpu.roll(here, HEAD_DIM, 1), pltpu.roll(there, HEAD_DIM, 1)
        )
        return jnp.where(
            first == base, here, jnp.where(first == base + HEAD_DIM, turned, there)
        )

    for copy in loads[:3]:
        copy.wait()
    for part in range(3):
        raw = wraw[part].astype(FULL)
        wq[my_rows, 128 * part : 128 * (part + 1)] = two_heads(raw[:, :128], raw[:, 128:]).astype(LOW)
    qkv_bias = jnp.concatenate(
        [
            two_heads(
                jnp.broadcast_to(qkvb_ref[pl.ds(at128(width * part + base), 128)][None, :], (8, 128)),
                jnp.broadcast_to(qkvb_ref[pl.ds(at128(width * part + base + 128), 128)][None, :], (8, 128)),
            )
            for part in range(3)
        ],
        axis=1,
    )[:1]
    gain1, gain2 = gain1_ref[...][None, :], gain2_ref[...][None, :]
    bias1, bias2 = bias1_ref[...][None, :], bias2_ref[...][None, :]
    pos_tx[...] = jnp.broadcast_to(pos_ref[...], pos_tx.shape)
    x = x_ref[...].astype(FULL)
    mean = jnp.mean(x, axis=-1, keepdims=True)
    centered = x - mean
    r = lax.rsqrt(jnp.mean(centered * centered, axis=-1, keepdims=True) + EPSILON)
    normal = centered * r

    def tokens(j):
        return pl.ds(at128(block * j), block)

    n1[tokens(i)] = (normal * gain1 + bias1).astype(LOW)
    n2[pl.ds(0, block)] = (normal * gain2 + bias2).astype(LOW)
    pos_rx[i] = pos_tx[...]
    for e in mates:
        send(K_POS + e, pos_tx, pos_rx.at[i], {"ctx": mate(e)})

    class Relay:
        def __init__(self, piece):
            self.piece = piece
            self.direct = channels(Z)
            self.across = channels(2 * Z)
            self.to_right = channels(Z)
            self.to_left = channels(Z)

        def begin(self):
            mine = self.piece(i)
            send(self.to_right, mine, mine, right, self.direct + z, has_right)
            send(self.to_left, mine, mine, left, self.direct + z, has_left)
            send(self.across, mine, mine, partner, self.across + z)

        def step(self, k):
            @pl.when(z >= k)
            def _():
                arrived(self.direct + z - k, self.piece(i - 2 * k))

            piece = self.piece(i - 2 * k)
            if k < Z - 1:
                send(self.to_right + k, piece, piece, right, self.direct + z - k, (z >= k) & has_right)
            send(self.across + 2 * k - 1, piece, piece, partner, self.across + z - k, z >= k)

            @pl.when(z + k < Z)
            def _():
                arrived(self.direct + z + k, self.piece(i + 2 * k))

            piece = self.piece(i + 2 * k)
            if k < Z - 1:
                send(self.to_left + k, piece, piece, left, self.direct + z + k, (z + k < Z) & has_left)
            send(self.across + 2 * k, piece, piece, partner, self.across + z + k, z + k < Z)

        def end(self):
            for to in range(Z):
                arrived(self.across + to, self.piece(2 * to + other))

    normed = Relay(lambda j: n1.at[tokens(j)])
    normed.begin()
    for copy in loads[3:]:
        copy.wait()

    K_DO = channels(ctxs)
    K_DOS = channels(ctxs)
    K_DOM = channels(shards)

    def grad_attn(d):
        if d:
            arrived(K_COT + d, cot.at[pl.ds(block * d, block)])
        field = dot(cot[pl.ds(block * d, block)], wout[...], COLS_CONTRACT)
        for core in range(2):
            do_tx[d, core] = field[:, 128 * core : 128 * (core + 1)].astype(LOW)
        if d:
            send(K_DOM + d, do_tx.at[d], do_mid.at[d], {"shard": plane(d)})
        else:
            do_mid[0] = do_tx[0]

    def grad_attn_on(d):
        if d:
            arrived(K_DOM + d, do_mid.at[d])
        for core in range(2):
            target = 2 * plane(d) + core
            piece = do_mid.at[d, core]
            send(K_DOS + 2 * d + core, piece, do_rx.at[i], {"ctx": target}, K_DO + i, i != target)

            @pl.when(i == target)
            def _():
                do_rx[i] = do_mid[d, core]

    def send_wq(d):
        send(K_WQ + d, wq.at[my_rows], wq.at[my_rows], {"shard": plane(d)})

    near_planes, last_plane = planes[:-1], planes[-1]
    for d in (0, *near_planes):
        grad_attn(d)
    for d in near_planes:
        send_wq(d)
    normed.step(1)
    grad_attn_on(0)
    grad_attn(last_plane)
    send_wq(last_plane)
    my_half = pl.ds(at16(s * rows + c * half_rows), half_rows)
    for d in planes:
        send(
            K_WU + d,
            wup_hbm.at[
                pl.ds(at16(c * half_rows), half_rows), pl.ds(at128(plane(d) * width), width)
            ],
            wup.at[my_half],
            {"shard": plane(d)},
        )
    for d in planes:
        send(K_N2 + d, n2.at[pl.ds(0, block)], n2.at[pl.ds(block * d, block)], {"shard": plane(d)})
    for d in near_planes:
        grad_attn_on(d)
    normed.step(2)
    for e in mates:
        arrived(K_POS + e, pos_rx.at[mate(e)])
    to_scalar = pltpu.make_async_copy(pos_rx, pos_sm, lsem.at[len(loads)])
    to_scalar.start()
    grad_attn_on(last_plane)
    for k in range(3, Z):
        normed.step(k)
    normed.end()
    to_scalar.wait()
    rank = [lax.div(pos_sm[j, 0, 0], block) for j in range(ctxs)]
    place = []
    for g in range(ctxs):
        found = jnp.int32(0)
        for j in range(1, ctxs):
            found = found + j * (rank[j] == g).astype(jnp.int32)
        place.append(lax.rem(found, ctxs))

    for d in planes:
        arrived(K_WQ + d, wq.at[pl.ds(at16(plane(d) * rows), rows)])

    @pl.loop(0, ctxs // 2)
    def _(m):
        here = pl.ds(at128(m * 2 * block), 2 * block)
        qkv[pl.ds(2 * m, 2)] = dot(n1[here], wq[...]).reshape(2, block, 384)

    lane = lax.broadcasted_iota(jnp.int32, (block, 128), 1)
    leads = lax.rem(lane, HEAD_DIM) < ROTARY // 2

    def across(field):
        return jnp.where(
            leads,
            pltpu.roll(field, 128 - ROTARY // 2, 1),
            pltpu.roll(field, ROTARY // 2, 1),
        )

    def tables(g):
        off_cos, off_sin = rot_ref[pl.ds(0, block)], rot_ref[pl.ds(block, block)]
        start_cos = rot_ref[pl.ds(2 * block + g, 1)]
        start_sin = rot_ref[pl.ds(2 * block + ctxs + g, 1)]
        cosine = start_cos * off_cos - start_sin * off_sin
        sine = start_sin * off_cos + start_cos * off_sin
        return cosine, sine

    for j in range(ctxs):

        @pl.when(j != i)
        def _():
            arrived(K_DO + j, do_rx.at[j])

    for g in range(ctxs):
        here = pl.ds(block * g, block)
        field = qkv[place[g]] + qkv_bias
        cosine, sine = tables(g)
        q_raw, k_raw = field[:, :128], field[:, 128:256]
        turned_q = (q_raw * cosine + across(q_raw) * sine).astype(LOW)
        q_s[here] = turned_q * jnp.asarray(HEAD_DIM**-0.5, LOW)
        k_s[here] = (k_raw * cosine + across(k_raw) * sine).astype(LOW)
        v_s[here] = field[:, 256:].astype(LOW)
        do_s[here] = do_rx[place[g]]

    o_s[...] = jnp.zeros_like(o_s)
    dq_s[...] = jnp.zeros_like(dq_s)
    dk_s[...] = jnp.zeros_like(dk_s)
    dv_s[...] = jnp.zeros_like(dv_s)

    @pl.loop(0, 2)
    def _(h):
        mine = lax.div(lane, HEAD_DIM) == h
        for g in range(ctxs):
            share = 0 if g % 4 in (0, 3) else 1

            @pl.when((h == c) | (c == share))
            def _():
                here = pl.ds(block * g, block)
                upto = pl.ds(0, block * (g + 1))
                span = block * (g + 1)
                zero = jnp.zeros((block, 128), LOW)
                q_h = jnp.where(mine, q_s[here], zero)
                do_h = jnp.where(mine, do_s[here], zero)
                scores = dot(q_h, k_s[upto], COLS_CONTRACT)
                token = lax.broadcasted_iota(jnp.int32, (block, span), 0) + block * g
                key = lax.broadcasted_iota(jnp.int32, (block, span), 1)
                masked = jnp.where(key <= token, scores, NEGATIVE)
                top = jnp.max(masked, axis=-1, keepdims=True)
                weight = jnp.exp(masked - top)
                probability = weight * (1.0 / jnp.sum(weight, axis=-1, keepdims=True))
                prob_low = probability.astype(LOW)
                attended = jnp.where(mine, dot(prob_low, v_s[upto]), 0.0)
                o_s[g] += attended
                grad_prob = dot(do_h, v_s[upto], COLS_CONTRACT)
                row_delta = jnp.sum(do_h.astype(FULL) * attended, axis=-1, keepdims=True)
                grad_score = (probability * (grad_prob - row_delta)).astype(LOW)
                dq_s[here] += jnp.where(mine, dot(grad_score, k_s[upto]), 0.0)
                dk_s[upto] += dot(grad_score, q_h, ROWS_CONTRACT)
                dv_s[upto] += dot(prob_low, do_h, ROWS_CONTRACT)

    K_O = channels(2 * shards)
    K_OS = channels(ctxs)
    for j in range(ctxs):
        o_tx[j] = o_s[rank[j]].astype(LOW)
        away = (s != z) | (j != i)
        send(K_OS + j, o_tx.at[j], o_rx.at[2 * s + c], {"shard": z, "ctx": j}, K_O + 2 * s + c, away)

        @pl.when(jnp.logical_not(away))
        def _():
            o_rx[2 * s + c] = o_tx[j]

    bias_sum = jnp.zeros((1, 384), FULL)
    for g in range(ctxs):
        here = pl.ds(block * g, block)
        cosine, sine = tables(g)
        dq = dq_s[here] * (HEAD_DIM**-0.5)
        dk = dk_s[here]
        parts = (dq * cosine - across(dq) * sine, dk * cosine - across(dk) * sine, dv_s[here])
        part = jnp.concatenate(parts, axis=1).astype(LOW)
        gp_s[g] = part
        bias_sum = bias_sum + jnp.sum(part.astype(FULL), axis=0, keepdims=True)
    for j in range(ctxs):
        gp_e[pl.ds(block * j, block)] = gp_s[rank[j]]

    @pl.loop(0, ctxs // 2)
    def _(m):
        here = pl.ds(at128(m * 2 * block), 2 * block)
        a1_p[pl.ds(2 * m, 2)] = (
            dot(gp_e[here], wq[...], COLS_CONTRACT).astype(LOW).reshape(2, block, width)
        )

    K_A1D = channels(Z)
    for t in range(Z):
        send(K_A1D + t, a1_p.at[2 * t + other], a1_d2d.at[t], partner)

    @pl.loop(0, width // 256)
    def _(m):
        here = pl.ds(at128(m * 256), 256)
        gq_tx[here] = dot(n1[:, here], gp_e[...], ROWS_CONTRACT).astype(LOW)

    K_GQ = channels(shards)
    for d in planes:
        send(
            K_GQ + d, gq_tx.at[pl.ds(at16(plane(d) * rows), rows)], gq_rx.at[d], {"shard": plane(d)}
        )

    for t in range(Z):
        arrived(K_A1D + t, a1_d2d.at[t])
        a1_own[t] = (a1_p[2 * t + c].astype(FULL) + a1_d2d[t].astype(FULL)).astype(LOW)

    K_A1R = channels(Z)
    K_A1L = channels(Z)

    def a1_ends():
        for t in reversed(range(1, Z)):
            send(K_A1R + t, a1_own.at[t], a1_rx_r.at[t], right, None, z == 0)
        for t in range(Z - 1):
            send(K_A1L + t, a1_own.at[t], a1_rx_l.at[t], left, None, z == Z - 1)

    low_side = z < Z // 2

    def a1_right(t, here):
        when = (z > 0) & (z < t) & here

        @pl.when(when)
        def _():
            arrived(K_A1R + t, a1_rx_r.at[t])
            a1_tx_r[t] = (a1_own[t].astype(FULL) + a1_rx_r[t].astype(FULL)).astype(LOW)

        send(K_A1R + t, a1_tx_r.at[t], a1_rx_r.at[t], right, None, when)

    def a1_left(t, here):
        when = (z < Z - 1) & (z > t) & here

        @pl.when(when)
        def _():
            arrived(K_A1L + t, a1_rx_l.at[t])
            a1_tx_l[t] = (a1_own[t].astype(FULL) + a1_rx_l[t].astype(FULL)).astype(LOW)

        send(K_A1L + t, a1_tx_l.at[t], a1_rx_l.at[t], left, None, when)

    a1_ends()

    @pl.when(z == 0)
    def _():
        a1_rx_r[0] = jnp.zeros((block, width), LOW)

    @pl.when(z == Z - 1)
    def _():
        a1_rx_l[Z - 1] = jnp.zeros((block, width), LOW)

    early_a[...] = jnp.zeros_like(early_a)
    for d in planes:
        arrived(K_WU + d, wup.at[pl.ds(at16(plane(d) * rows + c * half_rows), half_rows)])
        part = wup.at[pl.ds(at16(plane(d) * rows + c * half_rows), half_rows)]
        send(K_WU2 + d, part, part, partner)
    for d in planes:
        arrived(K_N2 + d, n2.at[pl.ds(block * d, block)])
    for d in planes:
        arrived(K_WU2 + d, wup.at[pl.ds(at16(plane(d) * rows + other * half_rows), half_rows)])
    out_acc[...] = jnp.zeros_like(out_acc)
    a2_acc[...] = jnp.zeros_like(a2_acc)

    @pl.loop(0, width // 256)
    def _(t):
        units = pl.ds(at128(t * 256), 256)
        bias = upb_ref[pl.ds(at128(s * width + t * 256), 256)][None, :]
        pre = dot(n2[...], wup[:, units]) + bias
        cdf = 0.5 * (1.0 + lax.erf(pre * INV_ROOT_TWO))
        hidden = (pre * cdf).astype(LOW)
        slope = cdf + pre * (jnp.exp(-0.5 * pre * pre) * INV_ROOT_TWO_PI)
        grad_hidden = dot(cot[...], wdn[units], COLS_CONTRACT)
        grad_pre = (grad_hidden * slope).astype(LOW)
        early_a[pl.ds(t, 1)] = jnp.sum(grad_pre.astype(FULL), axis=0, keepdims=True)
        out_acc[...] += dot(hidden, wdn[units])
        a2_acc[...] += dot(grad_pre, wup[:, units], COLS_CONTRACT)
        gd16[units] = dot(hidden, cot[...], ROWS_CONTRACT).astype(LOW)
        gu16[:, units] = dot(n2[...], grad_pre, ROWS_CONTRACT).astype(LOW)

    K_GD = channels(1)
    K_GU = channels(shards)
    K_GUX = channels(shards)
    K_OUT = channels(shards)
    K_A2 = channels(shards)
    K_GO = channels(1)

    def rows_of(d, core):
        return pl.ds(at16(plane(d) * rows + core * half_rows), half_rows)

    for d in range(shards):
        send(K_GU + d, gu16.at[rows_of(d, other)], gu_rx.at[d], partner)
    send(K_GD, gd16.at[pl.ds(at16(other * half_width), half_width)], gd_rx, partner)
    for d in planes:
        a2_tx[d] = a2_acc[pl.ds(block * d, block)].astype(LOW)

    for seq in range(shards):
        for core in range(2):
            k = 2 * seq + core

            @pl.when((seq != s) | (2 * s + core != i))
            def _():
                arrived(K_O + k, o_rx.at[k])

            attn[pl.ds(block * seq, block), 128 * core : 128 * (core + 1)] = o_rx[k]
    for d in range(shards):
        mine = attn[tokens(plane(d))]
        total = out_acc[pl.ds(block * d, block)] + dot(mine, wout[...])
        if d:
            out_tx[d] = total.astype(LOW)
        else:
            out_acc[pl.ds(0, block)] = total
    go = dot(attn[tokens(plane(0))], cot[pl.ds(0, block)], ROWS_CONTRACT)
    for d in planes:
        go = go + dot(attn[tokens(plane(d))], cot[pl.ds(block * d, block)], ROWS_CONTRACT)
    go16[pl.ds(0, HEAD_DIM)] = go[:HEAD_DIM].astype(LOW)
    go16[pl.ds(HEAD_DIM, HEAD_DIM)] = (
        go[HEAD_DIM : 2 * HEAD_DIM] + go[2 * HEAD_DIM : 3 * HEAD_DIM]
    ).astype(LOW)
    go16[pl.ds(2 * HEAD_DIM, HEAD_DIM)] = go[3 * HEAD_DIM :].astype(LOW)
    send(K_GO, go16.at[pl.ds(at16(other * half_rows), half_rows)], go_rx, partner)

    own_gq = gq_tx[my_rows].astype(FULL)
    for d in planes:
        arrived(K_GQ + d, gq_rx.at[d])
        own_gq = own_gq + gq_rx[d].astype(FULL)
    qkvfin_ref[i] = own_gq.astype(LOW)
    spread = Relay(lambda j: qkvfin_ref.at[j])

    spread.begin()
    UP = half_width + half_rows

    def up_rows(index):
        return pl.ds(at16(UP + index * half_rows), half_rows)

    for d in (*planes, 0):
        arrived(K_GU + d, gu_rx.at[d])
        total = (gu16[rows_of(d, c)].astype(FULL) + gu_rx[d].astype(FULL)).astype(LOW)
        if d:
            gu_tx[d] = total
            send(K_GUX + d, gu_tx.at[d], line_own.at[up_rows(s)], {"shard": plane(d)})
        else:
            line_own[up_rows(s)] = total
    for d in planes:
        send(K_A2 + d, a2_tx.at[d], a2_rx.at[d], {"shard": plane(d)})
    for d in planes:
        send(K_OUT + d, out_tx.at[d], out_rx.at[d], {"shard": plane(d)})

    is_end = (z == 0) | (z == Z - 1)
    is_mid = jnp.logical_not(is_end)
    is_centre = (z == Z // 2 - 1) | (z == Z // 2)
    inward = jnp.where(z < Z // 2, 2, -2)
    inner = {"ctx": i + inward}
    outer = {"ctx": i - inward}
    to_inner = jnp.where(is_centre, 1, 0)
    line_rows = half_width + half_rows + shards * half_rows
    chunks = line_rows // CHUNK
    first_up = UP // CHUNK
    K_OUTER = channels(chunks)
    K_INNER = channels(chunks)
    K_NEAR = channels(chunks)
    K_FAR = channels(chunks)
    K_FIN = channels(chunks)

    def span_of(q):
        return pl.ds(q * CHUNK, CHUNK)

    def near_end(q):
        send(
            K_NEAR + q,
            line_own.at[span_of(q)],
            line_rx.at[to_inner, span_of(q)],
            inner,
            K_OUTER + chunks * to_inner + q,
            is_end,
        )

    def near_mid(q):
        @pl.when(is_mid)
        def _():
            arrived(K_OUTER + q, line_rx.at[0, span_of(q)])
            line_near[span_of(q)] = (
                line_rx[0, span_of(q)].astype(FULL) + line_own[span_of(q)].astype(FULL)
            ).astype(LOW)

        send(
            K_INNER + q,
            line_near.at[span_of(q)],
            line_rx.at[to_inner, span_of(q)],
            inner,
            K_OUTER + chunks * to_inner + q,
            is_mid,
        )

    def far(q):
        arrived(K_INNER + q, line_rx.at[1, span_of(q)])
        beyond = line_rx[1, span_of(q)].astype(FULL) + line_own[span_of(q)].astype(FULL)

        @pl.when(is_mid)
        def _():
            line_far[span_of(q)] = beyond.astype(LOW)

        send(
            K_FAR + q, line_far.at[span_of(q)], line_rx.at[1, span_of(q)], outer, K_INNER + q, is_mid
        )
        fin_ref[c, span_of(q)] = (beyond + line_rx[0, span_of(q)].astype(FULL)).astype(LOW)
        send(K_FIN + q, fin_ref.at[c, span_of(q)], fin_ref.at[c, span_of(q)], partner)

    @pl.when(is_end)
    def _():
        line_rx[0] = jnp.zeros((line_rows, width), LOW)

    arrived(K_GD, gd_rx)
    line_own[pl.ds(0, half_width)] = (
        gd16[pl.ds(at16(c * half_width), half_width)].astype(FULL) + gd_rx[...].astype(FULL)
    ).astype(LOW)
    for q in range(half_width // CHUNK):
        near_end(q)
    arrived(K_GO, go_rx)
    line_own[pl.ds(half_width, half_rows)] = (
        go16[pl.ds(at16(c * half_rows), half_rows)].astype(FULL) + go_rx[...].astype(FULL)
    ).astype(LOW)
    for q in range(half_width // CHUNK, first_up):
        near_end(q)

    for t in reversed(range(1, Z)):
        a1_right(t, low_side)
        a1_left(Z - 1 - t, jnp.logical_not(low_side))
    for t in reversed(range(1, Z)):
        a1_right(t, jnp.logical_not(low_side))
        a1_left(Z - 1 - t, low_side)
    spread.step(1)
    K_E = channels(ctxs)
    K_EX = channels(shards)
    early_a[3:4] = bias_sum[:, :256]
    early_a[4:5, 0:128] = bias_sum[:, 256:]
    for e in mates:
        send(K_E + e, early_a, early_rx.at[e], {"ctx": mate(e)})
    early_rx[0] = early_a[...]

    for q in range(2):
        near_mid(q)
    spread.step(2)
    for q in range(2, 4):
        near_mid(q)
    for d in planes:
        arrived(K_GUX + d, line_own.at[up_rows(plane(d))])
    for q in range(first_up, chunks):
        near_end(q)
    near_mid(4)
    far(0)
    near_mid(5)
    far(1)
    near_mid(6)
    far(2)
    near_mid(7)
    far(3)
    near_mid(8)
    far(4)
    near_mid(9)
    far(5)
    a1 = a1_own[z].astype(FULL)

    @pl.when(has_left)
    def _():
        arrived(K_A1R + z, a1_rx_r.at[z])

    @pl.when(has_right)
    def _():
        arrived(K_A1L + z, a1_rx_l.at[z])

    a1 = a1 + a1_rx_r[z].astype(FULL) + a1_rx_l[z].astype(FULL)
    a2 = a2_acc[pl.ds(0, block)]
    for d in planes:
        arrived(K_A2 + d, a2_rx.at[d])
        a2 = a2 + a2_rx[d].astype(FULL)
    sums = (a1 * normal, a1, a2 * normal, a2)
    for k, field in enumerate(sums):
        total = jnp.sum(field, axis=0, keepdims=True)
        late_a[2 * k : 2 * k + 1] = total[:, :half_width]
        late_a[2 * k + 1 : 2 * k + 2] = total[:, half_width:]
    K_L = channels(ctxs)
    K_LX = channels(shards)
    for e in mates:
        send(K_L + e, late_a, late_rx.at[e], {"ctx": mate(e)})
    late_rx[0] = late_a[...]
    mixed = a1 * gain1 + a2 * gain2
    back = r * (
        mixed
        - jnp.mean(mixed, axis=-1, keepdims=True)
        - normal * jnp.mean(mixed * normal, axis=-1, keepdims=True)
    )
    dx_ref[...] = (cot[pl.ds(0, block)].astype(FULL) + back).astype(LOW)
    for q in range(10, 12):
        near_mid(q)
        far(q - 4)
    for q in range(12, 15):
        near_mid(q)
        far(q - 4)
    total = x_ref[...].astype(FULL) + out_acc[pl.ds(0, block)]
    for d in planes:
        arrived(K_OUT + d, out_rx.at[d])
        total = total + out_rx[d].astype(FULL)
    y_ref[...] = total.astype(LOW)
    for e in mates:
        arrived(K_E + e, early_rx.at[e])
    summed = early_rx[0]
    for e in mates:
        summed = summed + early_rx[e]
    early_b[0, 0:8] = summed
    for j in range(ctxs):
        early_b[0, 8 + 2 * j : 10 + 2 * j] = early_rx[flip(i, j), 3:5]
    for e in mates:
        arrived(K_L + e, late_rx.at[e])
    summed = late_rx[0]
    for e in mates:
        summed = summed + late_rx[e]
    late_b[0] = summed
    for d in planes:
        send(K_EX + d, early_b.at[0], early_b.at[d], {"shard": plane(d)})
        send(K_LX + d, late_b.at[0], late_b.at[d], {"shard": plane(d)})
    for q in range(15, chunks):
        near_mid(q)
        far(q - 4)
    for q in range(chunks - 4, chunks):
        far(q)
    for d in planes:
        arrived(K_EX + d, early_b.at[d])
        arrived(K_LX + d, late_b.at[d])
    whole = early_b[0]
    late = late_b[0]
    for d in planes:
        whole = whole + early_b[d]
        late = late + late_b[d]
    late_ref[...] = late
    early_ref[0:24] = whole
    for j in range(shards):
        early_ref[24 + 8 * j : 32 + 8 * j] = early_b[flip(s, j), 0:8]
    for k in range(3, Z):
        spread.step(k)
    spread.end()
    for q in range(chunks):
        arrived(K_FIN + q, fin_ref.at[other, span_of(q)])
    assert used[0] <= ssem.shape[0]
    for copy, when in sent:
        if when is always:
            copy.wait_send()
        else:
            pl.when(when)(copy.wait_send)


def ring_on_device(
    layer_input,
    positions,
    cotangent,
    ln1_gain,
    ln1_bias,
    ln2_gain,
    ln2_bias,
    w_qkv,
    qkv_bias,
    w_out,
    w_up,
    up_bias,
    w_down,
):
    seqs_here, block_len, feature_count = layer_input.shape
    row_count = seqs_here * block_len
    head_count = HEADS
    head_size = HEAD_DIM
    score_scale = head_size ** (-0.5)
    whole_qkv, whole_out, whole_up, whole_down = (
        lax.all_gather(w_qkv, "shard", axis=0, tiled=True),
        lax.all_gather(w_out, "shard", axis=0, tiled=True),
        lax.all_gather(w_up, "shard", axis=0, tiled=True),
        lax.all_gather(w_down, "shard", axis=0, tiled=True),
    )
    all_positions = lax.all_gather(positions, "ctx", axis=1, tiled=True)
    cycle_size = lax.axis_size("ctx")
    my_index = lax.axis_index("ctx")
    inputs = layer_input.astype(jnp.float32).reshape(row_count, feature_count)
    normed_one = layer_norm(inputs, ln1_gain, ln1_bias).astype(jnp.bfloat16)
    normed_two = layer_norm(inputs, ln2_gain, ln2_bias).astype(jnp.bfloat16)
    projected = jnp.dot(normed_one, whole_qkv, preferred_element_type=jnp.float32) + qkv_bias
    split_heads = projected.reshape(seqs_here, block_len, 3, head_count, head_size)
    cosine, sine_table = rotary_tables(positions)
    queries = rotate(split_heads[:, :, 0], cosine, sine_table).astype(jnp.bfloat16)
    key_rows = rotate(split_heads[:, :, 1], cosine, sine_table).astype(jnp.bfloat16)
    value_rows = split_heads[:, :, 2].astype(jnp.bfloat16)
    top_query = jnp.max(positions)

    def attend_block(running, key_blk, value_blk, key_pos):

        def attend_update(current):
            run_max, run_sum, run_acc = current
            scores = (
                jnp.einsum("sqhd,skhd->shqk", queries, key_blk, preferred_element_type=jnp.float32)
                * score_scale
            )
            allowed = key_pos[:, None, None, :] <= positions[:, None, :, None]
            masked = jnp.where(allowed, scores, NEGATIVE)
            new_max = jnp.maximum(run_max, jnp.max(masked, axis=-1))
            shrink = jnp.exp(run_max - new_max)
            weights_now = jnp.where(allowed, jnp.exp(masked - new_max[..., None]), 0.0)
            run_sum = run_sum * shrink + jnp.sum(weights_now, axis=-1)
            added_term = jnp.einsum(
                "shqk,skhd->sqhd",
                weights_now.astype(jnp.bfloat16),
                value_blk,
                preferred_element_type=jnp.float32,
            )
            run_acc = run_acc * jnp.transpose(shrink, (0, 2, 1))[..., None] + added_term
            return (new_max, run_sum, run_acc)

        return lax.cond(
            jnp.min(key_pos) <= top_query, attend_update, lambda unchanged: unchanged, running
        )

    initial = (
        jnp.full((seqs_here, head_count, block_len), NEGATIVE, jnp.float32),
        jnp.zeros((seqs_here, head_count, block_len), jnp.float32),
        jnp.zeros((seqs_here, block_len, head_count, head_size), jnp.float32),
    )
    own_block = attend_block(initial, key_rows, value_rows, positions)

    def cycle_forward(turn_index, carried):
        current, key_cur, value_cur = carried
        key_cur, value_cur = shifted((key_cur, value_cur), "ctx", 1)
        source = (my_index - turn_index) % cycle_size
        key_pos = lax.dynamic_slice_in_dim(all_positions, source * block_len, block_len, 1)
        return (attend_block(current, key_cur, value_cur, key_pos), key_cur, value_cur)

    (run_max, run_sum, run_acc), unused_key, unused_value = lax.fori_loop(
        1, cycle_size, cycle_forward, (own_block, key_rows, value_rows)
    )
    attn_vals = run_acc / jnp.transpose(run_sum, (0, 2, 1))[..., None]
    log_total = run_max + jnp.log(run_sum)
    attn_low = attn_vals.astype(jnp.bfloat16).reshape(row_count, feature_count)
    attn_branch = jnp.dot(attn_low, whole_out, preferred_element_type=jnp.float32)
    hidden_pre = jnp.dot(normed_two, whole_up, preferred_element_type=jnp.float32) + up_bias
    hidden_low = gelu_exact(hidden_pre).astype(jnp.bfloat16)
    mlp_branch = jnp.dot(hidden_low, whole_down, preferred_element_type=jnp.float32)
    layer_output = (
        (inputs + attn_branch + mlp_branch)
        .astype(jnp.bfloat16)
        .reshape(seqs_here, block_len, feature_count)
    )
    cot_low = cotangent.reshape(row_count, feature_count)
    cot_full = cot_low.astype(jnp.float32)
    grad_down = jnp.einsum("rf,rd->fd", hidden_low, cot_low, preferred_element_type=jnp.float32)
    grad_hidden = jnp.einsum("rd,fd->rf", cot_low, whole_down, preferred_element_type=jnp.float32)
    unused_gelu, gelu_back = jax.vjp(gelu_exact, hidden_pre)
    grad_pre = gelu_back(grad_hidden)[0].astype(jnp.bfloat16)
    grad_up_bias = jnp.sum(grad_pre.astype(jnp.float32), axis=0)
    grad_up = jnp.einsum("rd,rf->df", normed_two, grad_pre, preferred_element_type=jnp.float32)
    grad_two = jnp.einsum("rf,df->rd", grad_pre, whole_up, preferred_element_type=jnp.float32)
    grad_out = jnp.einsum("rd,re->de", attn_low, cot_low, preferred_element_type=jnp.float32)
    grad_attn = (
        jnp.einsum("re,de->rd", cot_low, whole_out, preferred_element_type=jnp.float32)
        .astype(jnp.bfloat16)
        .reshape(seqs_here, block_len, head_count, head_size)
    )
    row_delta = jnp.transpose(
        jnp.sum(grad_attn.astype(jnp.float32) * attn_vals, axis=-1), (0, 2, 1)
    )

    def back_block(grads_in, key_blk, value_blk, key_pos):

        def back_update(current):
            grad_query, grad_key, grad_value = current
            scores = (
                jnp.einsum("sqhd,skhd->shqk", queries, key_blk, preferred_element_type=jnp.float32)
                * score_scale
            )
            allowed = key_pos[:, None, None, :] <= positions[:, None, :, None]
            masked = jnp.where(allowed, scores, NEGATIVE)
            probability = jnp.exp(masked - log_total[..., None])
            prob_low = probability.astype(jnp.bfloat16)
            grad_value = grad_value + jnp.einsum(
                "shqk,sqhd->skhd", prob_low, grad_attn, preferred_element_type=jnp.float32
            )
            grad_prob = jnp.einsum(
                "sqhd,skhd->shqk", grad_attn, value_blk, preferred_element_type=jnp.float32
            )
            grad_score = (probability * (grad_prob - row_delta[..., None])).astype(jnp.bfloat16)
            grad_query = (
                grad_query
                + jnp.einsum(
                    "shqk,skhd->sqhd", grad_score, key_blk, preferred_element_type=jnp.float32
                )
                * score_scale
            )
            grad_key = (
                grad_key
                + jnp.einsum(
                    "shqk,sqhd->skhd", grad_score, queries, preferred_element_type=jnp.float32
                )
                * score_scale
            )
            return (grad_query, grad_key, grad_value)

        return lax.cond(
            jnp.min(key_pos) <= top_query, back_update, lambda unchanged: unchanged, grads_in
        )

    zero_rows = jnp.zeros((seqs_here, block_len, head_count, head_size), jnp.float32)

    def pass_back(grad_key, grad_value):
        return (
            shifted(grad_key.astype(jnp.bfloat16), "ctx", 1).astype(grad_key.dtype),
            shifted(grad_value.astype(jnp.bfloat16), "ctx", 1).astype(grad_value.dtype),
        )

    grad_query, grad_key, grad_value = back_block(
        (zero_rows, zero_rows, zero_rows), key_rows, value_rows, positions
    )
    grad_key, grad_value = pass_back(grad_key, grad_value)

    def cycle_backward(turn_index, carried):
        grad_query, key_cur, value_cur, grad_key, grad_value = carried
        key_cur, value_cur = shifted((key_cur, value_cur), "ctx", 1)
        source = (my_index - turn_index) % cycle_size
        key_pos = lax.dynamic_slice_in_dim(all_positions, source * block_len, block_len, 1)
        grad_query, grad_key, grad_value = back_block(
            (grad_query, grad_key, grad_value), key_cur, value_cur, key_pos
        )
        grad_key, grad_value = pass_back(grad_key, grad_value)
        return (grad_query, key_cur, value_cur, grad_key, grad_value)

    grad_query, unused_key, unused_value, grad_key, grad_value = lax.fori_loop(
        1, cycle_size, cycle_backward, (grad_query, key_rows, value_rows, grad_key, grad_value)
    )
    unused_rot, rotate_back = jax.vjp(
        lambda field_in: rotate(field_in, cosine, sine_table), zero_rows
    )
    query_pre = rotate_back(grad_query)[0]
    key_pre = rotate_back(grad_key)[0]
    grad_proj = (
        jnp.stack([query_pre, key_pre, grad_value], axis=2)
        .reshape(row_count, 3 * feature_count)
        .astype(jnp.bfloat16)
    )
    grad_qkv_bias = jnp.sum(grad_proj.astype(jnp.float32), axis=0)
    grad_qkv = jnp.einsum("rd,re->de", normed_one, grad_proj, preferred_element_type=jnp.float32)
    grad_one = jnp.einsum("re,de->rd", grad_proj, whole_qkv, preferred_element_type=jnp.float32)
    unused_one, norm_back_one = jax.vjp(layer_norm, inputs, ln1_gain, ln1_bias)
    input_one, grad_gain_one, grad_bias_one = norm_back_one(grad_one)
    unused_two, norm_back_two = jax.vjp(layer_norm, inputs, ln2_gain, ln2_bias)
    input_two, grad_gain_two, grad_bias_two = norm_back_two(grad_two)
    grad_input = (
        (cot_full + input_one + input_two)
        .astype(jnp.bfloat16)
        .reshape(seqs_here, block_len, feature_count)
    )
    summed = (
        lax.psum(grad_qkv.astype(jnp.bfloat16), "ctx").astype(jnp.float32),
        lax.psum(grad_out.astype(jnp.bfloat16), "ctx").astype(jnp.float32),
        lax.psum(grad_up.astype(jnp.bfloat16), "ctx").astype(jnp.float32),
        lax.psum(grad_down.astype(jnp.bfloat16), "ctx").astype(jnp.float32),
        lax.psum(grad_gain_one.astype(jnp.bfloat16), "ctx").astype(jnp.float32),
        lax.psum(grad_bias_one.astype(jnp.bfloat16), "ctx").astype(jnp.float32),
        lax.psum(grad_gain_two.astype(jnp.bfloat16), "ctx").astype(jnp.float32),
        lax.psum(grad_bias_two.astype(jnp.bfloat16), "ctx").astype(jnp.float32),
        lax.psum(grad_qkv_bias.astype(jnp.bfloat16), "ctx").astype(jnp.float32),
        lax.psum(grad_up_bias.astype(jnp.bfloat16), "ctx").astype(jnp.float32),
    )
    sum_qkv, sum_out, sum_up, sum_down = (
        lax.psum_scatter(
            summed[0].astype(jnp.bfloat16), "shard", scatter_dimension=0, tiled=True
        ).astype(jnp.float32),
        lax.psum_scatter(
            summed[1].astype(jnp.bfloat16), "shard", scatter_dimension=0, tiled=True
        ).astype(jnp.float32),
        lax.psum_scatter(
            summed[2].astype(jnp.bfloat16), "shard", scatter_dimension=0, tiled=True
        ).astype(jnp.float32),
        lax.psum_scatter(
            summed[3].astype(jnp.bfloat16), "shard", scatter_dimension=0, tiled=True
        ).astype(jnp.float32),
    )
    sum_small = (
        lax.psum(summed[4].astype(jnp.bfloat16), "shard").astype(jnp.float32),
        lax.psum(summed[5].astype(jnp.bfloat16), "shard").astype(jnp.float32),
        lax.psum(summed[6].astype(jnp.bfloat16), "shard").astype(jnp.float32),
        lax.psum(summed[7].astype(jnp.bfloat16), "shard").astype(jnp.float32),
        lax.psum(summed[8].astype(jnp.bfloat16), "shard").astype(jnp.float32),
        lax.psum(summed[9].astype(jnp.bfloat16), "shard").astype(jnp.float32),
    )
    return (
        layer_output,
        grad_input,
        sum_small[0],
        sum_small[1],
        sum_small[2],
        sum_small[3],
        sum_qkv,
        sum_small[4],
        sum_out,
        sum_up,
        sum_small[5],
        sum_down,
    )


def finish_body(
    y_in, dx_in, fin_in, qkvfin_in, early_in, late_in,
    y_out, dx_out, g1_out, b1_out, g2_out, b2_out, gqkv_out, gqkvb_out, gout_out, gup_out, gupb_out, gdown_out,
    gqkv, gout, gup, gdown, fin, qkvfin, early, late, y, dx, sem, in_sem,
):
    width = y_in.shape[1]
    chips = qkvfin.shape[0] // 2
    rows = qkvfin.shape[1]
    half = rows // 2
    cut = width // 2
    shards = width // rows
    slabs = 8 + 4 * chips
    copies = []
    coming = []

    def bring(src, dst):
        copy = pltpu.make_async_copy(src, dst, in_sem.at[len(coming)])
        copy.start()
        coming.append(copy)

    for h in range(2):
        bring(fin_in.at[h, pl.ds(0, cut)], fin.at[h, pl.ds(0, cut)])
    for h in range(2):
        bring(
            fin_in.at[h, pl.ds(cut, fin.shape[1] - cut)], fin.at[h, pl.ds(cut, fin.shape[1] - cut)]
        )
    bring(qkvfin_in, qkvfin)
    bring(y_in, y)
    bring(dx_in, dx)
    bring(early_in, early)
    bring(late_in, late)

    def out(src, dst):
        copy = pltpu.make_async_copy(src, dst, sem.at[len(copies)])
        copy.start()
        copies.append(copy)

    for h in range(2):
        coming[h].wait()
        gdown[pl.ds(cut * h, cut)] = fin[h, pl.ds(0, cut)].astype(FULL)
        out(gdown.at[pl.ds(cut * h, cut)], gdown_out.at[pl.ds(cut * h, cut)])
    for h in range(2):
        coming[2 + h].wait()
        mine = pl.ds(half * h, half)
        for n in range(shards):
            here = fin[h, pl.ds(cut + half + half * n, half)]
            gup[mine, width * n : width * (n + 1)] = here.astype(FULL)
        out(gup.at[mine], gup_out.at[mine])

    for copy in coming[4:]:
        copy.wait()
    out(y, y_out.at[0])
    out(dx, dx_out.at[0])

    def tiles(piece, wide, put):
        lane = lax.broadcasted_iota(jnp.int32, wide, 1)
        low_lanes = lane < HEAD_DIM
        for part in range(3):
            for w in range(chips // 2):
                p0, p1, p2, p3 = (piece(4 * w + t, part) for t in range(4))
                r1, r2 = pltpu.roll(p1, HEAD_DIM, 1), pltpu.roll(p2, HEAD_DIM, 1)
                at = width * part + 384 * w
                put(at, p0 + jnp.where(low_lanes, 0.0, r1))
                put(at + 128, jnp.where(low_lanes, r1, r2))
                put(at + 256, p3 + jnp.where(low_lanes, r2, 0.0))

    def put_rows(at, tile):
        gqkv[:, at : at + 128] = tile

    tiles(
        lambda j, part: qkvfin[j, :, 128 * part : 128 * (part + 1)].astype(FULL),
        (rows, 128),
        put_rows,
    )
    out(gqkv, gqkv_out)
    for h in range(2):
        gout[pl.ds(half * h, half)] = fin[h, pl.ds(cut, half)].astype(FULL)
    out(gout, gout_out)

    def bias_piece(j, part):
        row = early[8 + 2 * j + part // 2, 128 * (part % 2) : 128 * (part % 2 + 1)]
        return jnp.broadcast_to(row[None, :], (8, 128))

    def put_bias(at, tile):
        gqkvb_out[pl.ds(at, 128)] = tile[0]

    tiles(bias_piece, (8, 128), put_bias)
    for n in range(shards):
        for t in range(width // 256):
            gupb_out[pl.ds(width * n + 256 * t, 256)] = early[slabs + 8 * n + t]
    for k, vector in enumerate((g1_out, b1_out, g2_out, b2_out)):
        vector[pl.ds(0, cut)] = late[2 * k]
        vector[pl.ds(cut, cut)] = late[2 * k + 1]
    for copy in copies:
        copy.wait()


def finish(rows, shards, ctxs, *pieces):
    block, width = pieces[0].shape
    vmem = pl.BlockSpec(memory_space=pltpu.VMEM)
    hbm = pl.BlockSpec(memory_space=pl.ANY)
    shape = jax.ShapeDtypeStruct
    vector = shape((width,), FULL)
    return pl.pallas_call(
        finish_body,
        out_shape=(
            shape((1, block, width), LOW),
            shape((1, block, width), LOW),
            vector,
            vector,
            vector,
            vector,
            shape((rows, 3 * width), FULL),
            shape((3 * width,), FULL),
            shape((rows, width), FULL),
            shape((rows, shards * width), FULL),
            shape((shards * width,), FULL),
            shape((width, width), FULL),
        ),
        in_specs=[hbm] * 6,
        out_specs=(hbm, hbm, vmem, vmem, vmem, vmem, hbm, vmem, hbm, hbm, vmem, hbm),
        scratch_shapes=[
            pltpu.VMEM((rows, 3 * width), FULL),
            pltpu.VMEM((rows, width), FULL),
            pltpu.VMEM((rows, shards * width), FULL),
            pltpu.VMEM((width, width), FULL),
            pltpu.VMEM(pieces[2].shape, LOW),
            pltpu.VMEM(pieces[3].shape, LOW),
            pltpu.VMEM(pieces[4].shape, FULL),
            pltpu.VMEM(pieces[5].shape, FULL),
            pltpu.VMEM((block, width), LOW),
            pltpu.VMEM((block, width), LOW),
            pltpu.SemaphoreType.DMA((8,)),
            pltpu.SemaphoreType.DMA((16,)),
        ],
        compiler_params=pltpu.CompilerParams(vmem_limit_bytes=60 * 1024 * 1024),
        name="finish",
    )(*pieces)


def fused_on_device(
    layer_input,
    positions,
    cotangent,
    ln1_gain,
    ln1_bias,
    ln2_gain,
    ln2_bias,
    w_qkv,
    qkv_bias,
    w_out,
    w_up,
    up_bias,
    w_down,
):
    shards, ctxs = lax.axis_size("shard"), lax.axis_size("ctx")
    block, width = layer_input.shape[1:]
    rows = w_qkv.shape[0]
    half = rows // 2
    line_rows = width // 2 + half + shards * half
    vmem = pl.BlockSpec(memory_space=pltpu.VMEM)
    hbm = pl.BlockSpec(memory_space=pl.ANY)
    low, full = (lambda *shape: pltpu.VMEM(shape, LOW)), (lambda *shape: pltpu.VMEM(shape, FULL))
    chips = ctxs // 2
    scratch = dict(
        wq=low(width, 384),
        wraw=low(3, rows, 256),
        wup=low(width, width),
        wout=low(256, width),
        wdn=low(width, width),
        n1=low(ctxs * block, width),
        n2=low(shards * block, width),
        cot=low(shards * block, width),
        pos_tx=pltpu.VMEM((8, block), jnp.int32),
        pos_rx=pltpu.VMEM((ctxs, 8, block), jnp.int32),
        pos_sm=pltpu.SMEM((ctxs, 8, block), jnp.int32),
        qkv=full(ctxs, block, 384),
        q_s=low(ctxs * block, 128),
        k_s=low(ctxs * block, 128),
        v_s=low(ctxs * block, 128),
        do_tx=low(shards, 2, block, 128),
        do_mid=low(shards, 2, block, 128),
        do_rx=low(ctxs, block, 128),
        do_s=low(ctxs * block, 128),
        o_s=full(ctxs, block, 128),
        dq_s=full(ctxs * block, 128),
        dk_s=full(ctxs * block, 128),
        dv_s=full(ctxs * block, 128),
        gp_s=low(ctxs, block, 384),
        gp_e=low(ctxs * block, 384),
        o_tx=low(ctxs, block, 128),
        o_rx=low(2 * shards, block, 128),
        attn=low(shards * block, 256),
        a1_p=low(ctxs, block, width),
        a1_d2d=low(chips, block, width),
        a1_own=low(chips, block, width),
        a1_tx_r=low(chips, block, width),
        a1_tx_l=low(chips, block, width),
        a1_rx_r=low(chips, block, width),
        a1_rx_l=low(chips, block, width),
        gq_tx=low(width, 384),
        gq_rx=low(shards, rows, 384),
        out_acc=full(shards * block, width),
        a2_acc=full(shards * block, width),
        out_tx=low(shards, block, width),
        out_rx=low(shards, block, width),
        a2_tx=low(shards, block, width),
        a2_rx=low(shards, block, width),
        gd16=low(width, width),
        gd_rx=low(width // 2, width),
        gu16=low(width, width),
        gu_rx=low(shards, half, width),
        gu_tx=low(shards, half, width),
        go16=low(rows, width),
        go_rx=low(half, width),
        line_own=low(line_rows, width),
        line_rx=low(2, line_rows, width),
        line_near=low(line_rows, width),
        line_far=low(line_rows, width),
        early_a=full(8, 256),
        early_rx=full(ctxs, 8, 256),
        early_b=full(shards, 8 + 2 * ctxs, 256),
        late_a=full(8, width // 2),
        late_rx=full(ctxs, 8, width // 2),
        late_b=full(shards, 8, width // 2),
        ssem=pltpu.SemaphoreType.DMA((320,)),
        rsem=pltpu.SemaphoreType.DMA((320,)),
        lsem=pltpu.SemaphoreType.DMA((16,)),
    )
    slabs = 8 + 2 * ctxs
    y, dx, fin, qkvfin, early, late = pl.pallas_call(
        functools.partial(fused_body, tuple(scratch)),
        out_shape=(
            jax.ShapeDtypeStruct((block, width), LOW),
            jax.ShapeDtypeStruct((block, width), LOW),
            jax.ShapeDtypeStruct((2, line_rows, width), LOW),
            jax.ShapeDtypeStruct((ctxs, rows, 384), LOW),
            jax.ShapeDtypeStruct((slabs + 8 * shards, 256), FULL),
            jax.ShapeDtypeStruct((8, width // 2), FULL),
        ),
        in_specs=[vmem] * 9 + [hbm] * 5,
        out_specs=(vmem,) * 6,
        scratch_shapes=list(scratch.values()),
        compiler_params=pltpu.CompilerParams(
            collective_id=0, has_side_effects=True, vmem_limit_bytes=60 * 1024 * 1024
        ),
        name="layer",
    )(
        layer_input[0],
        positions,
        ln1_gain,
        ln1_bias,
        ln2_gain,
        ln2_bias,
        qkv_bias,
        up_bias,
        jnp.asarray(rotary_constants(ctxs, block)),
        cotangent[0],
        w_qkv,
        w_up,
        w_out,
        w_down,
    )
    return finish(rows, shards, ctxs, y, dx, fin, qkvfin, early, late)


def on_device(layer_input, positions, cotangent, *params):
    shards, ctxs = lax.axis_size("shard"), lax.axis_size("ctx")
    seqs, block, width = layer_input.shape
    rows, ff = params[4].shape[0], params[7].shape[1]
    fits = (
        seqs == 1
        and block == 128
        and (shards, ctxs) == (4, 8)
        and 3 * ctxs == 2 * HEADS
        and HEAD_DIM == 64
        and rows * shards == width == HEADS * HEAD_DIM
        and ff == shards * width
    )
    path = fused_on_device if fits else ring_on_device
    return path(layer_input, positions, cotangent, *params)


def solution(mesh):
    placed = (
        P("shard", "ctx", None),
        P("shard", "ctx"),
        P("shard", "ctx", None),
        P(),
        P(),
        P(),
        P(),
        P("shard", None),
        P(),
        P("shard", None),
        P("shard", None),
        P(),
        P("shard", None),
    )
    return jax.shard_map(
        on_device,
        mesh=mesh,
        in_specs=placed,
        out_specs=(
            P("shard", "ctx", None),
            P("shard", "ctx", None),
            P(),
            P(),
            P(),
            P(),
            P("shard", None),
            P(),
            P("shard", None),
            P("shard", None),
            P(),
            P("shard", None),
        ),
        check_vma=False,
    )
```

```python
import functools

import jax
import jax.numpy as jnp
import numpy as np
from jax import lax
from jax.experimental import pallas as pl
from jax.experimental.pallas import tpu as pltpu
from jax.sharding import PartitionSpec as P

HEADS = 12
HEAD_DIM = 64
ROTARY = 16


EPSILON = 1e-05
NEGATIVE = -1e30


def shifted(shard, axis, by):
    count = lax.axis_size(axis)
    return lax.ppermute(shard, axis, [(i, (i + by) % count) for i in range(count)])


def layer_norm(values_in, gain_vec, bias_vec):
    centered = values_in - jnp.mean(values_in, axis=-1, keepdims=True)
    variance = jnp.mean(centered * centered, axis=-1, keepdims=True)
    return centered * lax.rsqrt(variance + EPSILON) * gain_vec + bias_vec


def rotary_tables(position_ids):
    half_dim = ROTARY // 2
    inverse_freq = 1.0 / 10000.0 ** (jnp.arange(half_dim, dtype=jnp.float32) * (2.0 / ROTARY))
    angles = position_ids.astype(jnp.float32)[..., None] * inverse_freq
    return (jnp.cos(angles), jnp.sin(angles))


def rotate(field_in, cosine, sine_table):
    half_dim = cosine.shape[-1]
    lead_part = field_in[..., :half_dim]
    second = field_in[..., half_dim : 2 * half_dim]
    remain = field_in[..., 2 * half_dim :]
    cos_wide = cosine[..., None, :]
    sin_wide = sine_table[..., None, :]
    return jnp.concatenate(
        [
            lead_part * cos_wide - second * sin_wide,
            second * cos_wide + lead_part * sin_wide,
            remain,
        ],
        axis=-1,
    )


def gelu_exact(field_in):
    return jax.nn.gelu(field_in, approximate=False)


MESH = pl.DeviceIdType.MESH
LOW = jnp.bfloat16
FULL = jnp.float32
ROWS_CONTRACT = (((0,), (0,)), ((), ()))
COLS_CONTRACT = (((1,), (1,)), ((), ()))
INV_ROOT_TWO = 0.7071067811865476
INV_ROOT_TWO_PI = 0.3989422804014327
CHUNK = 48
LAG = 2


def dot(lhs, rhs, dims=(((1,), (0,)), ((), ()))):
    return lax.dot_general(lhs, rhs, dims, preferred_element_type=FULL)


def flip(index, bits):
    for power in (1, 2, 4, 8):
        if bits & power:
            index = index + power - 2 * power * lax.rem(lax.div(index, power), 2)
    return index


def at16(value):
    return pl.multiple_of(value, 16)


def at128(value):
    return pl.multiple_of(value, 128)


def rotary_constants(blocks, block_len):
    lane = np.arange(128) % HEAD_DIM
    half = ROTARY // 2
    turning = lane < ROTARY
    freq = np.where(turning, 10000.0 ** (-(lane % half) * (2.0 / ROTARY)), 0.0)
    sign = np.where(lane < half, -1.0, 1.0) * turning
    offset = np.arange(block_len)[:, None] * freq
    start = (np.arange(blocks) * block_len)[:, None] * freq
    parts = (np.cos(offset), np.sin(offset) * sign, np.cos(start), np.sin(start) * sign)
    return np.concatenate(parts).astype(np.float32)


def fused_body(names, *refs):
    (
        x_ref, pos_ref, gain1_ref, bias1_ref, gain2_ref, bias2_ref, qkvb_ref, upb_ref, rot_ref,
        cot_hbm, wqkv_hbm, wup_hbm, wout_hbm, wdn_hbm,
        y_ref, dx_ref, fin_ref, qkvfin_ref, early_ref, late_ref,
    ) = refs[:20]
    scratch = dict(zip(names, refs[20:]))
    run_layer(
        x_ref, pos_ref, gain1_ref, bias1_ref, gain2_ref, bias2_ref, qkvb_ref, upb_ref, rot_ref,
        cot_hbm, wqkv_hbm, wup_hbm, wout_hbm, wdn_hbm,
        y_ref, dx_ref, fin_ref, qkvfin_ref, early_ref, late_ref, **scratch,
    )


def run_layer(
    x_ref, pos_ref, gain1_ref, bias1_ref, gain2_ref, bias2_ref, qkvb_ref, upb_ref, rot_ref,
    cot_hbm, wqkv_hbm, wup_hbm, wout_hbm, wdn_hbm,
    y_ref, dx_ref, fin_ref, qkvfin_ref, early_ref, late_ref,
    *,
    wq, wraw, wup, wout, wdn, n1, n2, cot, pos_tx, pos_rx, pos_sm, qkv, q_s, k_s, v_s, do_tx, do_mid, do_rx, do_s,
    o_s, dq_s, dk_s, dv_s, gp_s, gp_e, o_tx, o_rx, attn, a1_p, a1_d2d, a1_own, a1_tx_r, a1_tx_l, a1_rx_r, a1_rx_l,
    gq_tx, gq_rx, out_acc, a2_acc, out_tx, out_rx, a2_tx, a2_rx, gd16, gd_rx, gu16, gu_rx, gu_tx,
    go16, go_rx, line_own, line_rx, line_near, line_far, early_a, early_d2d, early_z, early_x, late_a, late_d2d, late_z, late_x, ssem, rsem, lsem,
):
    shards = lax.axis_size("shard")
    ctxs = lax.axis_size("ctx")
    s = lax.axis_index("shard")
    i = lax.axis_index("ctx")
    c = lax.rem(i, 2)
    z = lax.div(i, 2)
    other = 1 - c
    Z = ctxs // 2
    planes = range(1, shards)
    mates = range(1, ctxs)
    block = x_ref.shape[0]
    width = x_ref.shape[1]
    rows = width // shards
    half_rows = rows // 2
    half_width = width // 2
    sent = []
    used = [0]
    always = None

    def channels(count):
        first = used[0]
        used[0] += count
        return first

    def copy_of(send_k, recv_k, src, dst, device):
        return pltpu.make_async_remote_copy(
            src_ref=src,
            dst_ref=dst,
            send_sem=ssem.at[send_k],
            recv_sem=rsem.at[recv_k],
            device_id=device,
            device_id_type=MESH,
        )

    def send(k, src, dst, device, recv_k=None, when=always):
        copy = copy_of(k, k if recv_k is None else recv_k, src, dst, device)
        sent.append((copy, when))
        if when is always:
            copy.start()
        else:
            pl.when(when)(copy.start)

    def arrived(k, dst):
        copy_of(k, k, dst, dst, {"ctx": flip(i, 1)}).wait_recv()

    def plane(d):
        return flip(s, d)

    def mate(e):
        return flip(i, e)

    partner = {"ctx": flip(i, 1)}
    right = {"ctx": i + 2}
    left = {"ctx": i - 2}
    has_left = z > 0
    has_right = z < Z - 1
    low_side = z < Z // 2
    is_end = (z == 0) | (z == Z - 1)
    is_mid = jnp.logical_not(is_end)

    loads = []

    def load(src, dst):
        copy = pltpu.make_async_copy(src, dst, lsem.at[len(loads)])
        copy.start()
        loads.append(copy)

    my_rows = pl.ds(at16(s * rows), rows)
    first = HEAD_DIM * (3 * z + c)
    base = jnp.minimum(128 * lax.div(first, 128), width - 256)
    for part in range(3):
        load(wqkv_hbm.at[:, pl.ds(at128(width * part + base), 256)], wraw.at[part])
    load(cot_hbm, cot.at[pl.ds(0, block)])
    load(wout_hbm.at[pl.ds(0, 128)], wout.at[pl.ds(0, 128)])
    load(wout_hbm.at[pl.ds(HEAD_DIM, 128)], wout.at[pl.ds(128, 128)])
    load(wup_hbm.at[:, pl.ds(at128(s * width), width)], wup.at[my_rows])
    load(wdn_hbm, wdn)

    barrier = pltpu.get_barrier_semaphore()
    for d in range(shards):
        for e in range(ctxs):
            if d or e:
                pl.semaphore_signal(
                    barrier,
                    inc=1,
                    device_id={"shard": plane(d), "ctx": mate(e)},
                    device_id_type=MESH,
                )
    pl.semaphore_wait(barrier, shards * ctxs - 1)

    K_COT = channels(2 * shards)
    K_N2 = channels(2 * shards)
    K_WQ = channels(shards)
    K_WU = channels(shards)
    K_POS = channels(ctxs)
    side, over, across_plane = 1, 2, 3
    half_block = block // 2
    part_rows = rows // Z
    part_cols = width // 2

    def wup_part(owner, j):
        return wup.at[
            pl.ds(at16(owner * rows + lax.div(j, 2) * part_rows), part_rows),
            pl.ds(at128(lax.rem(j, 2) * part_cols), part_cols),
        ]

    for d in planes:
        send(
            K_WU + d,
            wup_hbm.at[
                pl.ds(at16(z * part_rows), part_rows),
                pl.ds(at128(plane(d) * width + c * part_cols), part_cols),
            ],
            wup_part(s, i),
            {"shard": plane(d)},
        )
    for d in (side, over):
        send(K_COT + d, cot_hbm, cot.at[pl.ds(block * d, block)], {"shard": plane(d)})

    def two_heads(here, there):
        wide = lax.broadcasted_iota(jnp.int32, here.shape, 1)
        turned = jnp.where(
            wide < HEAD_DIM, pltpu.roll(here, HEAD_DIM, 1), pltpu.roll(there, HEAD_DIM, 1)
        )
        return jnp.where(
            first == base, here, jnp.where(first == base + HEAD_DIM, turned, there)
        )

    for copy in loads[:3]:
        copy.wait()
    for part in range(3):
        raw = wraw[part].astype(FULL)
        wq[my_rows, 128 * part : 128 * (part + 1)] = two_heads(raw[:, :128], raw[:, 128:]).astype(LOW)
    qkv_bias = jnp.concatenate(
        [
            two_heads(
                jnp.broadcast_to(qkvb_ref[pl.ds(at128(width * part + base), 128)][None, :], (8, 128)),
                jnp.broadcast_to(qkvb_ref[pl.ds(at128(width * part + base + 128), 128)][None, :], (8, 128)),
            )
            for part in range(3)
        ],
        axis=1,
    )[:1]
    gain1, gain2 = gain1_ref[...][None, :], gain2_ref[...][None, :]
    bias1, bias2 = bias1_ref[...][None, :], bias2_ref[...][None, :]
    pos_tx[...] = jnp.broadcast_to(pos_ref[...], pos_tx.shape)
    x = x_ref[...].astype(FULL)
    mean = jnp.mean(x, axis=-1, keepdims=True)
    centered = x - mean
    r = lax.rsqrt(jnp.mean(centered * centered, axis=-1, keepdims=True) + EPSILON)
    normal = centered * r

    def tokens(j):
        return pl.ds(at128(block * j), block)

    n1[tokens(i)] = (normal * gain1 + bias1).astype(LOW)
    n2[pl.ds(0, block)] = (normal * gain2 + bias2).astype(LOW)
    pos_rx[i] = pos_tx[...]
    for d in (side, over):
        send(K_N2 + d, n2.at[pl.ds(0, block)], n2.at[pl.ds(block * d, block)], {"shard": plane(d)})
    for e in mates:
        send(K_POS + e, pos_tx, pos_rx.at[i], {"ctx": mate(e)})

    def hand_on(k, field):
        for d, to, half in ((side, over, 0), (over, side, 1)):
            arrived(k + d, field.at[pl.ds(block * d, block)])
            send(
                k + across_plane + half,
                field.at[pl.ds(block * d + half_block * half, half_block)],
                field.at[pl.ds(block * across_plane + half_block * half, half_block)],
                {"shard": plane(to)},
            )

    def handed_on(k, field):
        for half in range(2):
            arrived(
                k + across_plane + half,
                field.at[pl.ds(block * across_plane + half_block * half, half_block)],
            )

    class Relay:
        def __init__(self, piece):
            self.piece = piece
            self.direct = channels(Z)
            self.across = channels(2 * Z)
            self.to_right = channels(Z)
            self.to_left = channels(Z)

        def begin(self):
            mine = self.piece(i)
            send(self.to_right, mine, mine, right, self.direct + z, has_right)
            send(self.to_left, mine, mine, left, self.direct + z, has_left)
            send(self.across, mine, mine, partner, self.across + z)

        def from_left(self, k, here=True):
            piece = self.piece(i - 2 * k)
            when = (z >= k) & here

            @pl.when(when)
            def _():
                arrived(self.direct + z - k, piece)

            if k < Z - 1:
                send(self.to_right + k, piece, piece, right, self.direct + z - k, when & has_right)
            send(self.across + 2 * k - 1, piece, piece, partner, self.across + z - k, when)

        def from_right(self, k, here=True):
            piece = self.piece(i + 2 * k)
            when = (z + k < Z) & here

            @pl.when(when)
            def _():
                arrived(self.direct + z + k, piece)

            if k < Z - 1:
                send(self.to_left + k, piece, piece, left, self.direct + z + k, when & has_left)
            send(self.across + 2 * k, piece, piece, partner, self.across + z + k, when)

        def step(self, k, here=True):
            self.from_left(k, here)
            self.from_right(k, here)

        def step_inner(self, k):
            self.from_left(k, jnp.logical_not(low_side))
            self.from_right(k, low_side)

        def step_outer(self, k):
            self.from_left(k, low_side)
            self.from_right(k, jnp.logical_not(low_side))

        def end(self):
            for to in range(Z):
                arrived(self.across + to, self.piece(2 * to + other))

    normed = Relay(lambda j: n1.at[tokens(j)])
    ups = [Relay(functools.partial(wup_part, plane(d))) for d in planes]
    for d in planes:
        arrived(K_WU + d, wup_part(plane(d), i))
        ups[d - 1].begin()
    for copy in loads[3:]:
        copy.wait()

    K_DO = channels(ctxs)
    K_DOS = channels(ctxs)
    K_DOM = channels(shards)

    def grad_attn(d):
        field = dot(cot[pl.ds(block * d, block)], wout[...], COLS_CONTRACT)
        for core in range(2):
            do_tx[d, core] = field[:, 128 * core : 128 * (core + 1)].astype(LOW)

    def grad_attn_on(d):
        if d:
            arrived(K_DOM + d, do_mid.at[d])
        for core in range(2):
            target = 2 * plane(d) + core
            piece = do_mid.at[d, core]
            send(K_DOS + 2 * d + core, piece, do_rx.at[i], {"ctx": target}, K_DO + i, i != target)

            @pl.when(i == target)
            def _():
                do_rx[i] = do_mid[d, core]

    grad_attn(0)
    do_mid[0] = do_tx[0]
    hand_on(K_COT, cot)
    grad_attn(side)
    grad_attn(over)
    for up in ups:
        up.step(1)
    hand_on(K_N2, n2)
    for up in ups:
        up.step(2)
    normed.begin()
    handed_on(K_COT, cot)
    grad_attn(across_plane)
    for d in planes:
        send(K_DOM + d, do_tx.at[d], do_mid.at[d], {"shard": plane(d)})
    for d in planes:
        send(K_WQ + d, wq.at[my_rows], wq.at[my_rows], {"shard": plane(d)})
    for e in mates:
        arrived(K_POS + e, pos_rx.at[mate(e)])
    to_scalar = pltpu.make_async_copy(pos_rx, pos_sm, lsem.at[len(loads)])
    to_scalar.start()
    out_acc[...] = jnp.zeros_like(out_acc)
    a2_acc[...] = jnp.zeros_like(a2_acc)
    early_a[...] = jnp.zeros_like(early_a)
    handed_on(K_N2, n2)
    for up in ups:
        for k in range(3, Z):
            up.step(k)
        up.end()
    normed.step(1, is_mid)

    @pl.loop(0, width // 256)
    def _(t):
        units = pl.ds(at128(t * 256), 256)
        bias = upb_ref[pl.ds(at128(s * width + t * 256), 256)][None, :]
        pre = dot(n2[...], wup[:, units]) + bias
        cdf = 0.5 * (1.0 + lax.erf(pre * INV_ROOT_TWO))
        hidden = (pre * cdf).astype(LOW)
        slope = cdf + pre * (jnp.exp(-0.5 * pre * pre) * INV_ROOT_TWO_PI)
        grad_hidden = dot(cot[...], wdn[units], COLS_CONTRACT)
        grad_pre = (grad_hidden * slope).astype(LOW)
        unit_sums = jnp.sum(grad_pre.astype(FULL), axis=0, keepdims=True)
        early_a[0, pl.ds(t, 1)] = unit_sums[:, :128]
        early_a[1, pl.ds(t, 1)] = unit_sums[:, 128:]
        out_acc[...] += dot(hidden, wdn[units])
        a2_acc[...] += dot(grad_pre, wup[:, units], COLS_CONTRACT)
        gd16[units] = dot(hidden, cot[...], ROWS_CONTRACT).astype(LOW)
        gu16[:, units] = dot(n2[...], grad_pre, ROWS_CONTRACT).astype(LOW)

    K_GD = channels(1)
    K_GU = channels(shards)
    K_GUX = channels(shards)
    K_OUT = channels(shards)
    K_A2 = channels(shards)
    K_GO = channels(1)

    def rows_of(d, core):
        return pl.ds(at16(plane(d) * rows + core * half_rows), half_rows)

    send(K_GD, gd16.at[pl.ds(at16(other * half_width), half_width)], gd_rx, partner)
    for d in (*planes, 0):
        send(K_GU + d, gu16.at[rows_of(d, other)], gu_rx.at[d], partner)
    normed.step(1, is_end)
    grad_attn_on(0)
    for d in planes:
        grad_attn_on(d)
    for d in planes:
        a2_tx[d] = a2_acc[pl.ds(block * d, block)].astype(LOW)

    is_centre = (z == Z // 2 - 1) | (z == Z // 2)
    inward = jnp.where(z < Z // 2, 2, -2)
    inner = {"ctx": i + inward}
    outer = {"ctx": i - inward}
    to_inner = jnp.where(is_centre, 1, 0)
    line_rows = half_width + half_rows + shards * half_rows
    chunks = line_rows // CHUNK
    UP = half_width
    OUT = half_width + shards * half_rows
    first_up, first_out = UP // CHUNK, OUT // CHUNK
    K_OUTER = channels(chunks)
    K_INNER = channels(chunks)
    K_NEAR = channels(chunks)
    K_FAR = channels(chunks)
    K_FIN = channels(chunks)

    def up_rows(index):
        return pl.ds(at16(UP + index * half_rows), half_rows)

    def span_of(q):
        return pl.ds(q * CHUNK, CHUNK)

    def near_copy(q, src, k):
        return copy_of(
            k + q,
            K_OUTER + chunks * to_inner + q,
            src.at[span_of(q)],
            line_rx.at[to_inner, span_of(q)],
            inner,
        )

    def far_copy(q):
        return copy_of(
            K_FAR + q, K_INNER + q, line_far.at[span_of(q)], line_rx.at[1, span_of(q)], outer
        )

    def fin_copy(q):
        piece = fin_ref.at[c, span_of(q)]
        return copy_of(K_FIN + q, K_FIN + q, piece, piece, partner)

    def near_end(q):
        pl.when(is_end)(near_copy(q, line_own, K_NEAR).start)

    def near_mid(q):
        arrived(K_OUTER + q, line_rx.at[0, span_of(q)])
        line_near[span_of(q)] = (
            line_rx[0, span_of(q)].astype(FULL) + line_own[span_of(q)].astype(FULL)
        ).astype(LOW)
        near_copy(q, line_near, K_INNER).start()

    def near(q):
        pl.when(is_mid)(functools.partial(near_mid, q))

    def far(q):
        arrived(K_INNER + q, line_rx.at[1, span_of(q)])
        beyond = line_rx[1, span_of(q)].astype(FULL) + line_own[span_of(q)].astype(FULL)

        @pl.when(is_mid)
        def _():
            line_far[span_of(q)] = beyond.astype(LOW)
            far_copy(q).start()

        fin_ref[c, span_of(q)] = (beyond + line_rx[0, span_of(q)].astype(FULL)).astype(LOW)
        fin_copy(q).start()

    @pl.when(is_end)
    def _():
        line_rx[0] = jnp.zeros((line_rows, width), LOW)

    arrived(K_GD, gd_rx)
    line_own[pl.ds(0, half_width)] = (
        gd16[pl.ds(at16(c * half_width), half_width)].astype(FULL) + gd_rx[...].astype(FULL)
    ).astype(LOW)
    for q in range(first_up):
        near_end(q)
    normed.step(2)
    for d in (*planes, 0):
        arrived(K_GU + d, gu_rx.at[d])
        total = (gu16[rows_of(d, c)].astype(FULL) + gu_rx[d].astype(FULL)).astype(LOW)
        if d:
            gu_tx[d] = total
            send(K_GUX + d, gu_tx.at[d], line_own.at[up_rows(s)], {"shard": plane(d)})
        else:
            line_own[up_rows(s)] = total
    for k in range(3, Z):
        normed.step(k)
    normed.end()
    for d in planes:
        arrived(K_WQ + d, wq.at[pl.ds(at16(plane(d) * rows), rows)])

    @pl.loop(0, ctxs // 2)
    def _(m):
        here = pl.ds(at128(m * 2 * block), 2 * block)
        qkv[pl.ds(2 * m, 2)] = dot(n1[here], wq[...]).reshape(2, block, 384)

    to_scalar.wait()
    rank = [lax.div(pos_sm[j, 0, 0], block) for j in range(ctxs)]
    place = []
    for g in range(ctxs):
        found = jnp.int32(0)
        for j in range(1, ctxs):
            found = found + j * (rank[j] == g).astype(jnp.int32)
        place.append(lax.rem(found, ctxs))

    lane = lax.broadcasted_iota(jnp.int32, (block, 128), 1)
    leads = lax.rem(lane, HEAD_DIM) < ROTARY // 2

    def across(field):
        return jnp.where(
            leads,
            pltpu.roll(field, 128 - ROTARY // 2, 1),
            pltpu.roll(field, ROTARY // 2, 1),
        )

    def tables(g):
        off_cos, off_sin = rot_ref[pl.ds(0, block)], rot_ref[pl.ds(block, block)]
        start_cos = rot_ref[pl.ds(2 * block + g, 1)]
        start_sin = rot_ref[pl.ds(2 * block + ctxs + g, 1)]
        cosine = start_cos * off_cos - start_sin * off_sin
        sine = start_sin * off_cos + start_cos * off_sin
        return cosine, sine

    for j in range(ctxs):

        @pl.when(j != i)
        def _():
            arrived(K_DO + j, do_rx.at[j])

    for g in range(ctxs):
        here = pl.ds(block * g, block)
        field = qkv[place[g]] + qkv_bias
        cosine, sine = tables(g)
        q_raw, k_raw = field[:, :128], field[:, 128:256]
        turned_q = (q_raw * cosine + across(q_raw) * sine).astype(LOW)
        q_s[here] = turned_q * jnp.asarray(HEAD_DIM**-0.5, LOW)
        k_s[here] = (k_raw * cosine + across(k_raw) * sine).astype(LOW)
        v_s[here] = field[:, 256:].astype(LOW)
        do_s[here] = do_rx[place[g]]

    o_s[...] = jnp.zeros_like(o_s)
    dq_s[...] = jnp.zeros_like(dq_s)
    dk_s[...] = jnp.zeros_like(dk_s)
    dv_s[...] = jnp.zeros_like(dv_s)

    slots = {3: 0, 5: 1, 6: 2, 7: 3}

    @pl.loop(0, 2)
    def _(h):
        mine = lax.div(lane, HEAD_DIM) == h
        for g in range(ctxs):
            share = 0 if g % 4 in (0, 3) else 1

            @pl.when((h == c) | (c == share))
            def _():
                here = pl.ds(block * g, block)
                upto = pl.ds(0, block * (g + 1))
                span = block * (g + 1)
                zero = jnp.zeros((block, 128), LOW)
                q_h = jnp.where(mine, q_s[here], zero)
                do_h = jnp.where(mine, do_s[here], zero)
                scores = dot(q_h, k_s[upto], COLS_CONTRACT)
                token = lax.broadcasted_iota(jnp.int32, (block, span), 0) + block * g
                key = lax.broadcasted_iota(jnp.int32, (block, span), 1)
                masked = jnp.where(key <= token, scores, NEGATIVE)
                top = jnp.max(masked, axis=-1, keepdims=True)
                weight = jnp.exp(masked - top)
                probability = weight * (1.0 / jnp.sum(weight, axis=-1, keepdims=True))
                prob_low = probability.astype(LOW)
                attended = jnp.where(mine, dot(prob_low, v_s[upto]), 0.0)
                o_s[g] += attended
                grad_prob = dot(do_h, v_s[upto], COLS_CONTRACT)
                row_delta = jnp.sum(do_h.astype(FULL) * attended, axis=-1, keepdims=True)
                grad_score = (probability * (grad_prob - row_delta)).astype(LOW)
                dq_s[here] += jnp.where(mine, dot(grad_score, k_s[upto]), 0.0)
                dk_s[upto] += dot(grad_score, q_h, ROWS_CONTRACT)
                dv_s[upto] += dot(prob_low, do_h, ROWS_CONTRACT)

            if g in slots:
                u = slots[g]
                pl.when((h == 0) & is_mid)(functools.partial(near_mid, u))
                pl.when((h == 1) & is_mid)(functools.partial(near_mid, 4 + u))
                pl.when((h == 1) & is_mid)(functools.partial(far, u))

        @pl.when(h == 0)
        def _():
            for d in planes:
                arrived(K_GUX + d, line_own.at[up_rows(plane(d))])
            for q in range(first_up, first_out):
                near_end(q)

    K_O = channels(2 * shards)
    K_OS = channels(ctxs)
    for j in range(ctxs):
        o_tx[j] = o_s[rank[j]].astype(LOW)
        away = (s != z) | (j != i)
        send(K_OS + j, o_tx.at[j], o_rx.at[2 * s + c], {"shard": z, "ctx": j}, K_O + 2 * s + c, away)

        @pl.when(jnp.logical_not(away))
        def _():
            o_rx[2 * s + c] = o_tx[j]

    bias_sum = jnp.zeros((1, 384), FULL)
    for g in range(ctxs):
        here = pl.ds(block * g, block)
        cosine, sine = tables(g)
        dq = dq_s[here] * (HEAD_DIM**-0.5)
        dk = dk_s[here]
        parts = (dq * cosine - across(dq) * sine, dk * cosine - across(dk) * sine, dv_s[here])
        part = jnp.concatenate(parts, axis=1).astype(LOW)
        gp_s[g] = part
        bias_sum = bias_sum + jnp.sum(part.astype(FULL), axis=0, keepdims=True)
    for j in range(ctxs):
        gp_e[pl.ds(block * j, block)] = gp_s[rank[j]]
    early_a[0, 3:4] = bias_sum[:, 0:128]
    early_a[1, 3:4] = bias_sum[:, 128:256]
    early_a[0, 4:5] = bias_sum[:, 256:384]
    K_ED = channels(1)
    K_EZ = channels(Z)
    K_EX = channels(shards)
    K_EF = channels(1)
    send(K_ED, early_a.at[other], early_d2d, partner)

    @pl.loop(0, ctxs // 2)
    def _(m):
        here = pl.ds(at128(m * 2 * block), 2 * block)
        a1_p[pl.ds(2 * m, 2)] = (
            dot(gp_e[here], wq[...], COLS_CONTRACT).astype(LOW).reshape(2, block, width)
        )

    K_A1D = channels(Z)
    for t in range(Z):
        send(K_A1D + t, a1_p.at[2 * t + other], a1_d2d.at[t], partner)

    @pl.loop(0, width // 256)
    def _(m):
        here = pl.ds(at128(m * 256), 256)
        gq_tx[here] = dot(n1[:, here], gp_e[...], ROWS_CONTRACT).astype(LOW)

    K_GQ = channels(shards)
    for d in planes:
        send(
            K_GQ + d, gq_tx.at[pl.ds(at16(plane(d) * rows), rows)], gq_rx.at[d], {"shard": plane(d)}
        )

    pl.when(is_mid)(functools.partial(far, 4))
    pl.when(is_mid)(functools.partial(far, 5))
    for t in range(Z):
        arrived(K_A1D + t, a1_d2d.at[t])
        a1_own[t] = (a1_p[2 * t + c].astype(FULL) + a1_d2d[t].astype(FULL)).astype(LOW)

    K_A1R = channels(Z)
    K_A1L = channels(Z)

    def a1_ends(hops):
        t = hops
        send(K_A1R + t, a1_own.at[t], a1_rx_r.at[t], right, None, z == 0)
        t = Z - 1 - hops
        send(K_A1L + t, a1_own.at[t], a1_rx_l.at[t], left, None, z == Z - 1)

    def a1_right(t, here):
        when = (z > 0) & (z < t) & here

        @pl.when(when)
        def _():
            arrived(K_A1R + t, a1_rx_r.at[t])
            a1_tx_r[t] = (a1_own[t].astype(FULL) + a1_rx_r[t].astype(FULL)).astype(LOW)

        send(K_A1R + t, a1_tx_r.at[t], a1_rx_r.at[t], right, None, when)

    def a1_left(t, here):
        when = (z < Z - 1) & (z > t) & here

        @pl.when(when)
        def _():
            arrived(K_A1L + t, a1_rx_l.at[t])
            a1_tx_l[t] = (a1_own[t].astype(FULL) + a1_rx_l[t].astype(FULL)).astype(LOW)

        send(K_A1L + t, a1_tx_l.at[t], a1_rx_l.at[t], left, None, when)

    for hops in reversed(range(1, Z)):
        a1_ends(hops)

    @pl.when(z == 0)
    def _():
        a1_rx_r[0] = jnp.zeros((block, width), LOW)

    @pl.when(z == Z - 1)
    def _():
        a1_rx_l[Z - 1] = jnp.zeros((block, width), LOW)

    arrived(K_ED, early_d2d)
    mine, theirs = early_a[c], early_d2d[...]
    early_z[0, 0:3] = mine[0:3] + theirs[0:3]
    even_core = c == 0
    early_z[0, 3:5] = jnp.where(even_core, mine[3:5], theirs[3:5])
    early_z[0, 5:7] = jnp.where(even_core, theirs[3:5], mine[3:5])
    early_z[0, 7:8] = jnp.zeros((1, 128), FULL)
    for k in range(1, Z):
        send(K_EZ + k, early_z.at[0], early_z.at[k], {"ctx": mate(2 * k)})
    near(8)
    near(9)
    pl.when(is_mid)(functools.partial(far, 6))
    pl.when(is_mid)(functools.partial(far, 7))
    near(10)
    near(11)
    pl.when(is_mid)(functools.partial(far, 8))
    pl.when(is_mid)(functools.partial(far, 9))
    near(12)
    near(13)
    pl.when(is_mid)(functools.partial(far, 10))
    pl.when(is_mid)(functools.partial(far, 11))
    near(14)
    near(15)
    pl.when(is_mid)(functools.partial(far, 12))
    pl.when(is_mid)(functools.partial(far, 13))
    own_gq = gq_tx[my_rows].astype(FULL)
    for d in planes:
        arrived(K_GQ + d, gq_rx.at[d])
        own_gq = own_gq + gq_rx[d].astype(FULL)
    qkvfin_ref[i] = own_gq.astype(LOW)
    spread = Relay(lambda j: qkvfin_ref.at[j])

    spread.begin()
    for d in planes:
        send(K_A2 + d, a2_tx.at[d], a2_rx.at[d], {"shard": plane(d)})
    for seq in range(shards):
        for core in range(2):
            k = 2 * seq + core

            @pl.when((seq != s) | (2 * s + core != i))
            def _():
                arrived(K_O + k, o_rx.at[k])

            attn[pl.ds(block * seq, block), 128 * core : 128 * (core + 1)] = o_rx[k]
    for d in range(shards):
        mine = attn[tokens(plane(d))]
        total = out_acc[pl.ds(block * d, block)] + dot(mine, wout[...])
        if d:
            out_tx[d] = total.astype(LOW)
        else:
            out_acc[pl.ds(0, block)] = total
    go = dot(attn[tokens(plane(0))], cot[pl.ds(0, block)], ROWS_CONTRACT)
    for d in planes:
        go = go + dot(attn[tokens(plane(d))], cot[pl.ds(block * d, block)], ROWS_CONTRACT)
    go16[pl.ds(0, HEAD_DIM)] = go[:HEAD_DIM].astype(LOW)
    go16[pl.ds(HEAD_DIM, HEAD_DIM)] = (
        go[HEAD_DIM : 2 * HEAD_DIM] + go[2 * HEAD_DIM : 3 * HEAD_DIM]
    ).astype(LOW)
    go16[pl.ds(2 * HEAD_DIM, HEAD_DIM)] = go[3 * HEAD_DIM :].astype(LOW)
    send(K_GO, go16.at[pl.ds(at16(other * half_rows), half_rows)], go_rx, partner)

    for d in planes:
        send(K_OUT + d, out_tx.at[d], out_rx.at[d], {"shard": plane(d)})
    arrived(K_GO, go_rx)
    line_own[pl.ds(OUT, half_rows)] = (
        go16[pl.ds(at16(c * half_rows), half_rows)].astype(FULL) + go_rx[...].astype(FULL)
    ).astype(LOW)
    for q in range(first_out, chunks):
        near_end(q)
    pl.when(is_mid)(functools.partial(far, 14))
    pl.when(is_mid)(functools.partial(far, 15))
    spread.step_inner(1)
    for t in reversed(range(1, Z)):
        a1_right(t, low_side)
        a1_left(Z - 1 - t, jnp.logical_not(low_side))
    for t in reversed(range(1, Z)):
        a1_right(t, jnp.logical_not(low_side))
        a1_left(Z - 1 - t, low_side)
    for k in range(1, Z):
        arrived(K_EZ + k, early_z.at[k])
    early_x[0, 0:8] = sum((early_z[k] for k in range(1, Z)), early_z[0])
    slabs_end = 8 + 4 * Z
    for chip in range(Z):
        early_x[0, 8 + 4 * chip : 12 + 4 * chip] = early_z[flip(z, chip), 3:7]
    for d in planes:
        send(K_EX + d, early_x.at[0], early_x.at[d], {"shard": plane(d)})
    for q in range(first_out):
        pl.when(is_end)(functools.partial(far, q))
    a1 = a1_own[z].astype(FULL)

    @pl.when(has_left)
    def _():
        arrived(K_A1R + z, a1_rx_r.at[z])

    @pl.when(has_right)
    def _():
        arrived(K_A1L + z, a1_rx_l.at[z])

    a1 = a1 + a1_rx_r[z].astype(FULL) + a1_rx_l[z].astype(FULL)
    a2 = a2_acc[pl.ds(0, block)]
    for d in planes:
        arrived(K_A2 + d, a2_rx.at[d])
        a2 = a2 + a2_rx[d].astype(FULL)
    sums = (a1 * normal, a1, a2 * normal, a2)
    for k, field in enumerate(sums):
        total = jnp.sum(field, axis=0, keepdims=True)
        for n in range(width // 128):
            at = (k % 2) * (width // 128) + n
            late_a[k // 2, at : at + 1] = total[:, 128 * n : 128 * (n + 1)]
    K_LD = channels(1)
    K_LZ = channels(Z)
    K_LX = channels(shards)
    K_LF = channels(1)
    send(K_LD, late_a.at[other], late_d2d, partner)
    mixed = a1 * gain1 + a2 * gain2
    back = r * (
        mixed
        - jnp.mean(mixed, axis=-1, keepdims=True)
        - normal * jnp.mean(mixed * normal, axis=-1, keepdims=True)
    )
    dx_ref[...] = (cot[pl.ds(0, block)].astype(FULL) + back).astype(LOW)
    spread.step_outer(1)
    arrived(K_LD, late_d2d)
    late_z[0] = late_a[c] + late_d2d[...]
    for k in range(1, Z):
        send(K_LZ + k, late_z.at[0], late_z.at[k], {"ctx": mate(2 * k)})
    for q in range(first_out, chunks):
        near(q)
    spread.step_inner(2)
    spread.step_outer(2)
    total = x_ref[...].astype(FULL) + out_acc[pl.ds(0, block)]
    for d in planes:
        arrived(K_OUT + d, out_rx.at[d])
        total = total + out_rx[d].astype(FULL)
    y_ref[...] = total.astype(LOW)
    for k in range(1, Z):
        arrived(K_LZ + k, late_z.at[k])
    late_x[0] = sum((late_z[k] for k in range(1, Z)), late_z[0])
    for d in planes:
        send(K_LX + d, late_x.at[0], late_x.at[d], {"shard": plane(d)})
    for q in range(first_out, chunks):
        far(q)
    for k in range(3, Z):
        spread.step(k)
    for d in planes:
        arrived(K_LX + d, late_x.at[d])
        arrived(K_EX + d, early_x.at[d])
    late_ref[c] = sum((late_x[d] for d in planes), late_x[0])
    early_ref[c, 0:slabs_end] = sum((early_x[d] for d in planes), early_x[0])
    for j in range(shards):
        at = slabs_end + 8 * j
        early_ref[c, at : at + 8] = early_x[flip(s, j), 0:8]
    send(K_LF, late_ref.at[c], late_ref.at[c], partner)
    send(K_EF, early_ref.at[c], early_ref.at[c], partner)
    spread.end()
    arrived(K_LF, late_ref.at[other])
    arrived(K_EF, early_ref.at[other])
    for q in range(chunks):
        arrived(K_FIN + q, fin_ref.at[other, span_of(q)])
    assert used[0] <= ssem.shape[0]
    for copy, when in sent:
        if when is always:
            copy.wait_send()
        else:
            pl.when(when)(copy.wait_send)
    for q in range(chunks):
        fin_copy(q).wait_send()
        pl.when(is_end)(near_copy(q, line_own, K_NEAR).wait_send)
        pl.when(is_mid)(near_copy(q, line_near, K_INNER).wait_send)
        pl.when(is_mid)(far_copy(q).wait_send)


def ring_on_device(
    layer_input,
    positions,
    cotangent,
    ln1_gain,
    ln1_bias,
    ln2_gain,
    ln2_bias,
    w_qkv,
    qkv_bias,
    w_out,
    w_up,
    up_bias,
    w_down,
):
    seqs_here, block_len, feature_count = layer_input.shape
    row_count = seqs_here * block_len
    head_count = HEADS
    head_size = HEAD_DIM
    score_scale = head_size ** (-0.5)
    whole_qkv, whole_out, whole_up, whole_down = (
        lax.all_gather(w_qkv, "shard", axis=0, tiled=True),
        lax.all_gather(w_out, "shard", axis=0, tiled=True),
        lax.all_gather(w_up, "shard", axis=0, tiled=True),
        lax.all_gather(w_down, "shard", axis=0, tiled=True),
    )
    all_positions = lax.all_gather(positions, "ctx", axis=1, tiled=True)
    cycle_size = lax.axis_size("ctx")
    my_index = lax.axis_index("ctx")
    inputs = layer_input.astype(jnp.float32).reshape(row_count, feature_count)
    normed_one = layer_norm(inputs, ln1_gain, ln1_bias).astype(jnp.bfloat16)
    normed_two = layer_norm(inputs, ln2_gain, ln2_bias).astype(jnp.bfloat16)
    projected = jnp.dot(normed_one, whole_qkv, preferred_element_type=jnp.float32) + qkv_bias
    split_heads = projected.reshape(seqs_here, block_len, 3, head_count, head_size)
    cosine, sine_table = rotary_tables(positions)
    queries = rotate(split_heads[:, :, 0], cosine, sine_table).astype(jnp.bfloat16)
    key_rows = rotate(split_heads[:, :, 1], cosine, sine_table).astype(jnp.bfloat16)
    value_rows = split_heads[:, :, 2].astype(jnp.bfloat16)
    top_query = jnp.max(positions)

    def attend_block(running, key_blk, value_blk, key_pos):

        def attend_update(current):
            run_max, run_sum, run_acc = current
            scores = (
                jnp.einsum("sqhd,skhd->shqk", queries, key_blk, preferred_element_type=jnp.float32)
                * score_scale
            )
            allowed = key_pos[:, None, None, :] <= positions[:, None, :, None]
            masked = jnp.where(allowed, scores, NEGATIVE)
            new_max = jnp.maximum(run_max, jnp.max(masked, axis=-1))
            shrink = jnp.exp(run_max - new_max)
            weights_now = jnp.where(allowed, jnp.exp(masked - new_max[..., None]), 0.0)
            run_sum = run_sum * shrink + jnp.sum(weights_now, axis=-1)
            added_term = jnp.einsum(
                "shqk,skhd->sqhd",
                weights_now.astype(jnp.bfloat16),
                value_blk,
                preferred_element_type=jnp.float32,
            )
            run_acc = run_acc * jnp.transpose(shrink, (0, 2, 1))[..., None] + added_term
            return (new_max, run_sum, run_acc)

        return lax.cond(
            jnp.min(key_pos) <= top_query, attend_update, lambda unchanged: unchanged, running
        )

    initial = (
        jnp.full((seqs_here, head_count, block_len), NEGATIVE, jnp.float32),
        jnp.zeros((seqs_here, head_count, block_len), jnp.float32),
        jnp.zeros((seqs_here, block_len, head_count, head_size), jnp.float32),
    )
    own_block = attend_block(initial, key_rows, value_rows, positions)

    def cycle_forward(turn_index, carried):
        current, key_cur, value_cur = carried
        key_cur, value_cur = shifted((key_cur, value_cur), "ctx", 1)
        source = (my_index - turn_index) % cycle_size
        key_pos = lax.dynamic_slice_in_dim(all_positions, source * block_len, block_len, 1)
        return (attend_block(current, key_cur, value_cur, key_pos), key_cur, value_cur)

    (run_max, run_sum, run_acc), unused_key, unused_value = lax.fori_loop(
        1, cycle_size, cycle_forward, (own_block, key_rows, value_rows)
    )
    attn_vals = run_acc / jnp.transpose(run_sum, (0, 2, 1))[..., None]
    log_total = run_max + jnp.log(run_sum)
    attn_low = attn_vals.astype(jnp.bfloat16).reshape(row_count, feature_count)
    attn_branch = jnp.dot(attn_low, whole_out, preferred_element_type=jnp.float32)
    hidden_pre = jnp.dot(normed_two, whole_up, preferred_element_type=jnp.float32) + up_bias
    hidden_low = gelu_exact(hidden_pre).astype(jnp.bfloat16)
    mlp_branch = jnp.dot(hidden_low, whole_down, preferred_element_type=jnp.float32)
    layer_output = (
        (inputs + attn_branch + mlp_branch)
        .astype(jnp.bfloat16)
        .reshape(seqs_here, block_len, feature_count)
    )
    cot_low = cotangent.reshape(row_count, feature_count)
    cot_full = cot_low.astype(jnp.float32)
    grad_down = jnp.einsum("rf,rd->fd", hidden_low, cot_low, preferred_element_type=jnp.float32)
    grad_hidden = jnp.einsum("rd,fd->rf", cot_low, whole_down, preferred_element_type=jnp.float32)
    unused_gelu, gelu_back = jax.vjp(gelu_exact, hidden_pre)
    grad_pre = gelu_back(grad_hidden)[0].astype(jnp.bfloat16)
    grad_up_bias = jnp.sum(grad_pre.astype(jnp.float32), axis=0)
    grad_up = jnp.einsum("rd,rf->df", normed_two, grad_pre, preferred_element_type=jnp.float32)
    grad_two = jnp.einsum("rf,df->rd", grad_pre, whole_up, preferred_element_type=jnp.float32)
    grad_out = jnp.einsum("rd,re->de", attn_low, cot_low, preferred_element_type=jnp.float32)
    grad_attn = (
        jnp.einsum("re,de->rd", cot_low, whole_out, preferred_element_type=jnp.float32)
        .astype(jnp.bfloat16)
        .reshape(seqs_here, block_len, head_count, head_size)
    )
    row_delta = jnp.transpose(
        jnp.sum(grad_attn.astype(jnp.float32) * attn_vals, axis=-1), (0, 2, 1)
    )

    def back_block(grads_in, key_blk, value_blk, key_pos):

        def back_update(current):
            grad_query, grad_key, grad_value = current
            scores = (
                jnp.einsum("sqhd,skhd->shqk", queries, key_blk, preferred_element_type=jnp.float32)
                * score_scale
            )
            allowed = key_pos[:, None, None, :] <= positions[:, None, :, None]
            masked = jnp.where(allowed, scores, NEGATIVE)
            probability = jnp.exp(masked - log_total[..., None])
            prob_low = probability.astype(jnp.bfloat16)
            grad_value = grad_value + jnp.einsum(
                "shqk,sqhd->skhd", prob_low, grad_attn, preferred_element_type=jnp.float32
            )
            grad_prob = jnp.einsum(
                "sqhd,skhd->shqk", grad_attn, value_blk, preferred_element_type=jnp.float32
            )
            grad_score = (probability * (grad_prob - row_delta[..., None])).astype(jnp.bfloat16)
            grad_query = (
                grad_query
                + jnp.einsum(
                    "shqk,skhd->sqhd", grad_score, key_blk, preferred_element_type=jnp.float32
                )
                * score_scale
            )
            grad_key = (
                grad_key
                + jnp.einsum(
                    "shqk,sqhd->skhd", grad_score, queries, preferred_element_type=jnp.float32
                )
                * score_scale
            )
            return (grad_query, grad_key, grad_value)

        return lax.cond(
            jnp.min(key_pos) <= top_query, back_update, lambda unchanged: unchanged, grads_in
        )

    zero_rows = jnp.zeros((seqs_here, block_len, head_count, head_size), jnp.float32)

    def pass_back(grad_key, grad_value):
        return (
            shifted(grad_key.astype(jnp.bfloat16), "ctx", 1).astype(grad_key.dtype),
            shifted(grad_value.astype(jnp.bfloat16), "ctx", 1).astype(grad_value.dtype),
        )

    grad_query, grad_key, grad_value = back_block(
        (zero_rows, zero_rows, zero_rows), key_rows, value_rows, positions
    )
    grad_key, grad_value = pass_back(grad_key, grad_value)

    def cycle_backward(turn_index, carried):
        grad_query, key_cur, value_cur, grad_key, grad_value = carried
        key_cur, value_cur = shifted((key_cur, value_cur), "ctx", 1)
        source = (my_index - turn_index) % cycle_size
        key_pos = lax.dynamic_slice_in_dim(all_positions, source * block_len, block_len, 1)
        grad_query, grad_key, grad_value = back_block(
            (grad_query, grad_key, grad_value), key_cur, value_cur, key_pos
        )
        grad_key, grad_value = pass_back(grad_key, grad_value)
        return (grad_query, key_cur, value_cur, grad_key, grad_value)

    grad_query, unused_key, unused_value, grad_key, grad_value = lax.fori_loop(
        1, cycle_size, cycle_backward, (grad_query, key_rows, value_rows, grad_key, grad_value)
    )
    unused_rot, rotate_back = jax.vjp(
        lambda field_in: rotate(field_in, cosine, sine_table), zero_rows
    )
    query_pre = rotate_back(grad_query)[0]
    key_pre = rotate_back(grad_key)[0]
    grad_proj = (
        jnp.stack([query_pre, key_pre, grad_value], axis=2)
        .reshape(row_count, 3 * feature_count)
        .astype(jnp.bfloat16)
    )
    grad_qkv_bias = jnp.sum(grad_proj.astype(jnp.float32), axis=0)
    grad_qkv = jnp.einsum("rd,re->de", normed_one, grad_proj, preferred_element_type=jnp.float32)
    grad_one = jnp.einsum("re,de->rd", grad_proj, whole_qkv, preferred_element_type=jnp.float32)
    unused_one, norm_back_one = jax.vjp(layer_norm, inputs, ln1_gain, ln1_bias)
    input_one, grad_gain_one, grad_bias_one = norm_back_one(grad_one)
    unused_two, norm_back_two = jax.vjp(layer_norm, inputs, ln2_gain, ln2_bias)
    input_two, grad_gain_two, grad_bias_two = norm_back_two(grad_two)
    grad_input = (
        (cot_full + input_one + input_two)
        .astype(jnp.bfloat16)
        .reshape(seqs_here, block_len, feature_count)
    )
    summed = (
        lax.psum(grad_qkv.astype(jnp.bfloat16), "ctx").astype(jnp.float32),
        lax.psum(grad_out.astype(jnp.bfloat16), "ctx").astype(jnp.float32),
        lax.psum(grad_up.astype(jnp.bfloat16), "ctx").astype(jnp.float32),
        lax.psum(grad_down.astype(jnp.bfloat16), "ctx").astype(jnp.float32),
        lax.psum(grad_gain_one.astype(jnp.bfloat16), "ctx").astype(jnp.float32),
        lax.psum(grad_bias_one.astype(jnp.bfloat16), "ctx").astype(jnp.float32),
        lax.psum(grad_gain_two.astype(jnp.bfloat16), "ctx").astype(jnp.float32),
        lax.psum(grad_bias_two.astype(jnp.bfloat16), "ctx").astype(jnp.float32),
        lax.psum(grad_qkv_bias.astype(jnp.bfloat16), "ctx").astype(jnp.float32),
        lax.psum(grad_up_bias.astype(jnp.bfloat16), "ctx").astype(jnp.float32),
    )
    sum_qkv, sum_out, sum_up, sum_down = (
        lax.psum_scatter(
            summed[0].astype(jnp.bfloat16), "shard", scatter_dimension=0, tiled=True
        ).astype(jnp.float32),
        lax.psum_scatter(
            summed[1].astype(jnp.bfloat16), "shard", scatter_dimension=0, tiled=True
        ).astype(jnp.float32),
        lax.psum_scatter(
            summed[2].astype(jnp.bfloat16), "shard", scatter_dimension=0, tiled=True
        ).astype(jnp.float32),
        lax.psum_scatter(
            summed[3].astype(jnp.bfloat16), "shard", scatter_dimension=0, tiled=True
        ).astype(jnp.float32),
    )
    sum_small = (
        lax.psum(summed[4].astype(jnp.bfloat16), "shard").astype(jnp.float32),
        lax.psum(summed[5].astype(jnp.bfloat16), "shard").astype(jnp.float32),
        lax.psum(summed[6].astype(jnp.bfloat16), "shard").astype(jnp.float32),
        lax.psum(summed[7].astype(jnp.bfloat16), "shard").astype(jnp.float32),
        lax.psum(summed[8].astype(jnp.bfloat16), "shard").astype(jnp.float32),
        lax.psum(summed[9].astype(jnp.bfloat16), "shard").astype(jnp.float32),
    )
    return (
        layer_output,
        grad_input,
        sum_small[0],
        sum_small[1],
        sum_small[2],
        sum_small[3],
        sum_qkv,
        sum_small[4],
        sum_out,
        sum_up,
        sum_small[5],
        sum_down,
    )


def finish_body(
    y_in, dx_in, fin_in, qkvfin_in, early_in, late_in,
    y_out, dx_out, g1_out, b1_out, g2_out, b2_out, gqkv_out, gqkvb_out, gout_out, gup_out, gupb_out, gdown_out,
    gqkv, gout, gup, gdown, fin, qkvfin, early, late, y, dx, sem, in_sem,
):
    width = y_in.shape[1]
    chips = qkvfin.shape[0] // 2
    rows = qkvfin.shape[1]
    half = rows // 2
    cut = width // 2
    shards = width // rows
    slabs = 8 + 4 * chips
    copies = []
    coming = []

    def bring(src, dst):
        copy = pltpu.make_async_copy(src, dst, in_sem.at[len(coming)])
        copy.start()
        coming.append(copy)

    for h in range(2):
        bring(fin_in.at[h, pl.ds(0, cut)], fin.at[h, pl.ds(0, cut)])
    for h in range(2):
        bring(
            fin_in.at[h, pl.ds(cut, fin.shape[1] - cut)], fin.at[h, pl.ds(cut, fin.shape[1] - cut)]
        )
    bring(qkvfin_in, qkvfin)
    bring(y_in, y)
    bring(dx_in, dx)
    bring(early_in, early)
    bring(late_in, late)

    def out(src, dst):
        copy = pltpu.make_async_copy(src, dst, sem.at[len(copies)])
        copy.start()
        copies.append(copy)

    for h in range(2):
        coming[h].wait()
        gdown[pl.ds(cut * h, cut)] = fin[h, pl.ds(0, cut)].astype(FULL)
        out(gdown.at[pl.ds(cut * h, cut)], gdown_out.at[pl.ds(cut * h, cut)])
    for h in range(2):
        coming[2 + h].wait()
        mine = pl.ds(half * h, half)
        for n in range(shards):
            here = fin[h, pl.ds(cut + half * n, half)]
            gup[mine, width * n : width * (n + 1)] = here.astype(FULL)
        out(gup.at[mine], gup_out.at[mine])

    for copy in coming[4:]:
        copy.wait()
    out(y, y_out.at[0])
    out(dx, dx_out.at[0])

    def tiles(piece, wide, put):
        lane = lax.broadcasted_iota(jnp.int32, wide, 1)
        low_lanes = lane < HEAD_DIM
        for part in range(3):
            for w in range(chips // 2):
                p0, p1, p2, p3 = (piece(4 * w + t, part) for t in range(4))
                r1, r2 = pltpu.roll(p1, HEAD_DIM, 1), pltpu.roll(p2, HEAD_DIM, 1)
                at = width * part + 384 * w
                put(at, p0 + jnp.where(low_lanes, 0.0, r1))
                put(at + 128, jnp.where(low_lanes, r1, r2))
                put(at + 256, p3 + jnp.where(low_lanes, r2, 0.0))

    def put_rows(at, tile):
        gqkv[:, at : at + 128] = tile

    tiles(
        lambda j, part: qkvfin[j, :, 128 * part : 128 * (part + 1)].astype(FULL),
        (rows, 128),
        put_rows,
    )
    out(gqkv, gqkv_out)
    for h in range(2):
        gout[pl.ds(half * h, half)] = fin[h, pl.ds(cut + half * shards, half)].astype(FULL)
    out(gout, gout_out)

    def bias_piece(j, part):
        row = early[part % 2, 8 + 2 * j + part // 2]
        return jnp.broadcast_to(row[None, :], (8, 128))

    def put_bias(at, tile):
        gqkvb_out[pl.ds(at, 128)] = tile[0]

    tiles(bias_piece, (8, 128), put_bias)
    for n in range(shards):
        for t in range(width // 256):
            for h in range(2):
                gupb_out[pl.ds(width * n + 256 * t + 128 * h, 128)] = early[h, slabs + 8 * n + t]
    for k, vector in enumerate((g1_out, b1_out, g2_out, b2_out)):
        for n in range(width // 128):
            vector[pl.ds(128 * n, 128)] = late[k // 2, (k % 2) * (width // 128) + n]
    for copy in copies:
        copy.wait()


def finish(rows, shards, ctxs, *pieces):
    block, width = pieces[0].shape
    vmem = pl.BlockSpec(memory_space=pltpu.VMEM)
    hbm = pl.BlockSpec(memory_space=pl.ANY)
    shape = jax.ShapeDtypeStruct
    vector = shape((width,), FULL)
    return pl.pallas_call(
        finish_body,
        out_shape=(
            shape((1, block, width), LOW),
            shape((1, block, width), LOW),
            vector,
            vector,
            vector,
            vector,
            shape((rows, 3 * width), FULL),
            shape((3 * width,), FULL),
            shape((rows, width), FULL),
            shape((rows, shards * width), FULL),
            shape((shards * width,), FULL),
            shape((width, width), FULL),
        ),
        in_specs=[hbm] * 6,
        out_specs=(hbm, hbm, vmem, vmem, vmem, vmem, hbm, vmem, hbm, hbm, vmem, hbm),
        scratch_shapes=[
            pltpu.VMEM((rows, 3 * width), FULL),
            pltpu.VMEM((rows, width), FULL),
            pltpu.VMEM((rows, shards * width), FULL),
            pltpu.VMEM((width, width), FULL),
            pltpu.VMEM(pieces[2].shape, LOW),
            pltpu.VMEM(pieces[3].shape, LOW),
            pltpu.VMEM(pieces[4].shape, FULL),
            pltpu.VMEM(pieces[5].shape, FULL),
            pltpu.VMEM((block, width), LOW),
            pltpu.VMEM((block, width), LOW),
            pltpu.SemaphoreType.DMA((8,)),
            pltpu.SemaphoreType.DMA((16,)),
        ],
        compiler_params=pltpu.CompilerParams(vmem_limit_bytes=60 * 1024 * 1024),
        name="finish",
    )(*pieces)


def fused_on_device(
    layer_input,
    positions,
    cotangent,
    ln1_gain,
    ln1_bias,
    ln2_gain,
    ln2_bias,
    w_qkv,
    qkv_bias,
    w_out,
    w_up,
    up_bias,
    w_down,
):
    shards, ctxs = lax.axis_size("shard"), lax.axis_size("ctx")
    block, width = layer_input.shape[1:]
    rows = w_qkv.shape[0]
    half = rows // 2
    line_rows = width // 2 + half + shards * half
    vmem = pl.BlockSpec(memory_space=pltpu.VMEM)
    hbm = pl.BlockSpec(memory_space=pl.ANY)
    low, full = (lambda *shape: pltpu.VMEM(shape, LOW)), (lambda *shape: pltpu.VMEM(shape, FULL))
    chips = ctxs // 2
    scratch = dict(
        wq=low(width, 384),
        wraw=low(3, rows, 256),
        wup=low(width, width),
        wout=low(256, width),
        wdn=low(width, width),
        n1=low(ctxs * block, width),
        n2=low(shards * block, width),
        cot=low(shards * block, width),
        pos_tx=pltpu.VMEM((8, block), jnp.int32),
        pos_rx=pltpu.VMEM((ctxs, 8, block), jnp.int32),
        pos_sm=pltpu.SMEM((ctxs, 8, block), jnp.int32),
        qkv=full(ctxs, block, 384),
        q_s=low(ctxs * block, 128),
        k_s=low(ctxs * block, 128),
        v_s=low(ctxs * block, 128),
        do_tx=low(shards, 2, block, 128),
        do_mid=low(shards, 2, block, 128),
        do_rx=low(ctxs, block, 128),
        do_s=low(ctxs * block, 128),
        o_s=full(ctxs, block, 128),
        dq_s=full(ctxs * block, 128),
        dk_s=full(ctxs * block, 128),
        dv_s=full(ctxs * block, 128),
        gp_s=low(ctxs, block, 384),
        gp_e=low(ctxs * block, 384),
        o_tx=low(ctxs, block, 128),
        o_rx=low(2 * shards, block, 128),
        attn=low(shards * block, 256),
        a1_p=low(ctxs, block, width),
        a1_d2d=low(chips, block, width),
        a1_own=low(chips, block, width),
        a1_tx_r=low(chips, block, width),
        a1_tx_l=low(chips, block, width),
        a1_rx_r=low(chips, block, width),
        a1_rx_l=low(chips, block, width),
        gq_tx=low(width, 384),
        gq_rx=low(shards, rows, 384),
        out_acc=full(shards * block, width),
        a2_acc=full(shards * block, width),
        out_tx=low(shards, block, width),
        out_rx=low(shards, block, width),
        a2_tx=low(shards, block, width),
        a2_rx=low(shards, block, width),
        gd16=low(width, width),
        gd_rx=low(width // 2, width),
        gu16=low(width, width),
        gu_rx=low(shards, half, width),
        gu_tx=low(shards, half, width),
        go16=low(rows, width),
        go_rx=low(half, width),
        line_own=low(line_rows, width),
        line_rx=low(2, line_rows, width),
        line_near=low(line_rows, width),
        line_far=low(line_rows, width),
        early_a=full(2, 8, 128),
        early_d2d=full(8, 128),
        early_z=full(chips, 8, 128),
        early_x=full(shards, 8 + 4 * chips, 128),
        late_a=full(2, width // 64, 128),
        late_d2d=full(width // 64, 128),
        late_z=full(chips, width // 64, 128),
        late_x=full(shards, width // 64, 128),
        ssem=pltpu.SemaphoreType.DMA((420,)),
        rsem=pltpu.SemaphoreType.DMA((420,)),
        lsem=pltpu.SemaphoreType.DMA((16,)),
    )
    slabs = 8 + 4 * chips
    y, dx, fin, qkvfin, early, late = pl.pallas_call(
        functools.partial(fused_body, tuple(scratch)),
        out_shape=(
            jax.ShapeDtypeStruct((block, width), LOW),
            jax.ShapeDtypeStruct((block, width), LOW),
            jax.ShapeDtypeStruct((2, line_rows, width), LOW),
            jax.ShapeDtypeStruct((ctxs, rows, 384), LOW),
            jax.ShapeDtypeStruct((2, slabs + 8 * shards, 128), FULL),
            jax.ShapeDtypeStruct((2, width // 64, 128), FULL),
        ),
        in_specs=[vmem] * 9 + [hbm] * 5,
        out_specs=(vmem,) * 6,
        scratch_shapes=list(scratch.values()),
        compiler_params=pltpu.CompilerParams(
            collective_id=0, has_side_effects=True, vmem_limit_bytes=60 * 1024 * 1024
        ),
        name="layer",
    )(
        layer_input[0],
        positions,
        ln1_gain,
        ln1_bias,
        ln2_gain,
        ln2_bias,
        qkv_bias,
        up_bias,
        jnp.asarray(rotary_constants(ctxs, block)),
        cotangent[0],
        w_qkv,
        w_up,
        w_out,
        w_down,
    )
    return finish(rows, shards, ctxs, y, dx, fin, qkvfin, early, late)


def on_device(layer_input, positions, cotangent, *params):
    shards, ctxs = lax.axis_size("shard"), lax.axis_size("ctx")
    seqs, block, width = layer_input.shape
    rows, ff = params[4].shape[0], params[7].shape[1]
    fits = (
        seqs == 1
        and block == 128
        and (shards, ctxs) == (4, 8)
        and 3 * ctxs == 2 * HEADS
        and HEAD_DIM == 64
        and rows * shards == width == HEADS * HEAD_DIM
        and ff == shards * width
    )
    path = fused_on_device if fits else ring_on_device
    return path(layer_input, positions, cotangent, *params)


def solution(mesh):
    placed = (
        P("shard", "ctx", None),
        P("shard", "ctx"),
        P("shard", "ctx", None),
        P(),
        P(),
        P(),
        P(),
        P("shard", None),
        P(),
        P("shard", None),
        P("shard", None),
        P(),
        P("shard", None),
    )
    return jax.shard_map(
        on_device,
        mesh=mesh,
        in_specs=placed,
        out_specs=(
            P("shard", "ctx", None),
            P("shard", "ctx", None),
            P(),
            P(),
            P(),
            P(),
            P("shard", None),
            P(),
            P("shard", None),
            P("shard", None),
            P(),
            P("shard", None),
        ),
        check_vma=False,
    )
```
